32 devices in a mesh: groups: 2 (over x), patch: 16 (over z, y, core).
Axes of the slice: x: 2, y: 2, z: 4, core: 2. Of those that a mesh axis runs over, the one named last changes fastest.
Arguments:
- tokens: bfloat16 [16384, 1152], P(('groups', 'patch')), parts along dimension 0, may hold values from -6 to 6
- stale_kv: bfloat16 [16384, 1152], P(('groups', 'patch')), parts along dimension 0, may hold values from -40 to 40, as said below
- mod_table: float32 [6, 1152], replicated, may hold values from -2 to 3
- mod_mix: float32 [6, 1152], replicated, may hold values from -3 to 3
- timestep: int32 [2], P('groups'), parts along dimension 0, may hold values from 0 to 999
- frame_order: int32 [8], P('groups'), parts along dimension 0, may hold values from 0 to 3, each once
- spatial_qkv: bfloat16 [3, 1152, 576], replicated, may hold values from -0.1875 to 0.1875
- spatial_out: bfloat16 [576, 1152], replicated, may hold values from -0.25 to 0.25
- temporal_qkv: bfloat16 [3, 1152, 576], replicated, may hold values from -0.1875 to 0.1875
- temporal_out: bfloat16 [576, 1152], replicated, may hold values from -0.25 to 0.25
Outputs:
- block_out: float32 [16384, 1152], P(('groups', 'patch')), parts along dimension 0
The draws below stay inside these ranges and needn't reach their ends.
There are 2 independent parts, one for each index of `groups`. The reference program is written for one: setup_inputs(seed, part) draws one part's arguments, and reference() takes and returns one part's arrays. A program takes and returns all parts, laid end to end along the dimension named above; an argument that names none is the same for every part. Nothing has to cross between parts.
Inputs may be any that keep to these rules, and one draw needn't show every extreme that they name: `frame_order`: a permutation of the 4 time positions. `stale_kv`: previous step's keys and values.
All inputs are finite; a program needn't handle non-finite values.
Results may differ from the reference program's by a relative error of at most 0.013.
The reference program's roundings to bfloat16 on the way count: a program that leaves them out, or rounds other values in their place, can miss the bound.
Values may be sent and summed in bfloat16 or wider, within the bound.
No kernel may reach another device: no remote copies, remote signals or barrier semaphores. Data moves between devices by JAX's collectives and lax.ppermute only.
A program may use at most 128 MiB of HBM per device.

```python
import math
import jax
import jax.numpy as jnp
from jax import lax

D = 1152
HEADS = 16
HEADS_WIN = 8
WIN = 576
PATCH_TOK = 512
FRAMES = 4
FRAME_TOK = 2048
TOKENS = 8192


def draw_stale_kv(key, part):
    width_win = HEADS_WIN * (D // HEADS)
    base = jnp.clip(jax.random.normal(jax.random.fold_in(key, 11), (TOKENS, 2 * width_win), jnp.float32), -5.0, 5.0)
    return base.astype(jnp.bfloat16)


def draw_mod_table(key, part):
    table = jnp.clip(0.5 * jax.random.normal(jax.random.fold_in(key, 21), (6, D), jnp.float32), -2.0, 2.0)
    return table


def levels(rng, shape, split, smallest, largest):
    loudness, own = 1.0, jax.random.fold_in(rng, 6)
    for axis_at, blocks in split:
        heights = jnp.exp(jax.random.uniform(jax.random.fold_in(own, axis_at), (blocks,), jnp.float32, smallest / len(split), largest / len(split)))
        loudness = loudness * jnp.repeat(heights, shape[axis_at] // blocks).reshape([-1 if axis == axis_at else 1 for axis in range(len(shape))])
    return loudness


def scatter_about(own_key, shape, width, limit, shards=(), kind=jnp.bfloat16):
    entries = jax.random.normal(own_key, shape, jnp.float32) * width
    if len(shards) > 0:
        entries = levels(own_key, shape, shards, -0.22, 0.18) * entries
    return jnp.clip(entries, min=-limit, max=limit).astype(kind)


def setup_inputs(seed: int = 0, part: int = 0) -> dict:
    key_list = jax.random.split(jax.random.key(seed), 11)
    part_keys = jax.random.split(jax.random.fold_in(key_list[10], part), 11)
    tokens = scatter_about(part_keys[0], (TOKENS, D), 1.0, 6.0, ((0, 16),))
    stale_kv = draw_stale_kv(jax.random.fold_in(jax.random.fold_in(key_list[10], part), 71), part)
    mod_table = draw_mod_table(jax.random.fold_in(key_list[10], 71), part)
    mod_mix = scatter_about(key_list[3], (6, D), 0.5, 3.0, (), jnp.float32)
    timestep = jax.random.randint(part_keys[4], (1,), 0, 1000).astype(jnp.int32)
    frame_order = jax.random.permutation(part_keys[5], FRAMES).astype(jnp.int32)
    spatial_qkv = scatter_about(key_list[6], (3, D, WIN), D ** -0.5, 0.1875)
    spatial_out = scatter_about(key_list[7], (WIN, D), WIN ** -0.5, 0.25)
    temporal_qkv = scatter_about(key_list[8], (3, D, WIN), D ** -0.5, 0.1875)
    temporal_out = scatter_about(key_list[9], (WIN, D), WIN ** -0.5, 0.25)
    return {"tokens": tokens, "stale_kv": stale_kv, "mod_table": mod_table, "mod_mix": mod_mix, "timestep": timestep, "frame_order": frame_order, "spatial_qkv": spatial_qkv, "spatial_out": spatial_out, "temporal_qkv": temporal_qkv, "temporal_out": temporal_out}


epsilon = 1e-06

def normalize(activations):
    row_mean = lax.optimization_barrier(jnp.mean(activations, axis=-1, keepdims=True))
    centered = activations - row_mean
    variance = lax.optimization_barrier(jnp.mean(centered * centered, axis=-1, keepdims=True))
    return centered * lax.rsqrt(variance + epsilon)

def sinusoid(position, feature_width):
    half_width = feature_width // 2
    frequencies = jnp.exp(-math.log(10000.0) * jnp.arange(half_width, dtype=jnp.float32) / half_width)
    angles = jnp.asarray(position).astype(jnp.float32)[..., None] * frequencies
    return jnp.concatenate([jnp.sin(angles), jnp.cos(angles)], axis=-1)

def softmax_rows(scores):
    row_top = lax.optimization_barrier(jnp.max(scores, axis=-1, keepdims=True))
    exp_scores = jnp.exp(scores - row_top)
    return (exp_scores / lax.optimization_barrier(jnp.sum(exp_scores, axis=-1, keepdims=True))).astype(jnp.bfloat16)

def project(inputs, weight):
    return jnp.dot(inputs, weight, preferred_element_type=jnp.float32)

def spatial_attend(queries, key_rows, value_rows):
    head_dim = D // HEADS
    query_heads = queries.reshape(-1, HEADS_WIN, head_dim).astype(jnp.float32)
    key_heads = key_rows.reshape(-1, HEADS_WIN, head_dim).astype(jnp.float32)
    value_heads = value_rows.reshape(-1, HEADS_WIN, head_dim).astype(jnp.float32)
    scores = jnp.einsum('qhe,khe->hqk', query_heads, key_heads) * head_dim ** (-0.5)
    weights = softmax_rows(scores)
    mixed_out = jnp.einsum('hqk,khe->qhe', weights.astype(jnp.float32), value_heads)
    return mixed_out.reshape(-1, HEADS_WIN * head_dim).astype(jnp.bfloat16)

def temporal_attend(queries, key_rows, value_rows):
    head_dim = D // HEADS
    frame_count = queries.shape[0]
    pixel_count = queries.shape[1]
    shape_heads = (frame_count, pixel_count, HEADS_WIN, head_dim)
    query_heads = queries.reshape(shape_heads).astype(jnp.float32)
    key_heads = key_rows.reshape(shape_heads).astype(jnp.float32)
    value_heads = value_rows.reshape(shape_heads).astype(jnp.float32)
    scores = jnp.einsum('fmhe,gmhe->mhfg', query_heads, key_heads) * head_dim ** (-0.5)
    weights = softmax_rows(scores)
    mixed_out = jnp.einsum('mhfg,gmhe->fmhe', weights.astype(jnp.float32), value_heads)
    return mixed_out.reshape(frame_count, pixel_count, HEADS_WIN * head_dim).astype(jnp.bfloat16)

def reference(tokens, stale_kv, mod_table, mod_mix, timestep, frame_order, spatial_qkv, spatial_out, temporal_qkv, temporal_out):
    width_win = HEADS_WIN * (D // HEADS)
    modulation = mod_table + mod_mix * sinusoid(timestep[0], D)[None, :]
    tokens_wide = tokens.astype(jnp.float32)
    spatial_in = (normalize(tokens_wide) * (1.0 + modulation[1]) + modulation[0]).astype(jnp.bfloat16)
    quartered = (FRAMES, 4, PATCH_TOK, width_win)
    fresh_q = project(spatial_in, spatial_qkv[0]).astype(jnp.bfloat16).reshape(quartered)
    fresh_k = project(spatial_in, spatial_qkv[1]).astype(jnp.bfloat16).reshape(quartered)
    fresh_v = project(spatial_in, spatial_qkv[2]).astype(jnp.bfloat16).reshape(quartered)
    stale_k = stale_kv[:, :width_win].reshape(quartered)
    stale_v = stale_kv[:, width_win:].reshape(quartered)

    def one_frame(inputs):
        frame_q, frame_k, frame_v, old_k, old_v = inputs
        results = []
        for quarter in range(4):
            key_rows = jnp.concatenate([frame_k[source] if source == quarter else old_k[source] for source in range(4)], axis=0)
            value_rows = jnp.concatenate([frame_v[source] if source == quarter else old_v[source] for source in range(4)], axis=0)
            results.append(spatial_attend(frame_q[quarter], key_rows, value_rows))
        return jnp.stack(results)
    spatial_mixed = lax.map(one_frame, (fresh_q, fresh_k, fresh_v, stale_k, stale_v)).reshape(TOKENS, width_win)
    after_spatial = tokens_wide + modulation[2] * project(spatial_mixed, spatial_out)
    positions = sinusoid(frame_order, D)
    temporal_in = normalize(after_spatial).reshape(FRAMES, FRAME_TOK, D) * (1.0 + modulation[4]) + modulation[3] + positions[:, None, :]
    temporal_in = temporal_in.astype(jnp.bfloat16).reshape(TOKENS, D)
    framed = (FRAMES, FRAME_TOK, width_win)
    temporal_q = project(temporal_in, temporal_qkv[0]).astype(jnp.bfloat16).reshape(framed)
    temporal_k = project(temporal_in, temporal_qkv[1]).astype(jnp.bfloat16).reshape(framed)
    temporal_v = project(temporal_in, temporal_qkv[2]).astype(jnp.bfloat16).reshape(framed)
    temporal_mixed = temporal_attend(temporal_q, temporal_k, temporal_v).reshape(TOKENS, width_win)
    return after_spatial + modulation[5] * project(temporal_mixed, temporal_out)
```

```python
import functools
import math

import jax
import jax.numpy as jnp
from jax import lax
from jax.experimental import pallas as pl
from jax.experimental.pallas import tpu as pltpu
from jax.sharding import PartitionSpec as P

HEADS = 16
LANES = 128
QUERY_ROWS = 128
PAIR_GROUPS = ((0, 1), (2,), (3,))
HALVES = 2

epsilon = 1e-06
bf16 = jnp.bfloat16
f32 = jnp.float32
NT = (((1,), (1,)), ((), ()))


def permute(value, target):
    count = lax.axis_size("patch")
    return lax.ppermute(value, "patch", [(source, target(source)) for source in range(count)])


def normalize(activations):
    row_mean = jnp.mean(activations, axis=-1, keepdims=True)
    centered = activations - row_mean
    variance = jnp.mean(centered * centered, axis=-1, keepdims=True)
    return centered * lax.rsqrt(variance + epsilon)


def sinusoid(position, feature_width):
    half_width = feature_width // 2
    frequencies = jnp.exp(
        -math.log(10000.0) * jnp.arange(half_width, dtype=jnp.float32) / half_width
    )
    angles = jnp.asarray(position).astype(jnp.float32)[..., None] * frequencies
    return jnp.concatenate([jnp.sin(angles), jnp.cos(angles)], axis=-1)


def column_mask(first, width, dtype):
    column = lax.broadcasted_iota(jnp.int32, (1, 2 * LANES), 1)
    inside = jnp.logical_and(column >= first, column < first + width)
    return jnp.where(inside, 1.0, 0.0).astype(dtype)


def softmax_scale(head_dim):
    return math.log2(math.e) * head_dim ** (-0.5)


def vmem_specs(count):
    return [pl.BlockSpec(memory_space=pltpu.VMEM) for _ in range(count)]


def pair_plan(width, head_dim):
    plan = []
    for first in range(0, width, 2 * head_dim):
        key_tile = first // LANES
        value_tile = (width + first) // LANES
        plan.append(
            (key_tile, first - key_tile * LANES, value_tile, width + first - value_tile * LANES)
        )
    return plan


def group_tiles(width, head_dim):
    plan = pair_plan(width, head_dim)
    seen, groups = set(), []
    for group in PAIR_GROUPS:
        need = []
        for pair in group:
            key_tile, _, value_tile, _ = plan[pair]
            need += [key_tile, key_tile + 1, value_tile, value_tile + 1]
        fresh = sorted(set(need) - seen)
        seen |= set(fresh)
        groups.append(tuple(fresh))
    return groups


def spatial_kernel(*refs, group, frames, head_dim, width, tiles, last):
    plan = pair_plan(width, head_dim)
    count = len(tiles)
    position = 0
    query_ref, own_ref, peer_ref = refs[:3]
    near_refs = refs[3 : 3 + count]
    far_refs = refs[3 + count : 3 + 2 * count]
    position = 3 + 2 * count
    first = group[0] == 0
    carry_ref = None
    if not first:
        carry_ref = refs[position]
        position += 1
    out_refs = refs[position : position + frames]
    carry_out = None if last else refs[position + frames]

    where = {tile: (c, j) for c, chunk in enumerate(tiles) for j, tile in enumerate(chunk)}

    def from_chunks(chunk_refs):
        def load(tile):
            chunk, at = where[tile]
            return chunk_refs[chunk][:, at * LANES : (at + 1) * LANES]

        return load

    def from_whole(ref):
        return lambda tile: ref[:, tile * LANES : (tile + 1) * LANES]

    blocks = [from_whole(own_ref), from_whole(peer_ref), from_chunks(near_refs), from_chunks(far_refs)]
    rows = query_ref.shape[0]
    scale = softmax_scale(head_dim)
    piece = rows // frames

    def two(block, tile):
        return jnp.concatenate([block(tile), block(tile + 1)], axis=1)

    def scores_of(pair, chunk):
        key_tile, key_lane, _, _ = plan[pair]
        window = query_ref[
            chunk * QUERY_ROWS : (chunk + 1) * QUERY_ROWS, key_tile * LANES : (key_tile + 2) * LANES
        ]
        stacked = jnp.concatenate(
            [
                window * column_mask(key_lane, head_dim, bf16),
                window * column_mask(key_lane + head_dim, head_dim, bf16),
            ],
            axis=0,
        )
        return [
            lax.dot_general(stacked, two(block, key_tile), NT, preferred_element_type=f32)
            for block in blocks
        ]

    def mix(pair, scores):
        _, key_lane, value_tile, value_lane = plan[pair]
        top = functools.reduce(jnp.maximum, [jnp.max(s, axis=-1, keepdims=True) for s in scores])
        top = top * scale
        weights = [jnp.exp2(s * scale - top) for s in scores]
        total = functools.reduce(jnp.add, [jnp.sum(w, axis=-1, keepdims=True) for w in weights])
        mixed = functools.reduce(
            jnp.add,
            [
                jnp.dot(w.astype(bf16), two(block, value_tile), preferred_element_type=f32)
                for w, block in zip(weights, blocks)
            ],
        )
        mixed = mixed / total
        joined = mixed[:QUERY_ROWS] * column_mask(value_lane, head_dim, f32) + mixed[
            QUERY_ROWS:
        ] * column_mask(value_lane + head_dim, head_dim, f32)
        return pltpu.roll(joined, (key_lane - value_lane) % (2 * LANES), 1)

    chunks = rows // QUERY_ROWS
    tasks = [(chunk, pair) for chunk in range(chunks) for pair in group]
    pending = scores_of(tasks[0][1], tasks[0][0])
    first_tile = plan[group[0]][0]
    parts = {}
    for index, (chunk, pair) in enumerate(tasks):
        scores = pending
        if index + 1 < len(tasks):
            pending = scores_of(tasks[index + 1][1], tasks[index + 1][0])
        joined = mix(pair, scores)
        tile = plan[pair][0]
        for side in range(2):
            half = joined[:, side * LANES : (side + 1) * LANES]
            parts[tile + side] = parts[tile + side] + half if tile + side in parts else half
        if pair != group[-1]:
            continue
        at = chunk * QUERY_ROWS
        if carry_ref is not None:
            parts[first_tile] = parts[first_tile] + carry_ref[at : at + QUERY_ROWS, :].astype(f32)
        done = sorted(parts)
        if carry_out is not None:
            carry_out[at : at + QUERY_ROWS, :] = parts[done[-1]].astype(bf16)
            done = done[:-1]
        values = jnp.concatenate([parts[tile] for tile in done], axis=1).astype(bf16)
        width_out = out_refs[0].shape[1]
        for sub in range(QUERY_ROWS // piece):
            out_refs[at // piece + sub][...] = values[sub * piece : (sub + 1) * piece, :width_out]
        parts = {}


def spatial_group(number, query, own_kv, peer_kv, near, far, carry, frames, head_dim, width):
    group = PAIR_GROUPS[number]
    last = number == len(PAIR_GROUPS) - 1
    plan = pair_plan(width, head_dim)
    tiles = tuple(group_tiles(width, head_dim)[: number + 1])
    rows = query.shape[0]
    first_column = plan[group[0]][0] * LANES
    end_column = width if last else (plan[group[-1]][0] + 1) * LANES
    columns = end_column - first_column
    out_shape = [jax.ShapeDtypeStruct((rows // frames, columns), bf16) for _ in range(frames)]
    if not last:
        out_shape.append(jax.ShapeDtypeStruct((rows, LANES), bf16))
    operands = [query, own_kv, peer_kv, *near[: number + 1], *far[: number + 1]]
    if carry is not None:
        operands.append(carry)
    keys = 4 * rows
    results = pl.pallas_call(
        functools.partial(
            spatial_kernel,
            group=group,
            frames=frames,
            head_dim=head_dim,
            width=width,
            tiles=tiles,
            last=last,
        ),
        out_shape=out_shape,
        in_specs=vmem_specs(len(operands)),
        out_specs=vmem_specs(len(out_shape)),
        cost_estimate=pl.CostEstimate(
            flops=len(group) * 2 * rows * keys * 256 * 4,
            bytes_accessed=4 * rows * 512 * 2,
            transcendentals=len(group) * 2 * rows * keys,
        ),
        name=f"spatial_{number}",
    )(*operands)
    return list(results[:frames]), (None if last else results[frames])


def temporal_kernel(*refs, frames, head_dim, groups):
    tokens_refs = refs[:frames]
    mixed_refs = refs[frames : frames + frames * groups]
    position = frames + frames * groups
    out_weight, qkv_weight, modulation_ref, place_ref = refs[position : position + 4]
    out_refs = refs[position + 4 : position + 4 + frames]
    query_ref, key_ref, value_ref = refs[position + 4 + frames :]
    piece, feature_width = tokens_refs[0].shape
    width = out_weight.shape[0]
    rows = frames * piece

    tokens_wide = jnp.concatenate([ref[...] for ref in tokens_refs], axis=0).astype(f32)
    mixed = jnp.concatenate(
        [
            jnp.concatenate([mixed_refs[frame * groups + g][...] for g in range(groups)], axis=1)
            for frame in range(frames)
        ],
        axis=0,
    )
    after = tokens_wide + modulation_ref[2:3, :] * jnp.dot(
        mixed, out_weight[...], preferred_element_type=f32
    )
    normal = normalize(after) * (1.0 + modulation_ref[4:5, :]) + modulation_ref[3:4, :]
    inputs = jnp.concatenate(
        [
            (normal[frame * piece : (frame + 1) * piece] + place_ref[frame : frame + 1, :]).astype(bf16)
            for frame in range(frames)
        ],
        axis=0,
    )
    padded = query_ref.shape[1]
    for number, ref in enumerate((query_ref, key_ref, value_ref)):
        ref[:, :width] = jnp.dot(
            inputs, qkv_weight[number], preferred_element_type=f32
        ).astype(bf16)
        ref[:, width:] = jnp.zeros((rows, padded - width), bf16)

    scale = softmax_scale(head_dim)
    step = max(16, min(piece, LANES // frames))
    block = frames * step
    row_at = lax.broadcasted_iota(jnp.int32, (2 * block, block), 0) % step
    column_at = lax.broadcasted_iota(jnp.int32, (2 * block, block), 1) % step
    same = row_at == column_at
    plan = pair_plan(width, head_dim)

    for start in range(0, piece, step):

        def window(ref, tile):
            return jnp.concatenate(
                [
                    ref[
                        frame * piece + start : frame * piece + start + step,
                        tile * LANES : (tile + 2) * LANES,
                    ]
                    for frame in range(frames)
                ],
                axis=0,
            )

        parts = {}
        for tile, lane, _, _ in plan:
            queries = window(query_ref, tile)
            stacked = jnp.concatenate(
                [
                    queries * column_mask(lane, head_dim, bf16),
                    queries * column_mask(lane + head_dim, head_dim, bf16),
                ],
                axis=0,
            )
            scores = lax.dot_general(stacked, window(key_ref, tile), NT, preferred_element_type=f32)
            scores = jnp.where(same, scores * scale, -jnp.inf)
            weights = jnp.exp2(scores - jnp.max(scores, axis=-1, keepdims=True))
            weights = (weights / jnp.sum(weights, axis=-1, keepdims=True)).astype(bf16)
            mixed_pair = jnp.dot(weights, window(value_ref, tile), preferred_element_type=f32)
            joined = mixed_pair[:block] * column_mask(lane, head_dim, f32) + mixed_pair[
                block:
            ] * column_mask(lane + head_dim, head_dim, f32)
            for side in range(2):
                half = joined[:, side * LANES : (side + 1) * LANES]
                parts[tile + side] = parts[tile + side] + half if tile + side in parts else half
        values = jnp.concatenate([parts[tile] for tile in sorted(parts)], axis=1).astype(bf16)
        for frame in range(frames):
            out_refs[frame][start : start + step, :] = values[
                frame * step : (frame + 1) * step, :width
            ]


def temporal(tokens, mixed, spatial_out, temporal_qkv, modulation, places, head_dim):
    frames, groups = len(tokens), len(mixed[0])
    piece = tokens[0].shape[0]
    width, feature_width = spatial_out.shape
    padded = -(-width // LANES) * LANES
    operands = [*tokens, *[part for frame in mixed for part in frame]]
    operands += [spatial_out, temporal_qkv, modulation, places]
    rows = frames * piece
    return pl.pallas_call(
        functools.partial(temporal_kernel, frames=frames, head_dim=head_dim, groups=groups),
        out_shape=[jax.ShapeDtypeStruct((piece, width), bf16) for _ in range(frames)],
        in_specs=vmem_specs(len(operands)),
        out_specs=vmem_specs(frames),
        scratch_shapes=[pltpu.VMEM((rows, padded), bf16) for _ in range(3)],
        cost_estimate=pl.CostEstimate(
            flops=2 * rows * feature_width * width * 8,
            bytes_accessed=rows * feature_width * 8,
            transcendentals=rows * 128 * 8,
        ),
        name="temporal",
    )(*operands)


def output_kernel(slot_ref, after_ref, weight_ref, modulation_ref, *refs, frames, halves):
    parts, out_ref = refs[:-1], refs[-1]
    for frame in range(frames):

        @pl.when(pl.program_id(0) == frame)
        def _():
            mixed = jnp.concatenate([parts[frame * halves + h][...] for h in range(halves)], axis=0)
            out_ref[...] = after_ref[...] + modulation_ref[5:6, :] * jnp.dot(
                mixed, weight_ref[...], preferred_element_type=f32
            )


def output(slot, after, weight, modulation, parts, frames):
    rows, feature_width = after.shape
    piece = rows // frames
    halves = len(parts[0])
    flat = [part for frame in parts for part in frame]

    def whole(array):
        return pl.BlockSpec(array.shape, lambda s, slot_ref: (0,) * array.ndim)

    return pl.pallas_call(
        functools.partial(output_kernel, frames=frames, halves=halves),
        out_shape=jax.ShapeDtypeStruct((rows, feature_width), f32),
        grid_spec=pltpu.PrefetchScalarGridSpec(
            num_scalar_prefetch=1,
            grid=(frames,),
            in_specs=[
                pl.BlockSpec((piece, feature_width), lambda s, slot_ref: (s, 0)),
                whole(weight),
                whole(modulation),
                *[whole(part) for part in flat],
            ],
            out_specs=pl.BlockSpec(
                (piece, feature_width), lambda s, slot_ref: ((s + slot_ref[0]) % frames, 0)
            ),
        ),
        name="block_output",
    )(slot, after, weight, modulation, *flat)


def per_device(
    tokens,
    stale_kv,
    mod_table,
    mod_mix,
    timestep,
    frame_order,
    spatial_qkv,
    spatial_out,
    temporal_qkv,
    temporal_out,
):
    devices = lax.axis_size("patch")
    frames = devices // 4
    slot = lax.axis_index("patch") // 4
    rows, feature_width = tokens.shape
    width = spatial_out.shape[0]
    head_dim = feature_width // HEADS
    piece = rows // frames
    padded = -(-width // LANES) * LANES

    def other_core(device):
        return device ^ 1

    def other_chip(device):
        return device ^ 2

    def ahead(steps):
        return lambda device: (device + 4 * steps) % devices

    near, far = [], []
    for tiles in group_tiles(width, head_dim):
        chunk = jnp.concatenate(
            [stale_kv[:, tile * LANES : (tile + 1) * LANES] for tile in tiles], axis=1
        )
        near.append(permute(chunk, other_chip))
        far.append(permute(near[-1], other_core))
    peer_kv = permute(stale_kv, other_core)

    pieces = [
        lax.dynamic_slice(tokens, ((slot + s) % frames * piece, 0), (piece, feature_width))
        for s in range(frames)
    ]
    there = [pieces[0]] + [permute(pieces[s], ahead(s)) for s in range(1, frames)]

    modulation = mod_table + mod_mix * sinusoid(timestep[0], feature_width)[None, :]
    sources = (slot - jnp.arange(frames)) % frames
    places = sinusoid(frame_order[sources], feature_width)

    tokens_wide = jnp.concatenate(pieces, axis=0).astype(f32)
    spatial_in = (normalize(tokens_wide) * (1.0 + modulation[1]) + modulation[0]).astype(bf16)
    fresh = [
        jnp.dot(spatial_in, spatial_qkv[j], preferred_element_type=f32).astype(bf16) for j in range(3)
    ]
    query = jnp.pad(fresh[0], ((0, 0), (0, padded - width)))
    own_kv = jnp.concatenate([fresh[1], fresh[2]], axis=1)

    carry = None
    local = [[] for _ in range(frames)]
    sent = [[] for _ in range(frames)]
    for number in range(len(PAIR_GROUPS)):
        outs, carry = spatial_group(
            number, query, own_kv, peer_kv, near, far, carry, frames, head_dim, width
        )
        for s in range(frames):
            local[s].append(outs[s])
            sent[s].append(outs[s] if s == 0 else permute(outs[s], ahead(s)))

    half = piece // HALVES
    back = [[] for _ in range(frames)]
    for h in range(HALVES):
        cut = slice(h * half, (h + 1) * half)
        outs = temporal(
            [t[cut] for t in there],
            [[m[cut] for m in frame] for frame in sent],
            spatial_out,
            temporal_qkv,
            modulation,
            places,
            head_dim,
        )
        for s in range(frames):
            back[s].append(outs[s] if s == 0 else permute(outs[s], ahead(-s)))

    spatial_mixed = jnp.concatenate([jnp.concatenate(local[s], axis=1) for s in range(frames)], axis=0)
    after = tokens_wide + modulation[2] * jnp.dot(
        spatial_mixed, spatial_out, preferred_element_type=f32
    )
    return output(
        slot.astype(jnp.int32)[None], after, temporal_out, modulation, back, frames
    )


def solution(mesh):
    return jax.shard_map(
        per_device,
        mesh=mesh,
        in_specs=(
            P(("groups", "patch"), None),
            P(("groups", "patch"), None),
            P(),
            P(),
            P("groups"),
            P("groups"),
            P(),
            P(),
            P(),
            P(),
        ),
        out_specs=P(("groups", "patch"), None),
        check_vma=False,
    )
```

```python
import functools
import math

import jax
import jax.numpy as jnp
from jax import lax
from jax.experimental import pallas as pl
from jax.experimental.pallas import tpu as pltpu
from jax.sharding import PartitionSpec as P

HEADS = 16
LANES = 128
QUERY_ROWS = 128
PAIR_GROUPS = ((0, 1), (2,), (3,))
HALVES = 2


epsilon = 1e-06
bf16 = jnp.bfloat16
f32 = jnp.float32
NT = (((1,), (1,)), ((), ()))


def permute(value, target):
    count = lax.axis_size("patch")
    return lax.ppermute(value, "patch", [(source, target(source)) for source in range(count)])


def normalize(activations):
    row_mean = jnp.mean(activations, axis=-1, keepdims=True)
    centered = activations - row_mean
    variance = jnp.mean(centered * centered, axis=-1, keepdims=True)
    return centered * lax.rsqrt(variance + epsilon)


def sinusoid(position, feature_width):
    half_width = feature_width // 2
    frequencies = jnp.exp(
        -math.log(10000.0) * jnp.arange(half_width, dtype=jnp.float32) / half_width
    )
    angles = jnp.asarray(position).astype(jnp.float32)[..., None] * frequencies
    return jnp.concatenate([jnp.sin(angles), jnp.cos(angles)], axis=-1)


def column_mask(first, width, dtype):
    column = lax.broadcasted_iota(jnp.int32, (1, 2 * LANES), 1)
    inside = jnp.logical_and(column >= first, column < first + width)
    return jnp.where(inside, 1.0, 0.0).astype(dtype)


def softmax_scale(head_dim):
    return math.log2(math.e) * head_dim ** (-0.5)


def vmem_specs(count):
    return [pl.BlockSpec(memory_space=pltpu.VMEM) for _ in range(count)]


def on_chip_call(kernel, name, operands, shapes, flops, limit_mib, transcendentals=0, scratch=()):
    return pl.pallas_call(
        kernel,
        out_shape=[pltpu.VMEM(shape, dtype) for shape, dtype in shapes],
        in_specs=vmem_specs(len(operands)),
        out_specs=vmem_specs(len(shapes)),
        scratch_shapes=list(scratch),
        compiler_params=pltpu.CompilerParams(vmem_limit_bytes=limit_mib * 2**20),
        cost_estimate=pl.CostEstimate(
            flops=flops,
            bytes_accessed=sum(array.size * array.dtype.itemsize for array in operands),
            transcendentals=transcendentals,
        ),
        name=name,
    )(*[pltpu.with_memory_space_constraint(array, pltpu.VMEM) for array in operands])


def projection_kernel(*refs, frames, width):
    pieces = refs[:frames]
    weight_ref, modulation_ref, query_ref, kv_ref = refs[frames:]
    tokens = jnp.concatenate([ref[...] for ref in pieces], axis=0).astype(f32)
    inputs = normalize(tokens) * (1.0 + modulation_ref[1:2, :]) + modulation_ref[0:1, :]
    inputs = inputs.astype(bf16)
    padded = query_ref.shape[1]
    query_ref[...] = lax.dot_general(
        inputs, weight_ref[:padded, :], NT, preferred_element_type=f32
    ).astype(bf16)
    kv_ref[...] = lax.dot_general(
        inputs, weight_ref[width:, :], NT, preferred_element_type=f32
    ).astype(bf16)


def projections(pieces, weight, modulation, width):
    frames = len(pieces)
    piece, feature_width = pieces[0].shape
    padded = -(-width // LANES) * LANES
    rows = frames * piece
    return on_chip_call(
        functools.partial(projection_kernel, frames=frames, width=width),
        "projections",
        [*pieces, weight, modulation],
        [((rows, padded), bf16), ((rows, 2 * width), bf16)],
        2 * rows * feature_width * 3 * width,
        16,
    )


def pair_plan(width, head_dim):
    plan = []
    for first in range(0, width, 2 * head_dim):
        key_tile = first // LANES
        value_tile = (width + first) // LANES
        plan.append(
            (key_tile, first - key_tile * LANES, value_tile, width + first - value_tile * LANES)
        )
    return plan


def group_tiles(width, head_dim):
    plan = pair_plan(width, head_dim)
    seen, groups = set(), []
    for group in PAIR_GROUPS:
        need = []
        for pair in group:
            key_tile, _, value_tile, _ = plan[pair]
            need += [key_tile, key_tile + 1, value_tile, value_tile + 1]
        fresh = sorted(set(need) - seen)
        seen |= set(fresh)
        groups.append(tuple(fresh))
    return groups


def spatial_kernel(*refs, group, frames, head_dim, width, tiles, last):
    plan = pair_plan(width, head_dim)
    count = len(tiles)
    position = 0
    query_ref, own_ref, peer_ref = refs[:3]
    near_refs = refs[3 : 3 + count]
    far_refs = refs[3 + count : 3 + 2 * count]
    position = 3 + 2 * count
    first = group[0] == 0
    carry_ref = None
    if not first:
        carry_ref = refs[position]
        position += 1
    out_refs = refs[position : position + frames]
    carry_out = None if last else refs[position + frames]

    where = {tile: (c, j) for c, chunk in enumerate(tiles) for j, tile in enumerate(chunk)}

    def from_chunks(chunk_refs):
        def load(tile):
            chunk, at = where[tile]
            return chunk_refs[chunk][:, at * LANES : (at + 1) * LANES]

        return load

    def from_whole(ref):
        return lambda tile: ref[:, tile * LANES : (tile + 1) * LANES]

    blocks = [from_whole(own_ref), from_whole(peer_ref), from_chunks(near_refs), from_chunks(far_refs)]
    rows = query_ref.shape[0]
    scale = softmax_scale(head_dim)
    piece = rows // frames

    def two(block, tile):
        return jnp.concatenate([block(tile), block(tile + 1)], axis=1)

    def scores_of(pair, chunk):
        key_tile, key_lane, _, _ = plan[pair]
        window = query_ref[
            chunk * QUERY_ROWS : (chunk + 1) * QUERY_ROWS, key_tile * LANES : (key_tile + 2) * LANES
        ]
        stacked = jnp.concatenate(
            [
                window * column_mask(key_lane, head_dim, bf16),
                window * column_mask(key_lane + head_dim, head_dim, bf16),
            ],
            axis=0,
        )
        return [
            lax.dot_general(stacked, two(block, key_tile), NT, preferred_element_type=f32)
            for block in blocks
        ]

    def mix(pair, scores):
        _, key_lane, value_tile, value_lane = plan[pair]
        top = functools.reduce(jnp.maximum, [jnp.max(s, axis=-1, keepdims=True) for s in scores])
        top = top * scale
        weights = [jnp.exp2(s * scale - top) for s in scores]
        total = functools.reduce(jnp.add, [jnp.sum(w, axis=-1, keepdims=True) for w in weights])
        mixed = functools.reduce(
            jnp.add,
            [
                jnp.dot(w.astype(bf16), two(block, value_tile), preferred_element_type=f32)
                for w, block in zip(weights, blocks)
            ],
        )
        mixed = mixed / total
        joined = mixed[:QUERY_ROWS] * column_mask(value_lane, head_dim, f32) + mixed[
            QUERY_ROWS:
        ] * column_mask(value_lane + head_dim, head_dim, f32)
        return pltpu.roll(joined, (key_lane - value_lane) % (2 * LANES), 1)

    chunks = rows // QUERY_ROWS
    tasks = [(chunk, pair) for chunk in range(chunks) for pair in group]
    pending = scores_of(tasks[0][1], tasks[0][0])
    first_tile = plan[group[0]][0]
    parts = {}
    for index, (chunk, pair) in enumerate(tasks):
        scores = pending
        if index + 1 < len(tasks):
            pending = scores_of(tasks[index + 1][1], tasks[index + 1][0])
        joined = mix(pair, scores)
        tile = plan[pair][0]
        for side in range(2):
            half = joined[:, side * LANES : (side + 1) * LANES]
            parts[tile + side] = parts[tile + side] + half if tile + side in parts else half
        if pair != group[-1]:
            continue
        at = chunk * QUERY_ROWS
        if carry_ref is not None:
            parts[first_tile] = parts[first_tile] + carry_ref[at : at + QUERY_ROWS, :].astype(f32)
        done = sorted(parts)
        if carry_out is not None:
            carry_out[at : at + QUERY_ROWS, :] = parts[done[-1]].astype(bf16)
            done = done[:-1]
        values = jnp.concatenate([parts[tile] for tile in done], axis=1).astype(bf16)
        width_out = out_refs[0].shape[1]
        for sub in range(QUERY_ROWS // piece):
            out_refs[at // piece + sub][...] = values[sub * piece : (sub + 1) * piece, :width_out]
        parts = {}


def spatial_group(number, query, own_kv, peer_kv, near, far, carry, frames, head_dim, width):
    group = PAIR_GROUPS[number]
    last = number == len(PAIR_GROUPS) - 1
    plan = pair_plan(width, head_dim)
    tiles = tuple(group_tiles(width, head_dim)[: number + 1])
    rows = query.shape[0]
    first_column = plan[group[0]][0] * LANES
    end_column = width if last else (plan[group[-1]][0] + 1) * LANES
    columns = end_column - first_column
    shapes = [((rows // frames, columns), bf16) for _ in range(frames)]
    if not last:
        shapes.append(((rows, LANES), bf16))
    operands = [query, own_kv, peer_kv, *near[: number + 1], *far[: number + 1]]
    if carry is not None:
        operands.append(carry)
    keys = 4 * rows
    results = on_chip_call(
        functools.partial(
            spatial_kernel,
            group=group,
            frames=frames,
            head_dim=head_dim,
            width=width,
            tiles=tiles,
            last=last,
        ),
        f"spatial_{number}",
        operands,
        shapes,
        len(group) * 2 * rows * keys * 256 * 4,
        24,
        len(group) * 2 * rows * keys,
    )
    return list(results[:frames]), (None if last else results[frames])


def temporal_kernel(*refs, frames, head_dim, groups, first, piece):
    tokens_refs = refs[:frames]
    mixed_refs = refs[frames : frames + frames * groups]
    position = frames + frames * groups
    out_weight, qkv_weight, modulation_ref, place_ref = refs[position : position + 4]
    out_refs = refs[position + 4 : position + 4 + frames]
    query_ref, kv_ref = refs[position + 4 + frames :]
    width = out_weight.shape[0]
    cut = slice(first, first + piece)

    tokens_wide = jnp.concatenate([ref[cut, :] for ref in tokens_refs], axis=0).astype(f32)
    mixed = jnp.concatenate(
        [
            jnp.concatenate([mixed_refs[frame * groups + g][cut, :] for g in range(groups)], axis=1)
            for frame in range(frames)
        ],
        axis=0,
    )
    after = tokens_wide + modulation_ref[2:3, :] * jnp.dot(
        mixed, out_weight[...], preferred_element_type=f32
    )
    normal = normalize(after) * (1.0 + modulation_ref[4:5, :]) + modulation_ref[3:4, :]
    inputs = jnp.concatenate(
        [
            (normal[frame * piece : (frame + 1) * piece] + place_ref[frame : frame + 1, :]).astype(bf16)
            for frame in range(frames)
        ],
        axis=0,
    )
    query_ref[...] = lax.dot_general(
        inputs, qkv_weight[: query_ref.shape[1], :], NT, preferred_element_type=f32
    ).astype(bf16)
    kv_ref[...] = lax.dot_general(
        inputs, qkv_weight[width:, :], NT, preferred_element_type=f32
    ).astype(bf16)

    scale = softmax_scale(head_dim)
    step = max(16, min(piece, LANES // frames))
    block = frames * step
    row_at = lax.broadcasted_iota(jnp.int32, (2 * block, block), 0) % step
    column_at = lax.broadcasted_iota(jnp.int32, (2 * block, block), 1) % step
    same = row_at == column_at
    plan = pair_plan(width, head_dim)

    for start in range(0, piece, step):

        def window(ref, tile):
            return jnp.concatenate(
                [
                    ref[
                        frame * piece + start : frame * piece + start + step,
                        tile * LANES : (tile + 2) * LANES,
                    ]
                    for frame in range(frames)
                ],
                axis=0,
            )

        parts = {}
        for tile, lane, value_tile, value_lane in plan:
            queries = window(query_ref, tile)
            stacked = jnp.concatenate(
                [
                    queries * column_mask(lane, head_dim, bf16),
                    queries * column_mask(lane + head_dim, head_dim, bf16),
                ],
                axis=0,
            )
            scores = lax.dot_general(stacked, window(kv_ref, tile), NT, preferred_element_type=f32)
            scores = jnp.where(same, scores * scale, -jnp.inf)
            weights = jnp.exp2(scores - jnp.max(scores, axis=-1, keepdims=True))
            weights = (weights / jnp.sum(weights, axis=-1, keepdims=True)).astype(bf16)
            mixed_pair = jnp.dot(weights, window(kv_ref, value_tile), preferred_element_type=f32)
            joined = mixed_pair[:block] * column_mask(value_lane, head_dim, f32) + mixed_pair[
                block:
            ] * column_mask(value_lane + head_dim, head_dim, f32)
            joined = pltpu.roll(joined, (lane - value_lane) % (2 * LANES), 1)
            for side in range(2):
                half = joined[:, side * LANES : (side + 1) * LANES]
                parts[tile + side] = parts[tile + side] + half if tile + side in parts else half
        values = jnp.concatenate([parts[tile] for tile in sorted(parts)], axis=1).astype(bf16)
        for frame in range(frames):
            out_refs[frame][start : start + step, :] = values[
                frame * step : (frame + 1) * step, :width
            ]


def temporal(tokens, mixed, spatial_out, temporal_qkv, modulation, places, head_dim, first, piece):
    frames, groups = len(tokens), len(mixed[0])
    width, feature_width = spatial_out.shape
    padded = -(-width // LANES) * LANES
    operands = [*tokens, *[part for frame in mixed for part in frame]]
    operands += [spatial_out, temporal_qkv, modulation, places]
    rows = frames * piece
    return on_chip_call(
        functools.partial(
            temporal_kernel,
            frames=frames,
            head_dim=head_dim,
            groups=groups,
            first=first,
            piece=piece,
        ),
        "temporal",
        operands,
        [((piece, width), bf16) for _ in range(frames)],
        2 * rows * feature_width * width * 8,
        16,
        rows * 128 * 8,
        [pltpu.VMEM((rows, padded), bf16), pltpu.VMEM((rows, 2 * width), bf16)],
    )


def after_kernel(*refs, frames, groups):
    tokens_refs = refs[:frames]
    mixed_refs = refs[frames : frames + frames * groups]
    weight_ref, modulation_ref, out_ref = refs[frames + frames * groups :]
    tokens_wide = jnp.concatenate([ref[...] for ref in tokens_refs], axis=0).astype(f32)
    mixed = jnp.concatenate(
        [
            jnp.concatenate([mixed_refs[frame * groups + g][...] for g in range(groups)], axis=1)
            for frame in range(frames)
        ],
        axis=0,
    )
    out_ref[...] = tokens_wide + modulation_ref[2:3, :] * jnp.dot(
        mixed, weight_ref[...], preferred_element_type=f32
    )


def after_spatial(tokens, mixed, weight, modulation):
    frames, groups = len(tokens), len(mixed[0])
    width, feature_width = weight.shape
    rows = frames * tokens[0].shape[0]
    return on_chip_call(
        functools.partial(after_kernel, frames=frames, groups=groups),
        "after_spatial",
        [*tokens, *[part for frame in mixed for part in frame], weight, modulation],
        [((rows, feature_width), f32)],
        2 * rows * feature_width * width,
        16,
    )[0]


def output_kernel(slot_ref, after_ref, weight_ref, modulation_ref, *refs, frames, halves):
    parts, (out_ref, stage_ref, sems) = refs[: frames * halves], refs[frames * halves :]
    piece = after_ref.shape[0] // frames
    copies = []
    for frame in range(frames):
        cut = slice(frame * piece, (frame + 1) * piece)
        mixed = jnp.concatenate([parts[frame * halves + h][...] for h in range(halves)], axis=0)
        stage_ref[cut, :] = after_ref[cut, :] + modulation_ref[5:6, :] * jnp.dot(
            mixed, weight_ref[...], preferred_element_type=f32
        )
        row = (frame + slot_ref[0]) % frames * piece
        copies.append(
            pltpu.make_async_copy(
                stage_ref.at[cut, :], out_ref.at[pl.ds(row, piece), :], sems.at[frame]
            )
        )
        copies[-1].start()
    for copy in copies:
        copy.wait()


def output(slot, after, weight, modulation, parts, frames):
    rows, feature_width = after.shape
    halves = len(parts[0])
    operands = [after, weight, modulation, *[part for frame in parts for part in frame]]
    return pl.pallas_call(
        functools.partial(output_kernel, frames=frames, halves=halves),
        out_shape=jax.ShapeDtypeStruct((rows, feature_width), f32),
        in_specs=[pl.BlockSpec(memory_space=pltpu.SMEM), *vmem_specs(len(operands))],
        out_specs=pl.BlockSpec(memory_space=pltpu.HBM),
        scratch_shapes=[
            pltpu.VMEM((rows, feature_width), f32),
            pltpu.SemaphoreType.DMA((frames,)),
        ],
        compiler_params=pltpu.CompilerParams(vmem_limit_bytes=16 * 2**20),
        name="block_output",
    )(slot, *[pltpu.with_memory_space_constraint(array, pltpu.VMEM) for array in operands])


def per_device(
    tokens,
    stale_kv,
    mod_table,
    mod_mix,
    timestep,
    frame_order,
    spatial_qkv,
    spatial_out,
    temporal_qkv,
    temporal_out,
):
    devices = lax.axis_size("patch")
    frames = devices // 4
    slot = lax.axis_index("patch") // 4
    rows, feature_width = tokens.shape
    width = spatial_out.shape[0]
    head_dim = feature_width // HEADS
    piece = rows // frames

    def other_core(device):
        return device ^ 1

    def other_chip(device):
        return device ^ 2

    def ahead(steps):
        return lambda device: (device + 4 * steps) % devices

    near, far = [], []
    for tiles in group_tiles(width, head_dim):
        chunk = jnp.concatenate(
            [stale_kv[:, tile * LANES : (tile + 1) * LANES] for tile in tiles], axis=1
        )
        near.append(permute(chunk, other_chip))
        far.append(permute(near[-1], other_core))
    peer_kv = permute(stale_kv, other_core)

    pieces = [
        lax.dynamic_slice(tokens, ((slot + s) % frames * piece, 0), (piece, feature_width))
        for s in range(frames)
    ]
    there = [pieces[0]] + [permute(pieces[s], ahead(s)) for s in range(1, frames)]

    modulation = mod_table + mod_mix * sinusoid(timestep[0], feature_width)[None, :]
    sources = (slot - jnp.arange(frames)) % frames
    places = sinusoid(frame_order[sources], feature_width)

    query, own_kv = projections(
        pieces,
        jnp.swapaxes(spatial_qkv, 1, 2).reshape(3 * width, feature_width),
        modulation,
        width,
    )

    carry = None
    local = [[] for _ in range(frames)]
    sent = [[] for _ in range(frames)]
    for number in range(len(PAIR_GROUPS)):
        outs, carry = spatial_group(
            number, query, own_kv, peer_kv, near, far, carry, frames, head_dim, width
        )
        for s in range(frames):
            local[s].append(outs[s])
            sent[s].append(outs[s] if s == 0 else permute(outs[s], ahead(s)))

    half = piece // HALVES
    back = [[] for _ in range(frames)]
    temporal_weight = jnp.swapaxes(temporal_qkv, 1, 2).reshape(3 * width, feature_width)
    for h in range(HALVES):
        outs = temporal(
            there, sent, spatial_out, temporal_weight, modulation, places, head_dim, h * half, half
        )
        for s in range(frames):
            back[s].append(outs[s] if s == 0 else permute(outs[s], ahead(-s)))

    after = after_spatial(pieces, local, spatial_out, modulation)
    return output(
        slot.astype(jnp.int32)[None], after, temporal_out, modulation, back, frames
    )


def solution(mesh):
    return jax.shard_map(
        per_device,
        mesh=mesh,
        in_specs=(
            P(("groups", "patch"), None),
            P(("groups", "patch"), None),
            P(),
            P(),
            P("groups"),
            P("groups"),
            P(),
            P(),
            P(),
            P(),
        ),
        out_specs=P(("groups", "patch"), None),
        check_vma=False,
    )
```

```python
import functools
import math

import jax
import jax.numpy as jnp
from jax import lax
from jax.experimental import pallas as pl
from jax.experimental.pallas import tpu as pltpu
from jax.sharding import PartitionSpec as P


HEADS = 16
LANES = 128
QUERY_ROWS = 128
PAIR_GROUPS = ((0,), (1,), (2,), (3,))
EMIT = (False, False, True, True)
HALVES = 2


epsilon = 1e-06
bf16 = jnp.bfloat16
f32 = jnp.float32
NT = (((1,), (1,)), ((), ()))


def permute(value, target):
    count = lax.axis_size("patch")
    return lax.ppermute(value, "patch", [(source, target(source)) for source in range(count)])


def partner_slot(slot, step, frames):
    if frames & (frames - 1) == 0:
        return slot ^ step
    return (slot + step) % frames


def source_slot(slot, step, frames):
    if frames & (frames - 1) == 0:
        return slot ^ step
    return (slot - step) % frames


def normalize(activations):
    row_mean = jnp.mean(activations, axis=-1, keepdims=True)
    centered = activations - row_mean
    variance = jnp.mean(centered * centered, axis=-1, keepdims=True)
    return centered * lax.rsqrt(variance + epsilon)


def sinusoid(position, feature_width):
    half_width = feature_width // 2
    frequencies = jnp.exp(
        -math.log(10000.0) * jnp.arange(half_width, dtype=jnp.float32) / half_width
    )
    angles = jnp.asarray(position).astype(jnp.float32)[..., None] * frequencies
    return jnp.concatenate([jnp.sin(angles), jnp.cos(angles)], axis=-1)


def column_mask(first, width, dtype):
    column = lax.broadcasted_iota(jnp.int32, (1, 2 * LANES), 1)
    inside = jnp.logical_and(column >= first, column < first + width)
    return jnp.where(inside, 1.0, 0.0).astype(dtype)


def softmax_scale(head_dim):
    return math.log2(math.e) * head_dim ** (-0.5)


def vmem_specs(count):
    return [pl.BlockSpec(memory_space=pltpu.VMEM) for _ in range(count)]


def on_chip_call(kernel, operands, shapes, flops, limit_mib, transcendentals=0, scratch=()):
    operands = [pltpu.with_memory_space_constraint(array, pltpu.VMEM) for array in operands]
    return pl.pallas_call(
        kernel,
        out_shape=[pltpu.VMEM(shape, dtype) for shape, dtype in shapes],
        in_specs=vmem_specs(len(operands)),
        out_specs=vmem_specs(len(shapes)),
        scratch_shapes=list(scratch),
        compiler_params=pltpu.CompilerParams(vmem_limit_bytes=limit_mib * 2**20),
        cost_estimate=pl.CostEstimate(
            flops=flops,
            bytes_accessed=sum(array.size * array.dtype.itemsize for array in operands),
            transcendentals=transcendentals,
        ),
    )(*operands)


def chunk_kernel(kv_ref, *refs, tiles):
    out_refs, sems = refs[:-1], refs[-1]
    copies = []
    for chunk, ref in zip(tiles, out_refs):
        for at, tile in enumerate(chunk):
            copies.append(
                pltpu.make_async_copy(
                    kv_ref.at[:, tile * LANES : (tile + 1) * LANES],
                    ref.at[:, at * LANES : (at + 1) * LANES],
                    sems.at[len(copies)],
                )
            )
            copies[-1].start()
    for copy in copies:
        copy.wait()


def stage_chunks(stale_kv, tiles):
    rows = stale_kv.shape[0]
    return pl.pallas_call(
        functools.partial(chunk_kernel, tiles=tiles),
        out_shape=[pltpu.VMEM((rows, len(chunk) * LANES), bf16) for chunk in tiles],
        in_specs=[pl.BlockSpec(memory_space=pltpu.HBM)],
        out_specs=vmem_specs(len(tiles)),
        scratch_shapes=[pltpu.SemaphoreType.DMA((sum(len(chunk) for chunk in tiles),))],
        compiler_params=pltpu.CompilerParams(vmem_limit_bytes=4 * 2**20),
        name="chunks",
    )(stale_kv)


def piece_kernel(slot_ref, tokens_ref, *refs, frames):
    out_refs, sems = refs[:-1], refs[-1]
    piece = tokens_ref.shape[0] // frames
    copies = []
    for step in range(frames):
        row = partner_slot(slot_ref[0], step, frames) * piece
        copies.append(
            pltpu.make_async_copy(
                tokens_ref.at[pl.ds(row, piece), :], out_refs[step], sems.at[step]
            )
        )
        copies[-1].start()
    for copy in copies:
        copy.wait()


def stage_pieces(slot, tokens, frames):
    rows, feature_width = tokens.shape
    return pl.pallas_call(
        functools.partial(piece_kernel, frames=frames),
        out_shape=[pltpu.VMEM((rows // frames, feature_width), bf16) for _ in range(frames)],
        in_specs=[
            pl.BlockSpec(memory_space=pltpu.SMEM),
            pl.BlockSpec(memory_space=pltpu.HBM),
        ],
        out_specs=vmem_specs(frames),
        scratch_shapes=[pltpu.SemaphoreType.DMA((frames,))],
        compiler_params=pltpu.CompilerParams(vmem_limit_bytes=4 * 2**20),
        name="pieces",
    )(slot, tokens)


def projection_kernel(*refs, frames, width):
    pieces = refs[:frames]
    weight_ref, modulation_ref, query_ref, kv_ref = refs[frames:]
    tokens = jnp.concatenate([ref[...] for ref in pieces], axis=0).astype(f32)
    inputs = normalize(tokens) * (1.0 + modulation_ref[1:2, :]) + modulation_ref[0:1, :]
    inputs = inputs.astype(bf16)
    padded = query_ref.shape[1]
    query_ref[...] = lax.dot_general(
        inputs, weight_ref[:padded, :], NT, preferred_element_type=f32
    ).astype(bf16)
    kv_ref[...] = lax.dot_general(
        inputs, weight_ref[width:, :], NT, preferred_element_type=f32
    ).astype(bf16)


def projections(pieces, weight, modulation, width):
    frames = len(pieces)
    piece, feature_width = pieces[0].shape
    padded = -(-width // LANES) * LANES
    rows = frames * piece
    return on_chip_call(
        functools.partial(projection_kernel, frames=frames, width=width),
        [*pieces, weight, modulation],
        [((rows, padded), bf16), ((rows, 2 * width), bf16)],
        2 * rows * feature_width * 3 * width,
        16,
    )


def pair_plan(width, head_dim):
    plan = []
    for first in range(0, width, 2 * head_dim):
        key_tile = first // LANES
        value_tile = (width + first) // LANES
        plan.append(
            (key_tile, first - key_tile * LANES, value_tile, width + first - value_tile * LANES)
        )
    return plan


def group_tiles(width, head_dim):
    plan = pair_plan(width, head_dim)
    seen, groups = set(), []
    for group in PAIR_GROUPS:
        need = []
        for pair in group:
            key_tile, _, value_tile, _ = plan[pair]
            need += [key_tile, key_tile + 1, value_tile, value_tile + 1]
        fresh = sorted(set(need) - seen)
        seen |= set(fresh)
        groups.append(tuple(fresh))
    return groups


def spatial_kernel(*refs, group, frames, head_dim, width, tiles, held, emitted, kept):
    plan = pair_plan(width, head_dim)
    count = len(tiles)
    position = 0
    query_ref, own_ref, peer_ref = refs[:3]
    near_refs = refs[3 : 3 + count]
    far_refs = refs[3 + count : 3 + 2 * count]
    position = 3 + 2 * count
    held_ref = None
    if held:
        held_ref = refs[position]
        position += 1
    out_count = frames if emitted else 0
    out_refs = refs[position : position + out_count]
    kept_ref = refs[position + out_count] if kept else None

    where = {tile: (c, j) for c, chunk in enumerate(tiles) for j, tile in enumerate(chunk)}

    def from_chunks(chunk_refs):
        def load(tile):
            chunk, at = where[tile]
            return chunk_refs[chunk][:, at * LANES : (at + 1) * LANES]

        return load

    def from_whole(ref):
        return lambda tile: ref[:, tile * LANES : (tile + 1) * LANES]

    blocks = [from_whole(own_ref), from_whole(peer_ref), from_chunks(near_refs), from_chunks(far_refs)]
    rows = query_ref.shape[0]
    scale = softmax_scale(head_dim)
    piece = rows // frames

    def two(block, tile):
        return jnp.concatenate([block(tile), block(tile + 1)], axis=1)

    def scores_of(pair, chunk):
        key_tile, key_lane, _, _ = plan[pair]
        window = query_ref[
            chunk * QUERY_ROWS : (chunk + 1) * QUERY_ROWS, key_tile * LANES : (key_tile + 2) * LANES
        ]
        stacked = jnp.concatenate(
            [
                window * column_mask(key_lane, head_dim, bf16),
                window * column_mask(key_lane + head_dim, head_dim, bf16),
            ],
            axis=0,
        )
        return [
            lax.dot_general(stacked, two(block, key_tile), NT, preferred_element_type=f32)
            for block in blocks
        ]

    def mix(pair, scores):
        _, key_lane, value_tile, value_lane = plan[pair]
        top = functools.reduce(jnp.maximum, [jnp.max(s, axis=-1, keepdims=True) for s in scores])
        top = top * scale
        weights = [jnp.exp2(s * scale - top) for s in scores]
        total = functools.reduce(jnp.add, [jnp.sum(w, axis=-1, keepdims=True) for w in weights])
        mixed = functools.reduce(
            jnp.add,
            [
                jnp.dot(w.astype(bf16), two(block, value_tile), preferred_element_type=f32)
                for w, block in zip(weights, blocks)
            ],
        )
        mixed = mixed / total
        joined = mixed[:QUERY_ROWS] * column_mask(value_lane, head_dim, f32) + mixed[
            QUERY_ROWS:
        ] * column_mask(value_lane + head_dim, head_dim, f32)
        return pltpu.roll(joined, (key_lane - value_lane) % (2 * LANES), 1)

    chunks = rows // QUERY_ROWS
    tasks = [(chunk, pair) for chunk in range(chunks) for pair in group]
    pending = scores_of(tasks[0][1], tasks[0][0])
    parts = {}
    for index, (chunk, pair) in enumerate(tasks):
        scores = pending
        if index + 1 < len(tasks):
            pending = scores_of(tasks[index + 1][1], tasks[index + 1][0])
        joined = mix(pair, scores)
        tile = plan[pair][0]
        for side in range(2):
            half = joined[:, side * LANES : (side + 1) * LANES]
            parts[tile + side] = parts[tile + side] + half if tile + side in parts else half
        if pair != group[-1]:
            continue
        at = chunk * QUERY_ROWS
        for number, tile in enumerate(held):
            old = held_ref[at : at + QUERY_ROWS, number * LANES : (number + 1) * LANES].astype(f32)
            parts[tile] = parts[tile] + old if tile in parts else old
        if kept:
            values = jnp.concatenate([parts[tile] for tile in kept], axis=1)
            kept_ref[at : at + QUERY_ROWS, :] = values.astype(bf16)
        if emitted:
            values = jnp.concatenate([parts[tile] for tile in emitted], axis=1).astype(bf16)
            width_out = out_refs[0].shape[1]
            for sub in range(QUERY_ROWS // piece):
                out_refs[at // piece + sub][...] = values[
                    sub * piece : (sub + 1) * piece, :width_out
                ]
        parts = {}


def tile_flow(width, head_dim):
    plan = pair_plan(width, head_dim)
    flow, held = [], ()
    for number, group in enumerate(PAIR_GROUPS):
        have = sorted({plan[pair][0] + side for pair in group for side in range(2)} | set(held))
        last = number == len(PAIR_GROUPS) - 1
        complete = [tile for tile in have if last or tile <= plan[group[-1]][0]]
        emitted = tuple(complete) if EMIT[number] else ()
        kept = tuple(tile for tile in have if tile not in emitted)
        flow.append((held, emitted, kept))
        held = kept
    return flow


def spatial_group(number, query, own_kv, peer_kv, near, far, carry, frames, head_dim, width):
    group = PAIR_GROUPS[number]
    held, emitted, kept = tile_flow(width, head_dim)[number]
    tiles = tuple(group_tiles(width, head_dim)[: number + 1])
    rows = query.shape[0]
    shapes = []
    if emitted:
        columns = min(width, (emitted[-1] + 1) * LANES) - emitted[0] * LANES
        shapes += [((rows // frames, columns), bf16) for _ in range(frames)]
    if kept:
        shapes.append(((rows, len(kept) * LANES), bf16))
    operands = [query, own_kv, peer_kv, *near[: number + 1], *far[: number + 1]]
    if held:
        operands.append(carry)
    keys = 4 * rows
    results = on_chip_call(
        functools.partial(
            spatial_kernel,
            group=group,
            frames=frames,
            head_dim=head_dim,
            width=width,
            tiles=tiles,
            held=held,
            emitted=emitted,
            kept=kept,
        ),
        operands,
        shapes,
        len(group) * 2 * rows * keys * 256 * 4,
        24,
        len(group) * 2 * rows * keys,
    )
    results = list(results)
    carry = results.pop() if kept else None
    return results, carry


def joined_rows(tokens_refs, mixed_refs):
    groups = len(mixed_refs) // len(tokens_refs)
    tokens = jnp.concatenate([ref[...] for ref in tokens_refs], axis=0).astype(f32)
    mixed = jnp.concatenate(
        [
            jnp.concatenate(
                [ref[...] for ref in mixed_refs[frame * groups : (frame + 1) * groups]], axis=1
            )
            for frame in range(len(tokens_refs))
        ],
        axis=0,
    )
    return tokens, mixed


def temporal_in_kernel(*refs, frames, groups):
    tokens_refs = refs[:frames]
    mixed_refs = refs[frames : frames + frames * groups]
    position = frames + frames * groups
    out_weight, qkv_weight, modulation_ref, place_ref, query_ref, kv_ref = refs[position:]
    width = out_weight.shape[0]
    piece = tokens_refs[0].shape[0]
    tokens, mixed = joined_rows(tokens_refs, mixed_refs)
    after = tokens + modulation_ref[2:3, :] * jnp.dot(
        mixed, out_weight[...], preferred_element_type=f32
    )
    normal = normalize(after) * (1.0 + modulation_ref[4:5, :]) + modulation_ref[3:4, :]
    inputs = jnp.concatenate(
        [
            (normal[frame * piece : (frame + 1) * piece] + place_ref[frame : frame + 1, :]).astype(bf16)
            for frame in range(frames)
        ],
        axis=0,
    )
    query_ref[...] = lax.dot_general(
        inputs, qkv_weight[: query_ref.shape[1], :], NT, preferred_element_type=f32
    ).astype(bf16)
    kv_ref[...] = lax.dot_general(
        inputs, qkv_weight[width:, :], NT, preferred_element_type=f32
    ).astype(bf16)


def temporal_in(tokens, mixed, spatial_out, temporal_qkv, modulation, places):
    frames, groups = len(tokens), len(mixed[0])
    width, feature_width = spatial_out.shape
    padded = -(-width // LANES) * LANES
    rows = frames * tokens[0].shape[0]
    return on_chip_call(
        functools.partial(temporal_in_kernel, frames=frames, groups=groups),
        [
            *tokens,
            *[part for frame in mixed for part in frame],
            spatial_out,
            temporal_qkv,
            modulation,
            places,
        ],
        [((rows, padded), bf16), ((rows, 2 * width), bf16)],
        2 * rows * feature_width * width * 4,
        20,
    )


def temporal_kernel(query_ref, kv_ref, *out_refs, head_dim, first):
    frames = len(out_refs)
    piece, width = out_refs[0].shape
    stride = query_ref.shape[0] // frames
    scale = softmax_scale(head_dim)
    step = max(16, min(piece, LANES // frames))
    block = frames * step
    row_at = lax.broadcasted_iota(jnp.int32, (2 * block, block), 0) % step
    column_at = lax.broadcasted_iota(jnp.int32, (2 * block, block), 1) % step
    same = row_at == column_at
    plan = pair_plan(width, head_dim)

    for start in range(0, piece, step):

        def window(ref, tile):
            return jnp.concatenate(
                [
                    ref[
                        frame * stride + first + start : frame * stride + first + start + step,
                        tile * LANES : (tile + 2) * LANES,
                    ]
                    for frame in range(frames)
                ],
                axis=0,
            )

        parts = {}
        for tile, lane, value_tile, value_lane in plan:
            queries = window(query_ref, tile)
            stacked = jnp.concatenate(
                [
                    queries * column_mask(lane, head_dim, bf16),
                    queries * column_mask(lane + head_dim, head_dim, bf16),
                ],
                axis=0,
            )
            scores = lax.dot_general(stacked, window(kv_ref, tile), NT, preferred_element_type=f32)
            scores = jnp.where(same, scores * scale, -jnp.inf)
            weights = jnp.exp2(scores - jnp.max(scores, axis=-1, keepdims=True))
            weights = (weights / jnp.sum(weights, axis=-1, keepdims=True)).astype(bf16)
            mixed_pair = jnp.dot(weights, window(kv_ref, value_tile), preferred_element_type=f32)
            joined = mixed_pair[:block] * column_mask(value_lane, head_dim, f32) + mixed_pair[
                block:
            ] * column_mask(value_lane + head_dim, head_dim, f32)
            joined = pltpu.roll(joined, (lane - value_lane) % (2 * LANES), 1)
            for side in range(2):
                half = joined[:, side * LANES : (side + 1) * LANES]
                parts[tile + side] = parts[tile + side] + half if tile + side in parts else half
        values = jnp.concatenate([parts[tile] for tile in sorted(parts)], axis=1).astype(bf16)
        for frame in range(frames):
            out_refs[frame][start : start + step, :] = values[
                frame * step : (frame + 1) * step, :width
            ]


def temporal(query, kv, frames, head_dim, first, piece):
    width = kv.shape[1] // 2
    rows = frames * piece
    return on_chip_call(
        functools.partial(temporal_kernel, head_dim=head_dim, first=first),
        [query, kv],
        [((piece, width), bf16) for _ in range(frames)],
        2 * rows * 128 * 256 * 16,
        8,
        rows * 128 * 8,
    )


def after_kernel(*refs, frames, groups):
    weight_ref, modulation_ref, out_ref = refs[frames + frames * groups :]
    tokens, mixed = joined_rows(refs[:frames], refs[frames : frames + frames * groups])
    out_ref[...] = tokens + modulation_ref[2:3, :] * jnp.dot(
        mixed, weight_ref[...], preferred_element_type=f32
    )


def after_spatial(tokens, mixed, weight, modulation):
    frames, groups = len(tokens), len(mixed[0])
    width, feature_width = weight.shape
    rows = frames * tokens[0].shape[0]
    return on_chip_call(
        functools.partial(after_kernel, frames=frames, groups=groups),
        [*tokens, *[part for frame in mixed for part in frame], weight, modulation],
        [((rows, feature_width), f32)],
        2 * rows * feature_width * width,
        16,
    )[0]


def output_kernel(slot_ref, after_ref, weight_ref, modulation_ref, *refs, frames, halves):
    parts, (out_ref, stage_ref, sems) = refs[: frames * halves], refs[frames * halves :]
    piece = after_ref.shape[0] // frames
    copies = []
    for frame in range(frames):
        cut = slice(frame * piece, (frame + 1) * piece)
        mixed = jnp.concatenate([parts[frame * halves + h][...] for h in range(halves)], axis=0)
        stage_ref[cut, :] = after_ref[cut, :] + modulation_ref[5:6, :] * jnp.dot(
            mixed, weight_ref[...], preferred_element_type=f32
        )
        row = partner_slot(slot_ref[0], frame, frames) * piece
        copies.append(
            pltpu.make_async_copy(
                stage_ref.at[cut, :], out_ref.at[pl.ds(row, piece), :], sems.at[frame]
            )
        )
        copies[-1].start()
    for copy in copies:
        copy.wait()


def output(slot, after, weight, modulation, parts, frames):
    rows, feature_width = after.shape
    halves = len(parts[0])
    operands = [after, weight, modulation, *[part for frame in parts for part in frame]]
    return pl.pallas_call(
        functools.partial(output_kernel, frames=frames, halves=halves),
        out_shape=jax.ShapeDtypeStruct((rows, feature_width), f32),
        in_specs=[pl.BlockSpec(memory_space=pltpu.SMEM), *vmem_specs(len(operands))],
        out_specs=pl.BlockSpec(memory_space=pltpu.HBM),
        scratch_shapes=[
            pltpu.VMEM((rows, feature_width), f32),
            pltpu.SemaphoreType.DMA((frames,)),
        ],
        compiler_params=pltpu.CompilerParams(vmem_limit_bytes=16 * 2**20),
        name="block_output",
    )(slot, *[pltpu.with_memory_space_constraint(array, pltpu.VMEM) for array in operands])


def per_device(
    tokens,
    stale_kv,
    mod_table,
    mod_mix,
    timestep,
    frame_order,
    spatial_qkv,
    spatial_out,
    temporal_qkv,
    temporal_out,
):
    devices = lax.axis_size("patch")
    frames = devices // 4
    slot = lax.axis_index("patch") // 4
    rows, feature_width = tokens.shape
    width = spatial_out.shape[0]
    head_dim = feature_width // HEADS
    piece = rows // frames

    def other_core(device):
        return device ^ 1

    def other_chip(device):
        return device ^ 2

    def ahead(step):
        return lambda device: partner_slot(device // 4, step, frames) * 4 + device % 4

    def behind(step):
        return lambda device: source_slot(device // 4, step, frames) * 4 + device % 4

    near, far = [], []
    for chunk in stage_chunks(stale_kv, group_tiles(width, head_dim)):
        near.append(permute(chunk, other_chip))
        far.append(permute(near[-1], other_core))
    peer_kv = permute(stale_kv, other_core)

    slot_word = slot.astype(jnp.int32)[None]
    pieces = stage_pieces(slot_word, tokens, frames)
    there = [pieces[0]]
    there += [permute(pieces[s], ahead(s)) for s in range(1, frames)]

    modulation = mod_table + mod_mix * sinusoid(timestep[0], feature_width)[None, :]
    sources = source_slot(slot, jnp.arange(frames), frames)
    places = sinusoid(frame_order[sources], feature_width)

    query, own_kv = projections(
        pieces,
        jnp.swapaxes(spatial_qkv, 1, 2).reshape(3 * width, feature_width),
        modulation,
        width,
    )

    carry = None
    local = [[] for _ in range(frames)]
    sent = [[] for _ in range(frames)]
    for number in range(len(PAIR_GROUPS)):
        outs, carry = spatial_group(
            number, query, own_kv, peer_kv, near, far, carry, frames, head_dim, width
        )
        for s, out in enumerate(outs):
            local[s].append(out)
            sent[s].append(out if s == 0 else permute(out, ahead(s)))

    after = after_spatial(pieces, local, spatial_out, modulation)
    temporal_query, temporal_kv = temporal_in(
        there,
        sent,
        spatial_out,
        jnp.swapaxes(temporal_qkv, 1, 2).reshape(3 * width, feature_width),
        modulation,
        places,
    )
    half = piece // HALVES
    back = [[] for _ in range(frames)]
    for h in range(HALVES):
        outs = temporal(temporal_query, temporal_kv, frames, head_dim, h * half, half)
        for s, out in enumerate(outs):
            back[s].append(out if s == 0 else permute(out, behind(s)))

    return output(
        slot_word, after, temporal_out, modulation, back, frames
    )


def solution(mesh):
    return jax.shard_map(
        per_device,
        mesh=mesh,
        in_specs=(
            P(("groups", "patch"), None),
            P(("groups", "patch"), None),
            P(),
            P(),
            P("groups"),
            P("groups"),
            P(),
            P(),
            P(),
            P(),
        ),
        out_specs=P(("groups", "patch"), None),
        check_vma=False,
    )
```

```python
import functools
import math

import jax
import jax.numpy as jnp
import numpy as np
from jax import lax
from jax.experimental import pallas as pl
from jax.experimental.pallas import tpu as pltpu
from jax.sharding import PartitionSpec as P


HEADS = 16
LANES = 128
QUERY_ROWS = 128
PAIR_GROUPS = ((0,), (1,), (2,), (3,))
EMIT = (False, False, True, True)
HALVES = 2


epsilon = 1e-06
bf16 = jnp.bfloat16
f32 = jnp.float32
NT = (((1,), (1,)), ((), ()))


def permute(value, target):
    count = lax.axis_size("patch")
    return lax.ppermute(value, "patch", [(source, target(source)) for source in range(count)])


def partner_slot(slot, step, frames):
    if frames & (frames - 1) == 0:
        return slot ^ step
    return (slot + step) % frames


def source_slot(slot, step, frames):
    if frames & (frames - 1) == 0:
        return slot ^ step
    return (slot - step) % frames


def normalize(activations):
    row_mean = jnp.mean(activations, axis=-1, keepdims=True)
    centered = activations - row_mean
    variance = jnp.mean(centered * centered, axis=-1, keepdims=True)
    return centered * lax.rsqrt(variance + epsilon)


def column_mask(first, width, dtype):
    column = lax.broadcasted_iota(jnp.int32, (1, 2 * LANES), 1)
    inside = jnp.logical_and(column >= first, column < first + width)
    return jnp.where(inside, 1.0, 0.0).astype(dtype)


def softmax_scale(head_dim):
    return math.log2(math.e) * head_dim ** (-0.5)


def vmem_specs(count):
    return [pl.BlockSpec(memory_space=pltpu.VMEM) for _ in range(count)]


def on_chip_call(kernel, operands, shapes, flops, limit_mib, transcendentals=0, scratch=()):
    operands = [pltpu.with_memory_space_constraint(array, pltpu.VMEM) for array in operands]
    return pl.pallas_call(
        kernel,
        out_shape=[pltpu.VMEM(shape, dtype) for shape, dtype in shapes],
        in_specs=vmem_specs(len(operands)),
        out_specs=vmem_specs(len(shapes)),
        scratch_shapes=list(scratch),
        compiler_params=pltpu.CompilerParams(vmem_limit_bytes=limit_mib * 2**20),
        cost_estimate=pl.CostEstimate(
            flops=flops,
            bytes_accessed=sum(array.size * array.dtype.itemsize for array in operands),
            transcendentals=transcendentals,
        ),
    )(*operands)


def chunk_kernel(kv_ref, *refs, tiles):
    out_refs, sems = refs[:-1], refs[-1]
    copies = []
    for chunk, ref in zip(tiles, out_refs):
        for at, tile in enumerate(chunk):
            copies.append(
                pltpu.make_async_copy(
                    kv_ref.at[:, tile * LANES : (tile + 1) * LANES],
                    ref.at[:, at * LANES : (at + 1) * LANES],
                    sems.at[len(copies)],
                )
            )
            copies[-1].start()
    for copy in copies:
        copy.wait()


def stage_chunks(stale_kv, tiles):
    rows = stale_kv.shape[0]
    return pl.pallas_call(
        functools.partial(chunk_kernel, tiles=tiles),
        out_shape=[pltpu.VMEM((rows, len(chunk) * LANES), bf16) for chunk in tiles],
        in_specs=[pl.BlockSpec(memory_space=pltpu.HBM)],
        out_specs=vmem_specs(len(tiles)),
        scratch_shapes=[pltpu.SemaphoreType.DMA((sum(len(chunk) for chunk in tiles),))],
        compiler_params=pltpu.CompilerParams(vmem_limit_bytes=2**20),
        name="chunks",
    )(pltpu.with_memory_space_constraint(stale_kv, pltpu.HBM))


def piece_kernel(slot_ref, tokens_ref, *refs, frames):
    out_refs, sems = refs[:-1], refs[-1]
    piece = tokens_ref.shape[0] // frames
    copies = []
    for step in range(frames):
        row = partner_slot(slot_ref[0], step, frames) * piece
        copies.append(
            pltpu.make_async_copy(
                tokens_ref.at[pl.ds(row, piece), :], out_refs[step], sems.at[step]
            )
        )
        copies[-1].start()
    for copy in copies:
        copy.wait()


def stage_pieces(slot, tokens, frames):
    rows, feature_width = tokens.shape
    return pl.pallas_call(
        functools.partial(piece_kernel, frames=frames),
        out_shape=[pltpu.VMEM((rows // frames, feature_width), bf16) for _ in range(frames)],
        in_specs=[
            pl.BlockSpec(memory_space=pltpu.SMEM),
            pl.BlockSpec(memory_space=pltpu.HBM),
        ],
        out_specs=vmem_specs(frames),
        scratch_shapes=[pltpu.SemaphoreType.DMA((frames,))],
        compiler_params=pltpu.CompilerParams(vmem_limit_bytes=2**20),
        name="pieces",
    )(slot, pltpu.with_memory_space_constraint(tokens, pltpu.HBM))


def modulation_kernel(slot_ref, time_ref, order_ref, rate_ref, table_ref, mix_ref, out_ref, place_ref):
    frames, feature_width = place_ref.shape
    rows = -(-(frames + 1) // 8) * 8
    row = lax.broadcasted_iota(jnp.int32, (rows, 1), 0)
    position = jnp.where(row == frames, time_ref[0], 0)
    for step in range(frames):
        frame = order_ref[source_slot(slot_ref[0], step, frames)]
        position = jnp.where(row == step, frame, position)
    angles = position.astype(f32) * rate_ref[...]
    column = lax.broadcasted_iota(jnp.int32, (rows, feature_width), 1)
    waves = jnp.where(column < feature_width // 2, jnp.sin(angles), jnp.cos(angles))
    place_ref[...] = waves[:frames]
    out_ref[...] = table_ref[...] + mix_ref[...] * waves[frames : frames + 1]


def modulate(slot, timestep, frame_order, mod_table, mod_mix):
    frames, feature_width = frame_order.shape[0], mod_table.shape[1]
    half = feature_width // 2
    rates = np.exp(-math.log(10000.0) * np.arange(half) / half).astype(np.float32)
    operands = [jnp.asarray(np.concatenate([rates, rates])[None]), mod_table, mod_mix]
    operands = [pltpu.with_memory_space_constraint(array, pltpu.VMEM) for array in operands]
    return pl.pallas_call(
        modulation_kernel,
        out_shape=[pltpu.VMEM(mod_table.shape, f32), pltpu.VMEM((frames, feature_width), f32)],
        in_specs=[pl.BlockSpec(memory_space=pltpu.SMEM) for _ in range(3)] + vmem_specs(3),
        out_specs=vmem_specs(2),
        compiler_params=pltpu.CompilerParams(vmem_limit_bytes=2**20),
        name="modulation",
    )(slot, timestep, frame_order, *operands)


def projection_kernel(*refs, frames, width):
    pieces = refs[:frames]
    weight_ref, modulation_ref, query_ref, kv_ref = refs[frames:]
    tokens = jnp.concatenate([ref[...] for ref in pieces], axis=0).astype(f32)
    inputs = normalize(tokens) * (1.0 + modulation_ref[1:2, :]) + modulation_ref[0:1, :]
    inputs = inputs.astype(bf16)
    padded = query_ref.shape[1]
    query_ref[...] = lax.dot_general(
        inputs, weight_ref[:padded, :], NT, preferred_element_type=f32
    ).astype(bf16)
    kv_ref[...] = lax.dot_general(
        inputs, weight_ref[width:, :], NT, preferred_element_type=f32
    ).astype(bf16)


def projections(pieces, weight, modulation, width):
    frames = len(pieces)
    piece, feature_width = pieces[0].shape
    padded = -(-width // LANES) * LANES
    rows = frames * piece
    return on_chip_call(
        functools.partial(projection_kernel, frames=frames, width=width),
        [*pieces, weight, modulation],
        [((rows, padded), bf16), ((rows, 2 * width), bf16)],
        2 * rows * feature_width * 3 * width,
        4,
    )


def pair_plan(width, head_dim):
    plan = []
    for first in range(0, width, 2 * head_dim):
        key_tile = first // LANES
        value_tile = (width + first) // LANES
        plan.append(
            (key_tile, first - key_tile * LANES, value_tile, width + first - value_tile * LANES)
        )
    return plan


def group_tiles(width, head_dim):
    plan = pair_plan(width, head_dim)
    seen, groups = set(), []
    for group in PAIR_GROUPS:
        need = []
        for pair in group:
            key_tile, _, value_tile, _ = plan[pair]
            need += [key_tile, key_tile + 1, value_tile, value_tile + 1]
        fresh = sorted(set(need) - seen)
        seen |= set(fresh)
        groups.append(tuple(fresh))
    return groups


def spatial_kernel(*refs, group, frames, head_dim, width, tiles, held, emitted, kept):
    plan = pair_plan(width, head_dim)
    count = len(tiles)
    position = 0
    refs, (scores_ref, weights_ref) = refs[:-2], refs[-2:]
    query_ref, own_ref, peer_ref = refs[:3]
    near_refs = refs[3 : 3 + count]
    far_refs = refs[3 + count : 3 + 2 * count]
    position = 3 + 2 * count
    held_ref = None
    if held:
        held_ref = refs[position]
        position += 1
    out_count = frames if emitted else 0
    out_refs = refs[position : position + out_count]
    kept_ref = refs[position + out_count] if kept else None

    where = {tile: (c, j) for c, chunk in enumerate(tiles) for j, tile in enumerate(chunk)}

    def from_chunks(chunk_refs):
        def load(tile):
            chunk, at = where[tile]
            return chunk_refs[chunk][:, at * LANES : (at + 1) * LANES]

        return load

    def from_whole(ref):
        return lambda tile: ref[:, tile * LANES : (tile + 1) * LANES]

    blocks = [from_whole(own_ref), from_whole(peer_ref), from_chunks(near_refs), from_chunks(far_refs)]
    rows = query_ref.shape[0]
    scale = softmax_scale(head_dim)
    piece = rows // frames

    def two(block, tile):
        return jnp.concatenate([block(tile), block(tile + 1)], axis=1)

    def score(index):
        chunk, pair = tasks[index]
        key_tile, key_lane, _, _ = plan[pair]
        window = query_ref[
            chunk * QUERY_ROWS : (chunk + 1) * QUERY_ROWS, key_tile * LANES : (key_tile + 2) * LANES
        ]
        stacked = jnp.concatenate(
            [
                window * column_mask(key_lane, head_dim, bf16),
                window * column_mask(key_lane + head_dim, head_dim, bf16),
            ],
            axis=0,
        )
        for number, block in enumerate(blocks):
            scores_ref[index % 2, :, number * rows : (number + 1) * rows] = lax.dot_general(
                stacked, two(block, key_tile), NT, preferred_element_type=f32
            )

    def weigh(index):
        totals = []
        for row in range(0, 2 * QUERY_ROWS, 16):
            scores = scores_ref[index % 2, row : row + 16, :]
            top = jnp.max(scores, axis=-1, keepdims=True) * scale
            weights = jnp.exp2(scores * scale - top)
            totals.append(jnp.sum(weights, axis=-1, keepdims=True))
            weights_ref[index % 2, row : row + 16, :] = weights.astype(bf16)
        return jnp.concatenate(totals, axis=0)

    def mix(index, total):
        _, key_lane, value_tile, value_lane = plan[tasks[index][1]]
        mixed = functools.reduce(
            jnp.add,
            [
                jnp.dot(
                    weights_ref[index % 2, :, number * rows : (number + 1) * rows],
                    two(block, value_tile),
                    preferred_element_type=f32,
                )
                for number, block in enumerate(blocks)
            ],
        )
        mixed = mixed / total
        joined = mixed[:QUERY_ROWS] * column_mask(value_lane, head_dim, f32) + mixed[
            QUERY_ROWS:
        ] * column_mask(value_lane + head_dim, head_dim, f32)
        return pltpu.roll(joined, (key_lane - value_lane) % (2 * LANES), 1)

    tasks = [(chunk, pair) for chunk in range(rows // QUERY_ROWS) for pair in group]
    parts = {}

    def finish(index, total):
        chunk, pair = tasks[index]
        joined = mix(index, total)
        tile = plan[pair][0]
        for side in range(2):
            half = joined[:, side * LANES : (side + 1) * LANES]
            parts[tile + side] = parts[tile + side] + half if tile + side in parts else half
        if pair != group[-1]:
            return
        at = chunk * QUERY_ROWS
        for number, tile in enumerate(held):
            old = held_ref[at : at + QUERY_ROWS, number * LANES : (number + 1) * LANES].astype(f32)
            parts[tile] = parts[tile] + old if tile in parts else old
        if kept:
            values = jnp.concatenate([parts[tile] for tile in kept], axis=1)
            kept_ref[at : at + QUERY_ROWS, :] = values.astype(bf16)
        if emitted:
            values = jnp.concatenate([parts[tile] for tile in emitted], axis=1).astype(bf16)
            width_out = out_refs[0].shape[1]
            for sub in range(QUERY_ROWS // piece):
                out_refs[at // piece + sub][...] = values[
                    sub * piece : (sub + 1) * piece, :width_out
                ]
        parts.clear()

    score(0)
    total = None
    for index in range(len(tasks)):
        if index + 1 < len(tasks):
            score(index + 1)
        if index > 0:
            finish(index - 1, total)
        total = weigh(index)
    finish(len(tasks) - 1, total)


def tile_flow(width, head_dim):
    plan = pair_plan(width, head_dim)
    flow, held = [], ()
    for number, group in enumerate(PAIR_GROUPS):
        have = sorted({plan[pair][0] + side for pair in group for side in range(2)} | set(held))
        last = number == len(PAIR_GROUPS) - 1
        complete = [tile for tile in have if last or tile <= plan[group[-1]][0]]
        emitted = tuple(complete) if EMIT[number] else ()
        kept = tuple(tile for tile in have if tile not in emitted)
        flow.append((held, emitted, kept))
        held = kept
    return flow


def spatial_group(number, query, own_kv, peer_kv, near, far, carry, frames, head_dim, width):
    group = PAIR_GROUPS[number]
    held, emitted, kept = tile_flow(width, head_dim)[number]
    tiles = tuple(group_tiles(width, head_dim)[: number + 1])
    rows = query.shape[0]
    shapes = []
    if emitted:
        columns = min(width, (emitted[-1] + 1) * LANES) - emitted[0] * LANES
        shapes += [((rows // frames, columns), bf16) for _ in range(frames)]
    if kept:
        shapes.append(((rows, len(kept) * LANES), bf16))
    operands = [query, own_kv, peer_kv, *near[: number + 1], *far[: number + 1]]
    if held:
        operands.append(carry)
    keys = 4 * rows
    results = on_chip_call(
        functools.partial(
            spatial_kernel,
            group=group,
            frames=frames,
            head_dim=head_dim,
            width=width,
            tiles=tiles,
            held=held,
            emitted=emitted,
            kept=kept,
        ),
        operands,
        shapes,
        len(group) * 2 * rows * keys * 256 * 4,
        8,
        len(group) * 2 * rows * keys,
        [
            pltpu.VMEM((2, 2 * QUERY_ROWS, keys), f32),
            pltpu.VMEM((2, 2 * QUERY_ROWS, keys), bf16),
        ],
    )
    results = list(results)
    carry = results.pop() if kept else None
    return results, carry


def joined_rows(tokens_refs, mixed_refs):
    groups = len(mixed_refs) // len(tokens_refs)
    tokens = jnp.concatenate([ref[...] for ref in tokens_refs], axis=0).astype(f32)
    mixed = jnp.concatenate(
        [
            jnp.concatenate(
                [ref[...] for ref in mixed_refs[frame * groups : (frame + 1) * groups]], axis=1
            )
            for frame in range(len(tokens_refs))
        ],
        axis=0,
    )
    return tokens, mixed


def temporal_in_kernel(*refs, frames, groups):
    tokens_refs = refs[:frames]
    mixed_refs = refs[frames : frames + frames * groups]
    position = frames + frames * groups
    out_weight, qkv_weight, modulation_ref, place_ref, query_ref, kv_ref = refs[position:]
    width = out_weight.shape[0]
    piece = tokens_refs[0].shape[0]
    tokens, mixed = joined_rows(tokens_refs, mixed_refs)
    after = tokens + modulation_ref[2:3, :] * jnp.dot(
        mixed, out_weight[...], preferred_element_type=f32
    )
    normal = normalize(after) * (1.0 + modulation_ref[4:5, :]) + modulation_ref[3:4, :]
    inputs = jnp.concatenate(
        [
            (normal[frame * piece : (frame + 1) * piece] + place_ref[frame : frame + 1, :]).astype(bf16)
            for frame in range(frames)
        ],
        axis=0,
    )
    query_ref[...] = lax.dot_general(
        inputs, qkv_weight[: query_ref.shape[1], :], NT, preferred_element_type=f32
    ).astype(bf16)
    kv_ref[...] = lax.dot_general(
        inputs, qkv_weight[width:, :], NT, preferred_element_type=f32
    ).astype(bf16)


def temporal_in(tokens, mixed, spatial_out, temporal_qkv, modulation, places):
    frames, groups = len(tokens), len(mixed[0])
    width, feature_width = spatial_out.shape
    padded = -(-width // LANES) * LANES
    rows = frames * tokens[0].shape[0]
    return on_chip_call(
        functools.partial(temporal_in_kernel, frames=frames, groups=groups),
        [
            *tokens,
            *[part for frame in mixed for part in frame],
            spatial_out,
            temporal_qkv,
            modulation,
            places,
        ],
        [((rows, padded), bf16), ((rows, 2 * width), bf16)],
        2 * rows * feature_width * width * 4,
        6,
    )


def temporal_kernel(query_ref, kv_ref, *out_refs, head_dim, first):
    frames = len(out_refs)
    piece, width = out_refs[0].shape
    stride = query_ref.shape[0] // frames
    scale = softmax_scale(head_dim)
    step = max(16, min(piece, LANES // frames))
    block = frames * step
    row_at = lax.broadcasted_iota(jnp.int32, (2 * block, block), 0) % step
    column_at = lax.broadcasted_iota(jnp.int32, (2 * block, block), 1) % step
    same = row_at == column_at
    plan = pair_plan(width, head_dim)

    for start in range(0, piece, step):

        def window(ref, tile):
            return jnp.concatenate(
                [
                    ref[
                        frame * stride + first + start : frame * stride + first + start + step,
                        tile * LANES : (tile + 2) * LANES,
                    ]
                    for frame in range(frames)
                ],
                axis=0,
            )

        parts = {}
        for tile, lane, value_tile, value_lane in plan:
            queries = window(query_ref, tile)
            stacked = jnp.concatenate(
                [
                    queries * column_mask(lane, head_dim, bf16),
                    queries * column_mask(lane + head_dim, head_dim, bf16),
                ],
                axis=0,
            )
            scores = lax.dot_general(stacked, window(kv_ref, tile), NT, preferred_element_type=f32)
            scores = jnp.where(same, scores * scale, -jnp.inf)
            weights = jnp.exp2(scores - jnp.max(scores, axis=-1, keepdims=True))
            weights = (weights / jnp.sum(weights, axis=-1, keepdims=True)).astype(bf16)
            mixed_pair = jnp.dot(weights, window(kv_ref, value_tile), preferred_element_type=f32)
            joined = mixed_pair[:block] * column_mask(value_lane, head_dim, f32) + mixed_pair[
                block:
            ] * column_mask(value_lane + head_dim, head_dim, f32)
            joined = pltpu.roll(joined, (lane - value_lane) % (2 * LANES), 1)
            for side in range(2):
                half = joined[:, side * LANES : (side + 1) * LANES]
                parts[tile + side] = parts[tile + side] + half if tile + side in parts else half
        values = jnp.concatenate([parts[tile] for tile in sorted(parts)], axis=1).astype(bf16)
        for frame in range(frames):
            out_refs[frame][start : start + step, :] = values[
                frame * step : (frame + 1) * step, :width
            ]


def temporal(query, kv, frames, head_dim, first, piece):
    width = kv.shape[1] // 2
    rows = frames * piece
    return on_chip_call(
        functools.partial(temporal_kernel, head_dim=head_dim, first=first),
        [query, kv],
        [((piece, width), bf16) for _ in range(frames)],
        2 * rows * 128 * 256 * 16,
        2,
        rows * 128 * 8,
    )


def after_kernel(*refs, frames, groups):
    weight_ref, modulation_ref, out_ref = refs[frames + frames * groups :]
    tokens, mixed = joined_rows(refs[:frames], refs[frames : frames + frames * groups])
    out_ref[...] = tokens + modulation_ref[2:3, :] * jnp.dot(
        mixed, weight_ref[...], preferred_element_type=f32
    )


def after_spatial(tokens, mixed, weight, modulation):
    frames, groups = len(tokens), len(mixed[0])
    width, feature_width = weight.shape
    rows = frames * tokens[0].shape[0]
    return on_chip_call(
        functools.partial(after_kernel, frames=frames, groups=groups),
        [*tokens, *[part for frame in mixed for part in frame], weight, modulation],
        [((rows, feature_width), f32)],
        2 * rows * feature_width * width,
        4,
    )[0]


def output_kernel(slot_ref, after_ref, weight_ref, modulation_ref, *refs, frames, halves):
    parts, (out_ref, stage_ref, sems) = refs[: frames * halves], refs[frames * halves :]
    piece = after_ref.shape[0] // frames
    copies = []
    for frame in range(frames):
        cut = slice(frame * piece, (frame + 1) * piece)
        mixed = jnp.concatenate([parts[frame * halves + h][...] for h in range(halves)], axis=0)
        stage_ref[cut, :] = after_ref[cut, :] + modulation_ref[5:6, :] * jnp.dot(
            mixed, weight_ref[...], preferred_element_type=f32
        )
        row = partner_slot(slot_ref[0], frame, frames) * piece
        copies.append(
            pltpu.make_async_copy(
                stage_ref.at[cut, :], out_ref.at[pl.ds(row, piece), :], sems.at[frame]
            )
        )
        copies[-1].start()
    for copy in copies:
        copy.wait()


def output(slot, after, weight, modulation, parts, frames):
    rows, feature_width = after.shape
    halves = len(parts[0])
    operands = [after, weight, modulation, *[part for frame in parts for part in frame]]
    return pl.pallas_call(
        functools.partial(output_kernel, frames=frames, halves=halves),
        out_shape=jax.ShapeDtypeStruct((rows, feature_width), f32),
        in_specs=[pl.BlockSpec(memory_space=pltpu.SMEM), *vmem_specs(len(operands))],
        out_specs=pl.BlockSpec(memory_space=pltpu.HBM),
        scratch_shapes=[
            pltpu.VMEM((rows, feature_width), f32),
            pltpu.SemaphoreType.DMA((frames,)),
        ],
        compiler_params=pltpu.CompilerParams(vmem_limit_bytes=4 * 2**20),
        name="block_output",
    )(slot, *[pltpu.with_memory_space_constraint(array, pltpu.VMEM) for array in operands])


def per_device(
    tokens,
    stale_kv,
    mod_table,
    mod_mix,
    timestep,
    frame_order,
    spatial_qkv,
    spatial_out,
    temporal_qkv,
    temporal_out,
):
    devices = lax.axis_size("patch")
    frames = devices // 4
    slot = lax.axis_index("patch") // 4
    rows, feature_width = tokens.shape
    width = spatial_out.shape[0]
    head_dim = feature_width // HEADS
    piece = rows // frames

    def other_core(device):
        return device ^ 1

    def other_chip(device):
        return device ^ 2

    def ahead(step):
        return lambda device: partner_slot(device // 4, step, frames) * 4 + device % 4

    def behind(step):
        return lambda device: source_slot(device // 4, step, frames) * 4 + device % 4

    near, far = [], []
    for chunk in stage_chunks(stale_kv, group_tiles(width, head_dim)):
        near.append(permute(chunk, other_chip))
        far.append(permute(near[-1], other_core))
    peer_kv = permute(stale_kv, other_core)

    slot_word = slot.astype(jnp.int32)[None]
    pieces = stage_pieces(slot_word, tokens, frames)
    there = [pieces[0]]
    there += [permute(pieces[s], ahead(s)) for s in range(1, frames)]

    modulation, places = modulate(slot_word, timestep, frame_order, mod_table, mod_mix)
    query, own_kv = projections(
        pieces,
        jnp.swapaxes(spatial_qkv, 1, 2).reshape(3 * width, feature_width),
        modulation,
        width,
    )

    carry = None
    local = [[] for _ in range(frames)]
    sent = [[] for _ in range(frames)]
    for number in range(len(PAIR_GROUPS)):
        outs, carry = spatial_group(
            number, query, own_kv, peer_kv, near, far, carry, frames, head_dim, width
        )
        for s, out in enumerate(outs):
            local[s].append(out)
            sent[s].append(out if s == 0 else permute(out, ahead(s)))

    after = after_spatial(pieces, local, spatial_out, modulation)
    temporal_query, temporal_kv = temporal_in(
        there,
        sent,
        spatial_out,
        jnp.swapaxes(temporal_qkv, 1, 2).reshape(3 * width, feature_width),
        modulation,
        places,
    )
    half = piece // HALVES
    back = [[] for _ in range(frames)]
    for h in range(HALVES):
        outs = temporal(temporal_query, temporal_kv, frames, head_dim, h * half, half)
        for s, out in enumerate(outs):
            back[s].append(out if s == 0 else permute(out, behind(s)))

    return output(
        slot_word, after, temporal_out, modulation, back, frames
    )


def solution(mesh):
    return jax.shard_map(
        per_device,
        mesh=mesh,
        in_specs=(
            P(("groups", "patch"), None),
            P(("groups", "patch"), None),
            P(),
            P(),
            P("groups"),
            P("groups"),
            P(),
            P(),
            P(),
            P(),
        ),
        out_specs=P(("groups", "patch"), None),
        check_vma=False,
    )
```

```python
import functools
import math

import jax
import jax.numpy as jnp
import numpy as np
from jax import lax
from jax.experimental import pallas as pl
from jax.experimental.pallas import tpu as pltpu
from jax.sharding import PartitionSpec as P


HEADS = 16
LANES = 128
QUERY_ROWS = 128
PAIR_GROUPS = ((0,), (1,), (2,), (3,))
EMIT = (False, True, False, True)
HALVES = 2


epsilon = 1e-06
bf16 = jnp.bfloat16
f32 = jnp.float32
NT = (((1,), (1,)), ((), ()))


def permute(value, target):
    count = lax.axis_size("patch")
    return lax.ppermute(value, "patch", [(source, target(source)) for source in range(count)])


def partner_slot(slot, step, frames):
    if frames & (frames - 1) == 0:
        return slot ^ step
    return (slot + step) % frames


def source_slot(slot, step, frames):
    if frames & (frames - 1) == 0:
        return slot ^ step
    return (slot - step) % frames


def normalize(activations):
    row_mean = jnp.mean(activations, axis=-1, keepdims=True)
    centered = activations - row_mean
    variance = jnp.mean(centered * centered, axis=-1, keepdims=True)
    return centered * lax.rsqrt(variance + epsilon)


def column_mask(first, width, dtype):
    column = lax.broadcasted_iota(jnp.int32, (1, 2 * LANES), 1)
    inside = jnp.logical_and(column >= first, column < first + width)
    return jnp.where(inside, 1.0, 0.0).astype(dtype)


def softmax_scale(head_dim):
    return math.log2(math.e) * head_dim ** (-0.5)


def vmem_specs(count):
    return [pl.BlockSpec(memory_space=pltpu.VMEM) for _ in range(count)]


def on_chip_call(kernel, operands, shapes, flops, limit_mib, transcendentals=0, scratch=()):
    operands = [pltpu.with_memory_space_constraint(array, pltpu.VMEM) for array in operands]
    return pl.pallas_call(
        kernel,
        out_shape=[pltpu.VMEM(shape, dtype) for shape, dtype in shapes],
        in_specs=vmem_specs(len(operands)),
        out_specs=vmem_specs(len(shapes)),
        scratch_shapes=list(scratch),
        compiler_params=pltpu.CompilerParams(vmem_limit_bytes=limit_mib * 2**20),
        cost_estimate=pl.CostEstimate(
            flops=flops,
            bytes_accessed=sum(array.size * array.dtype.itemsize for array in operands),
            transcendentals=transcendentals,
        ),
    )(*operands)


def chunk_kernel(kv_ref, *refs, tiles):
    out_refs, sems = refs[:-1], refs[-1]
    copies = []
    for chunk, ref in zip(tiles, out_refs):
        for at, tile in enumerate(chunk):
            copies.append(
                pltpu.make_async_copy(
                    kv_ref.at[:, tile * LANES : (tile + 1) * LANES],
                    ref.at[:, at * LANES : (at + 1) * LANES],
                    sems.at[len(copies)],
                )
            )
            copies[-1].start()
    for copy in copies:
        copy.wait()


def stage_chunks(stale_kv, tiles):
    rows = stale_kv.shape[0]
    return pl.pallas_call(
        functools.partial(chunk_kernel, tiles=tiles),
        out_shape=[pltpu.VMEM((rows, len(chunk) * LANES), bf16) for chunk in tiles],
        in_specs=[pl.BlockSpec(memory_space=pltpu.HBM)],
        out_specs=vmem_specs(len(tiles)),
        scratch_shapes=[pltpu.SemaphoreType.DMA((sum(len(chunk) for chunk in tiles),))],
        compiler_params=pltpu.CompilerParams(vmem_limit_bytes=2**20),
        name="chunks",
    )(pltpu.with_memory_space_constraint(stale_kv, pltpu.HBM))


def piece_kernel(slot_ref, tokens_ref, *refs, frames):
    out_refs, sems = refs[:-1], refs[-1]
    piece = tokens_ref.shape[0] // frames
    copies = []
    for step in range(frames):
        row = partner_slot(slot_ref[0], step, frames) * piece
        copies.append(
            pltpu.make_async_copy(
                tokens_ref.at[pl.ds(row, piece), :], out_refs[step], sems.at[step]
            )
        )
        copies[-1].start()
    for copy in copies:
        copy.wait()


def stage_pieces(slot, tokens, frames):
    rows, feature_width = tokens.shape
    return pl.pallas_call(
        functools.partial(piece_kernel, frames=frames),
        out_shape=[pltpu.VMEM((rows // frames, feature_width), bf16) for _ in range(frames)],
        in_specs=[
            pl.BlockSpec(memory_space=pltpu.SMEM),
            pl.BlockSpec(memory_space=pltpu.HBM),
        ],
        out_specs=vmem_specs(frames),
        scratch_shapes=[pltpu.SemaphoreType.DMA((frames,))],
        compiler_params=pltpu.CompilerParams(vmem_limit_bytes=2**20),
        name="pieces",
    )(slot, pltpu.with_memory_space_constraint(tokens, pltpu.HBM))


def modulation_kernel(slot_ref, time_ref, order_ref, rate_ref, table_ref, mix_ref, out_ref, place_ref):
    frames, feature_width = place_ref.shape
    rows = -(-(frames + 1) // 8) * 8
    row = lax.broadcasted_iota(jnp.int32, (rows, 1), 0)
    position = jnp.where(row == frames, time_ref[0], 0)
    for step in range(frames):
        frame = order_ref[source_slot(slot_ref[0], step, frames)]
        position = jnp.where(row == step, frame, position)
    angles = position.astype(f32) * rate_ref[...]
    column = lax.broadcasted_iota(jnp.int32, (rows, feature_width), 1)
    waves = jnp.where(column < feature_width // 2, jnp.sin(angles), jnp.cos(angles))
    place_ref[...] = waves[:frames]
    out_ref[...] = table_ref[...] + mix_ref[...] * waves[frames : frames + 1]


def modulate(slot, timestep, frame_order, mod_table, mod_mix):
    frames, feature_width = frame_order.shape[0], mod_table.shape[1]
    half = feature_width // 2
    rates = np.exp(-math.log(10000.0) * np.arange(half) / half).astype(np.float32)
    operands = [jnp.asarray(np.concatenate([rates, rates])[None]), mod_table, mod_mix]
    operands = [pltpu.with_memory_space_constraint(array, pltpu.VMEM) for array in operands]
    return pl.pallas_call(
        modulation_kernel,
        out_shape=[pltpu.VMEM(mod_table.shape, f32), pltpu.VMEM((frames, feature_width), f32)],
        in_specs=[pl.BlockSpec(memory_space=pltpu.SMEM) for _ in range(3)] + vmem_specs(3),
        out_specs=vmem_specs(2),
        compiler_params=pltpu.CompilerParams(vmem_limit_bytes=2**20),
        name="modulation",
    )(slot, timestep, frame_order, *operands)


def projection_kernel(weight_hbm, *refs, frames, width):
    pieces = refs[:frames]
    modulation_ref, query_ref, kv_ref, weight_ref, sems = refs[frames:]
    padded = query_ref.shape[1]
    parts = (slice(0, padded), slice(padded, weight_ref.shape[0]))
    copies = [
        pltpu.make_async_copy(weight_hbm.at[part, :], weight_ref.at[part, :], sems.at[number])
        for number, part in enumerate(parts)
    ]
    for copy in copies:
        copy.start()
    tokens = jnp.concatenate([ref[...] for ref in pieces], axis=0).astype(f32)
    inputs = normalize(tokens) * (1.0 + modulation_ref[1:2, :]) + modulation_ref[0:1, :]
    inputs = inputs.astype(bf16)
    copies[0].wait()
    query_ref[...] = lax.dot_general(
        inputs, weight_ref[:padded, :], NT, preferred_element_type=f32
    ).astype(bf16)
    copies[1].wait()
    kv_ref[...] = lax.dot_general(
        inputs, weight_ref[width:, :], NT, preferred_element_type=f32
    ).astype(bf16)


def projections(pieces, weight, modulation, width):
    frames = len(pieces)
    piece, feature_width = pieces[0].shape
    padded = -(-width // LANES) * LANES
    rows = frames * piece
    operands = [pltpu.with_memory_space_constraint(weight, pltpu.HBM)]
    operands += [pltpu.with_memory_space_constraint(x, pltpu.VMEM) for x in (*pieces, modulation)]
    return pl.pallas_call(
        functools.partial(projection_kernel, frames=frames, width=width),
        out_shape=[pltpu.VMEM((rows, padded), bf16), pltpu.VMEM((rows, 2 * width), bf16)],
        in_specs=[pl.BlockSpec(memory_space=pltpu.HBM), *vmem_specs(frames + 1)],
        out_specs=vmem_specs(2),
        scratch_shapes=[pltpu.VMEM(weight.shape, bf16), pltpu.SemaphoreType.DMA((2,))],
        compiler_params=pltpu.CompilerParams(vmem_limit_bytes=8 * 2**20),
        cost_estimate=pl.CostEstimate(
            flops=2 * rows * feature_width * 3 * width,
            bytes_accessed=2 * weight.size,
            transcendentals=0,
        ),
        name="projections",
    )(*operands)


def stack_rows(rows, width):
    return rows * width // LANES


def stack(tiles, width):
    rows = tiles[0].shape[0]
    whole = width // LANES
    stacked = list(tiles[:whole])
    if width % LANES:
        fold = tiles[whole]
        lane = lax.broadcasted_iota(jnp.int32, (1, LANES), 1)
        low = jnp.where(lane < LANES // 2, fold[: rows // 2], 0.0)
        high = jnp.where(lane < LANES // 2, fold[rows // 2 :], 0.0)
        stacked.append(low + pltpu.roll(high, LANES // 2, 1))
    return jnp.concatenate(stacked, axis=0).astype(bf16)


def unstack(stacked, rows, width, first, count):
    whole = width // LANES
    tiles = [stacked[t * rows + first : t * rows + first + count, :] for t in range(whole)]
    if width % LANES:
        half = rows // 2
        fold = stacked[whole * rows :, :]
        turned = pltpu.roll(fold.astype(f32), LANES // 2, 1).astype(stacked.dtype)
        both = jnp.concatenate([fold, turned], axis=0)
        if first % half == 0 and count == half:
            both = turned if first else fold
        else:
            both = both[first : first + count]
        tiles.append(both[:, : LANES // 2])
    return jnp.concatenate(tiles, axis=1)


def pair_plan(width, head_dim):
    plan = []
    for first in range(0, width, 2 * head_dim):
        key_tile = first // LANES
        value_tile = (width + first) // LANES
        plan.append(
            (key_tile, first - key_tile * LANES, value_tile, width + first - value_tile * LANES)
        )
    return plan


def group_tiles(width, head_dim):
    plan = pair_plan(width, head_dim)
    seen, groups = set(), []
    for group in PAIR_GROUPS:
        need = []
        for pair in group:
            key_tile, _, value_tile, _ = plan[pair]
            need += [key_tile, key_tile + 1, value_tile, value_tile + 1]
        fresh = sorted(set(need) - seen)
        seen |= set(fresh)
        groups.append(tuple(fresh))
    return groups


def spatial_kernel(*refs, group, frames, head_dim, width, tiles, held, emitted, kept, columns):
    plan = pair_plan(width, head_dim)
    count = len(tiles)
    position = 0
    refs, (scores_ref, weights_ref) = refs[:-2], refs[-2:]
    query_ref, own_ref, peer_ref = refs[:3]
    near_refs = refs[3 : 3 + count]
    far_refs = refs[3 + count : 3 + 2 * count]
    position = 3 + 2 * count
    held_ref = None
    if held:
        held_ref = refs[position]
        position += 1
    out_count = frames if emitted else 0
    out_refs = refs[position : position + out_count]
    kept_ref = refs[position + out_count] if kept else None

    where = {tile: (c, j) for c, chunk in enumerate(tiles) for j, tile in enumerate(chunk)}

    def from_chunks(chunk_refs):
        def load(tile):
            chunk, at = where[tile]
            return chunk_refs[chunk][:, at * LANES : (at + 1) * LANES]

        return load

    def from_whole(ref):
        return lambda tile: ref[:, tile * LANES : (tile + 1) * LANES]

    blocks = [from_whole(own_ref), from_whole(peer_ref), from_chunks(near_refs), from_chunks(far_refs)]
    rows = query_ref.shape[0]
    scale = softmax_scale(head_dim)
    piece = rows // frames

    def two(block, tile):
        return jnp.concatenate([block(tile), block(tile + 1)], axis=1)

    def score(index):
        chunk, pair = tasks[index]
        key_tile, key_lane, _, _ = plan[pair]
        window = query_ref[
            chunk * QUERY_ROWS : (chunk + 1) * QUERY_ROWS, key_tile * LANES : (key_tile + 2) * LANES
        ]
        stacked = jnp.concatenate(
            [
                window * column_mask(key_lane, head_dim, bf16),
                window * column_mask(key_lane + head_dim, head_dim, bf16),
            ],
            axis=0,
        )
        for number, block in enumerate(blocks):
            scores_ref[index % 2, :, number * rows : (number + 1) * rows] = lax.dot_general(
                stacked, two(block, key_tile), NT, preferred_element_type=f32
            )

    def weigh(index):
        totals = []
        for row in range(0, 2 * QUERY_ROWS, 16):
            scores = scores_ref[index % 2, row : row + 16, :]
            top = jnp.max(scores, axis=-1, keepdims=True) * scale
            weights = jnp.exp2(scores * scale - top)
            totals.append(jnp.sum(weights, axis=-1, keepdims=True))
            weights_ref[index % 2, row : row + 16, :] = weights.astype(bf16)
        return jnp.concatenate(totals, axis=0)

    def mix(index, total):
        _, key_lane, value_tile, value_lane = plan[tasks[index][1]]
        mixed = functools.reduce(
            jnp.add,
            [
                jnp.dot(
                    weights_ref[index % 2, :, number * rows : (number + 1) * rows],
                    two(block, value_tile),
                    preferred_element_type=f32,
                )
                for number, block in enumerate(blocks)
            ],
        )
        mixed = mixed / total
        joined = mixed[:QUERY_ROWS] * column_mask(value_lane, head_dim, f32) + mixed[
            QUERY_ROWS:
        ] * column_mask(value_lane + head_dim, head_dim, f32)
        return pltpu.roll(joined, (key_lane - value_lane) % (2 * LANES), 1)

    tasks = [(chunk, pair) for chunk in range(rows // QUERY_ROWS) for pair in group]
    parts = {}

    def finish(index, total):
        chunk, pair = tasks[index]
        joined = mix(index, total)
        tile = plan[pair][0]
        for side in range(2):
            half = joined[:, side * LANES : (side + 1) * LANES]
            parts[tile + side] = parts[tile + side] + half if tile + side in parts else half
        if pair != group[-1]:
            return
        at = chunk * QUERY_ROWS
        for number, tile in enumerate(held):
            old = held_ref[at : at + QUERY_ROWS, number * LANES : (number + 1) * LANES].astype(f32)
            parts[tile] = parts[tile] + old if tile in parts else old
        if kept:
            values = jnp.concatenate([parts[tile] for tile in kept], axis=1)
            kept_ref[at : at + QUERY_ROWS, :] = values.astype(bf16)
        if emitted:
            for sub in range(QUERY_ROWS // piece):
                cut = slice(sub * piece, (sub + 1) * piece)
                out_refs[at // piece + sub][...] = stack(
                    [parts[tile][cut] for tile in emitted], columns
                )
        parts.clear()

    score(0)
    total = None
    for index in range(len(tasks)):
        if index + 1 < len(tasks):
            score(index + 1)
        if index > 0:
            finish(index - 1, total)
        total = weigh(index)
    finish(len(tasks) - 1, total)


def tile_flow(width, head_dim):
    plan = pair_plan(width, head_dim)
    flow, held = [], ()
    for number, group in enumerate(PAIR_GROUPS):
        have = sorted({plan[pair][0] + side for pair in group for side in range(2)} | set(held))
        last = number == len(PAIR_GROUPS) - 1
        complete = [tile for tile in have if last or tile <= plan[group[-1]][0]]
        emitted = tuple(complete) if EMIT[number] else ()
        kept = tuple(tile for tile in have if tile not in emitted)
        flow.append((held, emitted, kept))
        held = kept
    return flow


def emitted_columns(emitted, width):
    return min(width, (emitted[-1] + 1) * LANES) - emitted[0] * LANES if emitted else 0


def group_columns(width, head_dim):
    flow = tile_flow(width, head_dim)
    return tuple(emitted_columns(emitted, width) for _, emitted, _ in flow if emitted)


def spatial_group(number, query, own_kv, peer_kv, near, far, carry, frames, head_dim, width):
    group = PAIR_GROUPS[number]
    held, emitted, kept = tile_flow(width, head_dim)[number]
    tiles = tuple(group_tiles(width, head_dim)[: number + 1])
    rows = query.shape[0]
    shapes = []
    columns = emitted_columns(emitted, width)
    if emitted:
        shapes += [((stack_rows(rows // frames, columns), LANES), bf16) for _ in range(frames)]
    if kept:
        shapes.append(((rows, len(kept) * LANES), bf16))
    operands = [query, own_kv, peer_kv, *near[: number + 1], *far[: number + 1]]
    if held:
        operands.append(carry)
    keys = 4 * rows
    results = on_chip_call(
        functools.partial(
            spatial_kernel,
            group=group,
            frames=frames,
            head_dim=head_dim,
            width=width,
            tiles=tiles,
            held=held,
            emitted=emitted,
            kept=kept,
            columns=columns,
        ),
        operands,
        shapes,
        len(group) * 2 * rows * keys * 256 * 4,
        8,
        len(group) * 2 * rows * keys,
        [
            pltpu.VMEM((2, 2 * QUERY_ROWS, keys), f32),
            pltpu.VMEM((2, 2 * QUERY_ROWS, keys), bf16),
        ],
    )
    results = list(results)
    carry = results.pop() if kept else None
    return results, carry


def joined_rows(tokens_refs, mixed_refs, columns, first, count):
    groups = len(columns)
    piece = tokens_refs[0].shape[0]
    cut = slice(first, first + count)
    tokens = jnp.concatenate([ref[cut, :] for ref in tokens_refs], axis=0).astype(f32)
    mixed = jnp.concatenate(
        [
            jnp.concatenate(
                [
                    unstack(mixed_refs[frame * groups + g][...], piece, columns[g], first, count)
                    for g in range(groups)
                ],
                axis=1,
            )
            for frame in range(len(tokens_refs))
        ],
        axis=0,
    )
    return tokens, mixed


def temporal_kernel(*refs, frames, head_dim, columns, first, piece):
    groups = len(columns)
    tokens_refs = refs[:frames]
    mixed_refs = refs[frames : frames + frames * groups]
    position = frames + frames * groups
    out_weight, qkv_weight, modulation_ref, place_ref = refs[position : position + 4]
    out_refs = refs[position + 4 : position + 4 + frames]
    query_ref, kv_ref = refs[position + 4 + frames :]
    width = out_weight.shape[0]
    tokens, mixed = joined_rows(tokens_refs, mixed_refs, columns, first, piece)
    after = tokens + modulation_ref[2:3, :] * jnp.dot(
        mixed, out_weight[...], preferred_element_type=f32
    )
    normal = normalize(after) * (1.0 + modulation_ref[4:5, :]) + modulation_ref[3:4, :]
    inputs = jnp.concatenate(
        [
            (normal[frame * piece : (frame + 1) * piece] + place_ref[frame : frame + 1, :]).astype(bf16)
            for frame in range(frames)
        ],
        axis=0,
    )
    query_ref[...] = lax.dot_general(
        inputs, qkv_weight[: query_ref.shape[1], :], NT, preferred_element_type=f32
    ).astype(bf16)
    kv_ref[...] = lax.dot_general(
        inputs, qkv_weight[width:, :], NT, preferred_element_type=f32
    ).astype(bf16)

    scale = softmax_scale(head_dim)
    step = max(16, min(piece, LANES // frames))
    block = frames * step
    row_at = lax.broadcasted_iota(jnp.int32, (2 * block, block), 0) % step
    column_at = lax.broadcasted_iota(jnp.int32, (2 * block, block), 1) % step
    same = row_at == column_at
    plan = pair_plan(width, head_dim)

    def window(ref, start, tile):
        return jnp.concatenate(
            [
                ref[
                    frame * piece + start : frame * piece + start + step,
                    tile * LANES : (tile + 2) * LANES,
                ]
                for frame in range(frames)
            ],
            axis=0,
        )

    def score(start, tile, lane):
        queries = window(query_ref, start, tile)
        stacked = jnp.concatenate(
            [
                queries * column_mask(lane, head_dim, bf16),
                queries * column_mask(lane + head_dim, head_dim, bf16),
            ],
            axis=0,
        )
        scores = lax.dot_general(
            stacked, window(kv_ref, start, tile), NT, preferred_element_type=f32
        )
        return jnp.where(same, scores * scale, -jnp.inf)

    def weigh(scores):
        weights = jnp.exp2(scores - jnp.max(scores, axis=-1, keepdims=True))
        return (weights / jnp.sum(weights, axis=-1, keepdims=True)).astype(bf16)

    starts = range(0, piece, step)
    tasks = [(start, *entry) for start in starts for entry in plan]
    scores = [score(start, tile, lane) for start, tile, lane, _, _ in tasks]
    weights = [weigh(value) for value in scores]
    mixed_pairs = [
        jnp.dot(value, window(kv_ref, start, value_tile), preferred_element_type=f32)
        for value, (start, _, _, value_tile, _) in zip(weights, tasks)
    ]
    parts = {start: {} for start in starts}
    for pair, (start, tile, lane, _, value_lane) in zip(mixed_pairs, tasks):
        joined = pair[:block] * column_mask(value_lane, head_dim, f32) + pair[
            block:
        ] * column_mask(value_lane + head_dim, head_dim, f32)
        joined = pltpu.roll(joined, (lane - value_lane) % (2 * LANES), 1)
        have = parts[start]
        for side in range(2):
            half = joined[:, side * LANES : (side + 1) * LANES]
            have[tile + side] = have[tile + side] + half if tile + side in have else half
    for frame in range(frames):
        cut = slice(frame * step, (frame + 1) * step)
        out_refs[frame][...] = stack(
            [
                jnp.concatenate([parts[start][tile][cut] for start in starts], axis=0)
                for tile in sorted(parts[0])
            ],
            width,
        )


def temporal(tokens, mixed, columns, weights, modulation, places, head_dim, first, piece):
    frames = len(tokens)
    spatial_out, temporal_qkv = weights
    width, feature_width = spatial_out.shape
    padded = -(-width // LANES) * LANES
    rows = frames * piece
    return on_chip_call(
        functools.partial(
            temporal_kernel,
            frames=frames,
            head_dim=head_dim,
            columns=columns,
            first=first,
            piece=piece,
        ),
        [
            *tokens,
            *[part for frame in mixed for part in frame],
            spatial_out,
            temporal_qkv,
            modulation,
            places,
        ],
        [((stack_rows(piece, width), LANES), bf16) for _ in range(frames)],
        2 * rows * feature_width * width * 5,
        6,
        rows * 128 * 8,
        [pltpu.VMEM((rows, padded), bf16), pltpu.VMEM((rows, 2 * width), bf16)],
    )


def after_kernel(*refs, frames, columns):
    mixed_end = frames * (1 + len(columns))
    weight_ref, modulation_ref, out_ref = refs[mixed_end:]
    piece = refs[0].shape[0]
    tokens, mixed = joined_rows(refs[:frames], refs[frames:mixed_end], columns, 0, piece)
    out_ref[...] = tokens + modulation_ref[2:3, :] * jnp.dot(
        mixed, weight_ref[...], preferred_element_type=f32
    )


def after_spatial(tokens, mixed, columns, weight, modulation):
    frames = len(tokens)
    width, feature_width = weight.shape
    rows = frames * tokens[0].shape[0]
    return on_chip_call(
        functools.partial(after_kernel, frames=frames, columns=columns),
        [*tokens, *[part for frame in mixed for part in frame], weight, modulation],
        [((rows, feature_width), f32)],
        2 * rows * feature_width * width,
        6,
    )[0]


def output_kernel(slot_ref, after_ref, weight_ref, modulation_ref, *refs, frames, number):
    parts = refs[:frames]
    out_ref, stage_ref, sems = refs[-3:]
    piece = after_ref.shape[0] // frames
    half = piece // HALVES
    first = number * half
    width = weight_ref.shape[0]
    mixed = jnp.concatenate(
        [unstack(ref[...].astype(f32), half, width, 0, half).astype(bf16) for ref in parts], axis=0
    )
    after = jnp.concatenate(
        [after_ref[frame * piece + first : frame * piece + first + half, :] for frame in range(frames)],
        axis=0,
    )
    stage_ref[...] = after + modulation_ref[5:6, :] * jnp.dot(
        mixed, weight_ref[...], preferred_element_type=f32
    )
    copies = []
    for frame in range(frames):
        row = partner_slot(slot_ref[0], frame, frames) * piece + first
        copies.append(
            pltpu.make_async_copy(
                stage_ref.at[frame * half : (frame + 1) * half, :],
                out_ref.at[pl.ds(row, half), :],
                sems.at[frame],
            )
        )
        copies[-1].start()
    for copy in copies:
        copy.wait()


def output(number, slot, after, weight, modulation, parts, result):
    frames = len(parts)
    rows, feature_width = after.shape
    operands = [after, weight, modulation, *parts]
    specs = [pl.BlockSpec(memory_space=pltpu.SMEM), *vmem_specs(len(operands))]
    operands = [pltpu.with_memory_space_constraint(array, pltpu.VMEM) for array in operands]
    aliases = {}
    if result is not None:
        aliases = {len(specs): 0}
        specs.append(pl.BlockSpec(memory_space=pltpu.HBM))
        operands.append(result)
    return pl.pallas_call(
        functools.partial(output_kernel, frames=frames, number=number),
        out_shape=jax.ShapeDtypeStruct((rows, feature_width), f32),
        in_specs=specs,
        out_specs=pl.BlockSpec(memory_space=pltpu.HBM),
        scratch_shapes=[
            pltpu.VMEM((rows // HALVES, feature_width), f32),
            pltpu.SemaphoreType.DMA((frames,)),
        ],
        input_output_aliases=aliases,
        compiler_params=pltpu.CompilerParams(vmem_limit_bytes=4 * 2**20),
    )(slot, *operands)


def per_device(
    tokens,
    stale_kv,
    mod_table,
    mod_mix,
    timestep,
    frame_order,
    spatial_qkv,
    spatial_out,
    temporal_qkv,
    temporal_out,
):
    devices = lax.axis_size("patch")
    frames = devices // 4
    slot = lax.axis_index("patch") // 4
    rows, feature_width = tokens.shape
    width = spatial_out.shape[0]
    head_dim = feature_width // HEADS
    piece = rows // frames

    def other_core(device):
        return device ^ 1

    def other_chip(device):
        return device ^ 2

    def ahead(step):
        return lambda device: partner_slot(device // 4, step, frames) * 4 + device % 4

    def behind(step):
        return lambda device: source_slot(device // 4, step, frames) * 4 + device % 4

    near, far = [], []
    for chunk in stage_chunks(stale_kv, group_tiles(width, head_dim)):
        near.append(permute(chunk, other_chip))
        far.append(permute(near[-1], other_core))
    peer_kv = permute(stale_kv, other_core)

    slot_word = slot.astype(jnp.int32)[None]
    pieces = stage_pieces(slot_word, tokens, frames)
    there = [pieces[0]]
    there += [permute(pieces[s], ahead(s)) for s in range(1, frames)]

    modulation, places = modulate(slot_word, timestep, frame_order, mod_table, mod_mix)
    query, own_kv = projections(
        pieces,
        jnp.swapaxes(spatial_qkv, 1, 2).reshape(3 * width, feature_width),
        modulation,
        width,
    )

    carry = None
    local = [[] for _ in range(frames)]
    sent = [[] for _ in range(frames)]
    for number in range(len(PAIR_GROUPS)):
        outs, carry = spatial_group(
            number, query, own_kv, peer_kv, near, far, carry, frames, head_dim, width
        )
        for s, out in enumerate(outs):
            local[s].append(out)
            sent[s].append(out if s == 0 else permute(out, ahead(s)))

    columns = group_columns(width, head_dim)
    after = after_spatial(pieces, local, columns, spatial_out, modulation)
    weights = (spatial_out, jnp.swapaxes(temporal_qkv, 1, 2).reshape(3 * width, feature_width))
    half = piece // HALVES
    back = []
    for h in range(HALVES):
        outs = temporal(there, sent, columns, weights, modulation, places, head_dim, h * half, half)
        back.append([out if s == 0 else permute(out, behind(s)) for s, out in enumerate(outs)])
    result = None
    for h in range(HALVES):
        result = output(h, slot_word, after, temporal_out, modulation, back[h], result)
    return result


def solution(mesh):
    return jax.shard_map(
        per_device,
        mesh=mesh,
        in_specs=(
            P(("groups", "patch"), None),
            P(("groups", "patch"), None),
            P(),
            P(),
            P("groups"),
            P("groups"),
            P(),
            P(),
            P(),
            P(),
        ),
        out_specs=P(("groups", "patch"), None),
        check_vma=False,
    )
```

```python
import functools
import math

import jax
import jax.numpy as jnp
import numpy as np
from jax import lax
from jax.experimental import pallas as pl
from jax.experimental.pallas import tpu as pltpu
from jax.sharding import PartitionSpec as P


HEADS = 16
LANES = 128
QUERY_ROWS = 128
PAIR_GROUPS = ((0,), (1,), (2,), (3,))
EMIT = (False, False, True, True)
HALVES = 2


epsilon = 1e-06
bf16 = jnp.bfloat16
f32 = jnp.float32
NT = (((1,), (1,)), ((), ()))


def permute(value, target):
    count = lax.axis_size("patch")
    return lax.ppermute(value, "patch", [(source, target(source)) for source in range(count)])


def partner_slot(slot, step, frames):
    if frames & (frames - 1) == 0:
        return slot ^ step
    return (slot + step) % frames


def source_slot(slot, step, frames):
    if frames & (frames - 1) == 0:
        return slot ^ step
    return (slot - step) % frames


def normalize(activations):
    row_mean = jnp.mean(activations, axis=-1, keepdims=True)
    centered = activations - row_mean
    variance = jnp.mean(centered * centered, axis=-1, keepdims=True)
    return centered * lax.rsqrt(variance + epsilon)


def column_mask(first, width, dtype):
    column = lax.broadcasted_iota(jnp.int32, (1, 2 * LANES), 1)
    inside = jnp.logical_and(column >= first, column < first + width)
    return jnp.where(inside, 1.0, 0.0).astype(dtype)


def softmax_scale(head_dim):
    return math.log2(math.e) * head_dim ** (-0.5)


def vmem_specs(count):
    return [pl.BlockSpec(memory_space=pltpu.VMEM) for _ in range(count)]


def on_chip_call(kernel, operands, shapes, flops, limit_mib, transcendentals=0, scratch=()):
    operands = [pltpu.with_memory_space_constraint(array, pltpu.VMEM) for array in operands]
    return pl.pallas_call(
        kernel,
        out_shape=[pltpu.VMEM(shape, dtype) for shape, dtype in shapes],
        in_specs=vmem_specs(len(operands)),
        out_specs=vmem_specs(len(shapes)),
        scratch_shapes=list(scratch),
        compiler_params=pltpu.CompilerParams(vmem_limit_bytes=limit_mib * 2**20),
        cost_estimate=pl.CostEstimate(
            flops=flops,
            bytes_accessed=sum(array.size * array.dtype.itemsize for array in operands),
            transcendentals=transcendentals,
        ),
    )(*operands)


def chunk_kernel(kv_ref, *refs, tiles):
    out_refs, sems = refs[:-1], refs[-1]
    copies = []
    for chunk, ref in zip(tiles, out_refs):
        for at, tile in enumerate(chunk):
            copies.append(
                pltpu.make_async_copy(
                    kv_ref.at[:, tile * LANES : (tile + 1) * LANES],
                    ref.at[:, at * LANES : (at + 1) * LANES],
                    sems.at[len(copies)],
                )
            )
            copies[-1].start()
    for copy in copies:
        copy.wait()


def stage_chunks(stale_kv, tiles):
    rows = stale_kv.shape[0]
    return pl.pallas_call(
        functools.partial(chunk_kernel, tiles=tiles),
        out_shape=[pltpu.VMEM((rows, len(chunk) * LANES), bf16) for chunk in tiles],
        in_specs=[pl.BlockSpec(memory_space=pltpu.HBM)],
        out_specs=vmem_specs(len(tiles)),
        scratch_shapes=[pltpu.SemaphoreType.DMA((sum(len(chunk) for chunk in tiles),))],
        compiler_params=pltpu.CompilerParams(vmem_limit_bytes=2**20),
        name="chunks",
    )(pltpu.with_memory_space_constraint(stale_kv, pltpu.HBM))


def piece_kernel(slot_ref, tokens_ref, *refs, frames):
    out_refs, sems = refs[:-1], refs[-1]
    piece = tokens_ref.shape[0] // frames
    copies = []
    for step in range(frames):
        row = partner_slot(slot_ref[0], step, frames) * piece
        copies.append(
            pltpu.make_async_copy(
                tokens_ref.at[pl.ds(row, piece), :], out_refs[step], sems.at[step]
            )
        )
        copies[-1].start()
    for copy in copies:
        copy.wait()


def stage_pieces(slot, tokens, frames):
    rows, feature_width = tokens.shape
    return pl.pallas_call(
        functools.partial(piece_kernel, frames=frames),
        out_shape=[pltpu.VMEM((rows // frames, feature_width), bf16) for _ in range(frames)],
        in_specs=[
            pl.BlockSpec(memory_space=pltpu.SMEM),
            pl.BlockSpec(memory_space=pltpu.HBM),
        ],
        out_specs=vmem_specs(frames),
        scratch_shapes=[pltpu.SemaphoreType.DMA((frames,))],
        compiler_params=pltpu.CompilerParams(vmem_limit_bytes=2**20),
        name="pieces",
    )(slot, pltpu.with_memory_space_constraint(tokens, pltpu.HBM))


def projection_kernel(slot_ref, time_ref, order_ref, weight_hbm, *refs, frames, width):
    rate_ref, table_ref, mix_ref = refs[:3]
    pieces = refs[3 : 3 + frames]
    query_ref, kv_ref, modulation_ref, place_ref, weight_ref, sems = refs[3 + frames :]
    padded = query_ref.shape[1]
    feature_width = place_ref.shape[1]
    middle = width + padded
    parts = (slice(0, padded), slice(padded, middle), slice(middle, weight_ref.shape[0]))
    copies = [
        pltpu.make_async_copy(weight_hbm.at[part, :], weight_ref.at[part, :], sems.at[number])
        for number, part in enumerate(parts)
    ]
    for copy in copies:
        copy.start()

    rows = -(-(frames + 1) // 8) * 8
    row = lax.broadcasted_iota(jnp.int32, (rows, 1), 0)
    position = jnp.where(row == frames, time_ref[0], 0)
    for step in range(frames):
        frame = order_ref[source_slot(slot_ref[0], step, frames)]
        position = jnp.where(row == step, frame, position)
    angles = position.astype(f32) * rate_ref[...]
    column = lax.broadcasted_iota(jnp.int32, (rows, feature_width), 1)
    waves = jnp.where(column < feature_width // 2, jnp.sin(angles), jnp.cos(angles))
    place_ref[...] = waves[:frames]
    modulation = table_ref[...] + mix_ref[...] * waves[frames : frames + 1]
    modulation_ref[...] = modulation

    tokens = jnp.concatenate([ref[...] for ref in pieces], axis=0).astype(f32)
    inputs = normalize(tokens) * (1.0 + modulation[1:2, :]) + modulation[0:1, :]
    inputs = inputs.astype(bf16)

    def project(first, last):
        return lax.dot_general(
            inputs, weight_ref[first:last, :], NT, preferred_element_type=f32
        ).astype(bf16)

    copies[0].wait()
    query_ref[...] = project(0, padded)
    copies[1].wait()
    kv_ref[:, :padded] = project(width, middle)
    copies[2].wait()
    kv_ref[:, padded:] = project(middle, weight_ref.shape[0])


def projections(slot, timestep, frame_order, weight, mod_table, mod_mix, pieces, width):
    frames = len(pieces)
    piece, feature_width = pieces[0].shape
    padded = -(-width // LANES) * LANES
    rows = frames * piece
    half = feature_width // 2
    rates = np.exp(-math.log(10000.0) * np.arange(half) / half).astype(np.float32)
    rates = jnp.asarray(np.concatenate([rates, rates])[None])
    operands = [pltpu.with_memory_space_constraint(weight, pltpu.HBM)]
    operands += [
        pltpu.with_memory_space_constraint(x, pltpu.VMEM)
        for x in (rates, mod_table, mod_mix, *pieces)
    ]
    return pl.pallas_call(
        functools.partial(projection_kernel, frames=frames, width=width),
        out_shape=[
            pltpu.VMEM((rows, padded), bf16),
            pltpu.VMEM((rows, 2 * width), bf16),
            pltpu.VMEM(mod_table.shape, f32),
            pltpu.VMEM((frames, feature_width), f32),
        ],
        in_specs=[
            *[pl.BlockSpec(memory_space=pltpu.SMEM) for _ in range(3)],
            pl.BlockSpec(memory_space=pltpu.HBM),
            *vmem_specs(3 + frames),
        ],
        out_specs=vmem_specs(4),
        scratch_shapes=[pltpu.VMEM(weight.shape, bf16), pltpu.SemaphoreType.DMA((3,))],
        compiler_params=pltpu.CompilerParams(vmem_limit_bytes=8 * 2**20),
        cost_estimate=pl.CostEstimate(
            flops=2 * rows * feature_width * 3 * width,
            bytes_accessed=2 * weight.size,
            transcendentals=0,
        ),
        name="projections",
    )(slot, timestep, frame_order, *operands)


def stack_rows(rows, width):
    return rows * width // LANES


def stack(tiles, width):
    rows = tiles[0].shape[0]
    whole = width // LANES
    stacked = list(tiles[:whole])
    if width % LANES:
        fold = tiles[whole]
        lane = lax.broadcasted_iota(jnp.int32, (1, LANES), 1)
        low = jnp.where(lane < LANES // 2, fold[: rows // 2], 0.0)
        high = jnp.where(lane < LANES // 2, fold[rows // 2 :], 0.0)
        stacked.append(low + pltpu.roll(high, LANES // 2, 1))
    return jnp.concatenate(stacked, axis=0).astype(bf16)


def unstack(stacked, rows, width, first, count):
    whole = width // LANES
    tiles = [stacked[t * rows + first : t * rows + first + count, :] for t in range(whole)]
    if width % LANES:
        half = rows // 2
        fold = stacked[whole * rows :, :]
        turned = pltpu.roll(fold.astype(f32), LANES // 2, 1).astype(stacked.dtype)
        both = jnp.concatenate([fold, turned], axis=0)
        if first % half == 0 and count == half:
            both = turned if first else fold
        else:
            both = both[first : first + count]
        tiles.append(both[:, : LANES // 2])
    return jnp.concatenate(tiles, axis=1)


def pair_plan(width, head_dim):
    plan = []
    for first in range(0, width, 2 * head_dim):
        key_tile = first // LANES
        value_tile = (width + first) // LANES
        plan.append(
            (key_tile, first - key_tile * LANES, value_tile, width + first - value_tile * LANES)
        )
    return plan


def group_tiles(width, head_dim):
    plan = pair_plan(width, head_dim)
    seen, groups = set(), []
    for group in PAIR_GROUPS:
        need = []
        for pair in group:
            key_tile, _, value_tile, _ = plan[pair]
            need += [key_tile, key_tile + 1, value_tile, value_tile + 1]
        fresh = sorted(set(need) - seen)
        seen |= set(fresh)
        groups.append(tuple(fresh))
    return groups


def spatial_kernel(*refs, group, frames, head_dim, width, tiles, held, emitted, kept, columns):
    plan = pair_plan(width, head_dim)
    count = len(tiles)
    position = 0
    refs, (scores_ref, weights_ref) = refs[:-2], refs[-2:]
    query_ref, own_ref, peer_ref = refs[:3]
    near_refs = refs[3 : 3 + count]
    far_refs = refs[3 + count : 3 + 2 * count]
    position = 3 + 2 * count
    held_ref = None
    if held:
        held_ref = refs[position]
        position += 1
    out_count = frames if emitted else 0
    out_refs = refs[position : position + out_count]
    kept_ref = refs[position + out_count] if kept else None

    where = {tile: (c, j) for c, chunk in enumerate(tiles) for j, tile in enumerate(chunk)}

    def from_chunks(chunk_refs):
        def load(tile):
            chunk, at = where[tile]
            return chunk_refs[chunk][:, at * LANES : (at + 1) * LANES]

        return load

    def from_whole(ref):
        return lambda tile: ref[:, tile * LANES : (tile + 1) * LANES]

    blocks = [from_whole(own_ref), from_whole(peer_ref), from_chunks(near_refs), from_chunks(far_refs)]
    rows = query_ref.shape[0]
    scale = softmax_scale(head_dim)
    piece = rows // frames

    def two(block, tile):
        return jnp.concatenate([block(tile), block(tile + 1)], axis=1)

    def score(index):
        chunk, pair = tasks[index]
        key_tile, key_lane, _, _ = plan[pair]
        window = query_ref[
            chunk * QUERY_ROWS : (chunk + 1) * QUERY_ROWS, key_tile * LANES : (key_tile + 2) * LANES
        ]
        stacked = jnp.concatenate(
            [
                window * column_mask(key_lane, head_dim, bf16),
                window * column_mask(key_lane + head_dim, head_dim, bf16),
            ],
            axis=0,
        )
        for number, block in enumerate(blocks):
            scores_ref[index % 2, :, number * rows : (number + 1) * rows] = lax.dot_general(
                stacked, two(block, key_tile), NT, preferred_element_type=f32
            )

    def weigh(index):
        totals = []
        for row in range(0, 2 * QUERY_ROWS, 16):
            scores = scores_ref[index % 2, row : row + 16, :]
            top = jnp.max(scores, axis=-1, keepdims=True) * scale
            weights = jnp.exp2(scores * scale - top)
            totals.append(jnp.sum(weights, axis=-1, keepdims=True))
            weights_ref[index % 2, row : row + 16, :] = weights.astype(bf16)
        return jnp.concatenate(totals, axis=0)

    def mix(index, total):
        _, key_lane, value_tile, value_lane = plan[tasks[index][1]]
        mixed = functools.reduce(
            jnp.add,
            [
                jnp.dot(
                    weights_ref[index % 2, :, number * rows : (number + 1) * rows],
                    two(block, value_tile),
                    preferred_element_type=f32,
                )
                for number, block in enumerate(blocks)
            ],
        )
        mixed = mixed / total
        joined = mixed[:QUERY_ROWS] * column_mask(value_lane, head_dim, f32) + mixed[
            QUERY_ROWS:
        ] * column_mask(value_lane + head_dim, head_dim, f32)
        return pltpu.roll(joined, (key_lane - value_lane) % (2 * LANES), 1)

    tasks = [(chunk, pair) for chunk in range(rows // QUERY_ROWS) for pair in group]
    parts = {}

    def finish(index, total):
        chunk, pair = tasks[index]
        joined = mix(index, total)
        tile = plan[pair][0]
        for side in range(2):
            half = joined[:, side * LANES : (side + 1) * LANES]
            parts[tile + side] = parts[tile + side] + half if tile + side in parts else half
        if pair != group[-1]:
            return
        at = chunk * QUERY_ROWS
        for number, tile in enumerate(held):
            old = held_ref[at : at + QUERY_ROWS, number * LANES : (number + 1) * LANES].astype(f32)
            parts[tile] = parts[tile] + old if tile in parts else old
        if kept:
            values = jnp.concatenate([parts[tile] for tile in kept], axis=1)
            kept_ref[at : at + QUERY_ROWS, :] = values.astype(bf16)
        if emitted:
            for sub in range(QUERY_ROWS // piece):
                cut = slice(sub * piece, (sub + 1) * piece)
                out_refs[at // piece + sub][...] = stack(
                    [parts[tile][cut] for tile in emitted], columns
                )
        parts.clear()

    score(0)
    total = None
    for index in range(len(tasks)):
        if index + 1 < len(tasks):
            score(index + 1)
        if index > 0:
            finish(index - 1, total)
        total = weigh(index)
    finish(len(tasks) - 1, total)


def tile_flow(width, head_dim):
    plan = pair_plan(width, head_dim)
    flow, held = [], ()
    for number, group in enumerate(PAIR_GROUPS):
        have = sorted({plan[pair][0] + side for pair in group for side in range(2)} | set(held))
        last = number == len(PAIR_GROUPS) - 1
        complete = [tile for tile in have if last or tile <= plan[group[-1]][0]]
        emitted = tuple(complete) if EMIT[number] else ()
        kept = tuple(tile for tile in have if tile not in emitted)
        flow.append((held, emitted, kept))
        held = kept
    return flow


def emitted_columns(emitted, width):
    return min(width, (emitted[-1] + 1) * LANES) - emitted[0] * LANES if emitted else 0


def group_columns(width, head_dim):
    flow = tile_flow(width, head_dim)
    return tuple(emitted_columns(emitted, width) for _, emitted, _ in flow if emitted)


def spatial_group(number, query, own_kv, peer_kv, near, far, carry, frames, head_dim, width):
    group = PAIR_GROUPS[number]
    held, emitted, kept = tile_flow(width, head_dim)[number]
    tiles = tuple(group_tiles(width, head_dim)[: number + 1])
    rows = query.shape[0]
    shapes = []
    columns = emitted_columns(emitted, width)
    if emitted:
        shapes += [((stack_rows(rows // frames, columns), LANES), bf16) for _ in range(frames)]
    if kept:
        shapes.append(((rows, len(kept) * LANES), bf16))
    operands = [query, own_kv, peer_kv, *near[: number + 1], *far[: number + 1]]
    if held:
        operands.append(carry)
    keys = 4 * rows
    results = on_chip_call(
        functools.partial(
            spatial_kernel,
            group=group,
            frames=frames,
            head_dim=head_dim,
            width=width,
            tiles=tiles,
            held=held,
            emitted=emitted,
            kept=kept,
            columns=columns,
        ),
        operands,
        shapes,
        len(group) * 2 * rows * keys * 256 * 4,
        8,
        len(group) * 2 * rows * keys,
        [
            pltpu.VMEM((2, 2 * QUERY_ROWS, keys), f32),
            pltpu.VMEM((2, 2 * QUERY_ROWS, keys), bf16),
        ],
    )
    results = list(results)
    carry = results.pop() if kept else None
    return results, carry


def joined_rows(tokens_refs, mixed_refs, columns, first, count):
    groups = len(columns)
    piece = tokens_refs[0].shape[0]
    cut = slice(first, first + count)
    tokens = jnp.concatenate([ref[cut, :] for ref in tokens_refs], axis=0).astype(f32)
    mixed = jnp.concatenate(
        [
            jnp.concatenate(
                [
                    unstack(mixed_refs[frame * groups + g][...], piece, columns[g], first, count)
                    for g in range(groups)
                ],
                axis=1,
            )
            for frame in range(len(tokens_refs))
        ],
        axis=0,
    )
    return tokens, mixed


def temporal_kernel(*refs, frames, head_dim, columns, first, piece):
    groups = len(columns)
    tokens_refs = refs[:frames]
    mixed_refs = refs[frames : frames + frames * groups]
    position = frames + frames * groups
    out_weight, qkv_weight, modulation_ref, place_ref = refs[position : position + 4]
    out_refs = refs[position + 4 : position + 4 + frames]
    query_ref, kv_ref = refs[position + 4 + frames :]
    width = out_weight.shape[0]
    tokens, mixed = joined_rows(tokens_refs, mixed_refs, columns, first, piece)
    after = tokens + modulation_ref[2:3, :] * jnp.dot(
        mixed, out_weight[...], preferred_element_type=f32
    )
    normal = normalize(after) * (1.0 + modulation_ref[4:5, :]) + modulation_ref[3:4, :]
    inputs = jnp.concatenate(
        [
            (normal[frame * piece : (frame + 1) * piece] + place_ref[frame : frame + 1, :]).astype(bf16)
            for frame in range(frames)
        ],
        axis=0,
    )
    query_ref[...] = lax.dot_general(
        inputs, qkv_weight[: query_ref.shape[1], :], NT, preferred_element_type=f32
    ).astype(bf16)
    kv_ref[...] = lax.dot_general(
        inputs, qkv_weight[width:, :], NT, preferred_element_type=f32
    ).astype(bf16)

    scale = softmax_scale(head_dim)
    step = max(16, min(piece, LANES // frames))
    block = frames * step
    row_at = lax.broadcasted_iota(jnp.int32, (2 * block, block), 0) % step
    column_at = lax.broadcasted_iota(jnp.int32, (2 * block, block), 1) % step
    same = row_at == column_at
    plan = pair_plan(width, head_dim)

    def window(ref, start, tile):
        return jnp.concatenate(
            [
                ref[
                    frame * piece + start : frame * piece + start + step,
                    tile * LANES : (tile + 2) * LANES,
                ]
                for frame in range(frames)
            ],
            axis=0,
        )

    def score(start, tile, lane):
        queries = window(query_ref, start, tile)
        stacked = jnp.concatenate(
            [
                queries * column_mask(lane, head_dim, bf16),
                queries * column_mask(lane + head_dim, head_dim, bf16),
            ],
            axis=0,
        )
        scores = lax.dot_general(
            stacked, window(kv_ref, start, tile), NT, preferred_element_type=f32
        )
        return jnp.where(same, scores * scale, -jnp.inf)

    def weigh(scores):
        weights = jnp.exp2(scores - jnp.max(scores, axis=-1, keepdims=True))
        return (weights / jnp.sum(weights, axis=-1, keepdims=True)).astype(bf16)

    starts = range(0, piece, step)
    tasks = [(start, *entry) for start in starts for entry in plan]
    scores = [score(start, tile, lane) for start, tile, lane, _, _ in tasks]
    weights = [weigh(value) for value in scores]
    mixed_pairs = [
        jnp.dot(value, window(kv_ref, start, value_tile), preferred_element_type=f32)
        for value, (start, _, _, value_tile, _) in zip(weights, tasks)
    ]
    parts = {start: {} for start in starts}
    for pair, (start, tile, lane, _, value_lane) in zip(mixed_pairs, tasks):
        joined = pair[:block] * column_mask(value_lane, head_dim, f32) + pair[
            block:
        ] * column_mask(value_lane + head_dim, head_dim, f32)
        joined = pltpu.roll(joined, (lane - value_lane) % (2 * LANES), 1)
        have = parts[start]
        for side in range(2):
            half = joined[:, side * LANES : (side + 1) * LANES]
            have[tile + side] = have[tile + side] + half if tile + side in have else half
    for frame in range(frames):
        cut = slice(frame * step, (frame + 1) * step)
        out_refs[frame][...] = stack(
            [
                jnp.concatenate([parts[start][tile][cut] for start in starts], axis=0)
                for tile in sorted(parts[0])
            ],
            width,
        )


def temporal(tokens, mixed, columns, weights, modulation, places, head_dim, first, piece):
    frames = len(tokens)
    spatial_out, temporal_qkv = weights
    width, feature_width = spatial_out.shape
    padded = -(-width // LANES) * LANES
    rows = frames * piece
    return on_chip_call(
        functools.partial(
            temporal_kernel,
            frames=frames,
            head_dim=head_dim,
            columns=columns,
            first=first,
            piece=piece,
        ),
        [
            *tokens,
            *[part for frame in mixed for part in frame],
            spatial_out,
            temporal_qkv,
            modulation,
            places,
        ],
        [((stack_rows(piece, width), LANES), bf16) for _ in range(frames)],
        2 * rows * feature_width * width * 5,
        6,
        rows * 128 * 8,
        [pltpu.VMEM((rows, padded), bf16), pltpu.VMEM((rows, 2 * width), bf16)],
    )


def after_kernel(*refs, frames, columns):
    mixed_end = frames * (1 + len(columns))
    weight_ref, modulation_ref, out_ref = refs[mixed_end:]
    piece = refs[0].shape[0]
    tokens, mixed = joined_rows(refs[:frames], refs[frames:mixed_end], columns, 0, piece)
    out_ref[...] = tokens + modulation_ref[2:3, :] * jnp.dot(
        mixed, weight_ref[...], preferred_element_type=f32
    )


def after_spatial(tokens, mixed, columns, weight, modulation):
    frames = len(tokens)
    width, feature_width = weight.shape
    rows = frames * tokens[0].shape[0]
    return on_chip_call(
        functools.partial(after_kernel, frames=frames, columns=columns),
        [*tokens, *[part for frame in mixed for part in frame], weight, modulation],
        [((rows, feature_width), f32)],
        2 * rows * feature_width * width,
        6,
    )[0]


def output_kernel(slot_ref, after_ref, weight_ref, modulation_ref, *refs, frames, number):
    parts = refs[:frames]
    out_ref, stage_ref, sems = refs[-3:]
    piece = after_ref.shape[0] // frames
    half = piece // HALVES
    first = number * half
    width = weight_ref.shape[0]
    mixed = jnp.concatenate(
        [unstack(ref[...].astype(f32), half, width, 0, half).astype(bf16) for ref in parts], axis=0
    )
    after = jnp.concatenate(
        [after_ref[frame * piece + first : frame * piece + first + half, :] for frame in range(frames)],
        axis=0,
    )
    stage_ref[...] = after + modulation_ref[5:6, :] * jnp.dot(
        mixed, weight_ref[...], preferred_element_type=f32
    )
    copies = []
    for frame in range(frames):
        row = partner_slot(slot_ref[0], frame, frames) * piece + first
        copies.append(
            pltpu.make_async_copy(
                stage_ref.at[frame * half : (frame + 1) * half, :],
                out_ref.at[pl.ds(row, half), :],
                sems.at[frame],
            )
        )
        copies[-1].start()
    for copy in copies:
        copy.wait()


def output(number, slot, after, weight, modulation, parts, result):
    frames = len(parts)
    rows, feature_width = after.shape
    operands = [after, weight, modulation, *parts]
    specs = [pl.BlockSpec(memory_space=pltpu.SMEM), *vmem_specs(len(operands))]
    operands = [pltpu.with_memory_space_constraint(array, pltpu.VMEM) for array in operands]
    aliases = {}
    if result is not None:
        aliases = {len(specs): 0}
        specs.append(pl.BlockSpec(memory_space=pltpu.HBM))
        operands.append(result)
    return pl.pallas_call(
        functools.partial(output_kernel, frames=frames, number=number),
        out_shape=jax.ShapeDtypeStruct((rows, feature_width), f32),
        in_specs=specs,
        out_specs=pl.BlockSpec(memory_space=pltpu.HBM),
        scratch_shapes=[
            pltpu.VMEM((rows // HALVES, feature_width), f32),
            pltpu.SemaphoreType.DMA((frames,)),
        ],
        input_output_aliases=aliases,
        compiler_params=pltpu.CompilerParams(vmem_limit_bytes=4 * 2**20),
    )(slot, *operands)


def per_device(
    tokens,
    stale_kv,
    mod_table,
    mod_mix,
    timestep,
    frame_order,
    spatial_qkv,
    spatial_out,
    temporal_qkv,
    temporal_out,
):
    devices = lax.axis_size("patch")
    frames = devices // 4
    slot = lax.axis_index("patch") // 4
    rows, feature_width = tokens.shape
    width = spatial_out.shape[0]
    head_dim = feature_width // HEADS
    piece = rows // frames

    def other_core(device):
        return device ^ 1

    def other_chip(device):
        return device ^ 2

    def ahead(step):
        return lambda device: partner_slot(device // 4, step, frames) * 4 + device % 4

    def behind(step):
        return lambda device: source_slot(device // 4, step, frames) * 4 + device % 4

    near, far = [], []
    for chunk in stage_chunks(stale_kv, group_tiles(width, head_dim)):
        near.append(permute(chunk, other_chip))
        far.append(permute(near[-1], other_core))
    peer_kv = permute(stale_kv, other_core)

    slot_word = slot.astype(jnp.int32)[None]
    pieces = stage_pieces(slot_word, tokens, frames)
    there = [pieces[0]]
    there += [permute(pieces[s], ahead(s)) for s in range(1, frames)]

    query, own_kv, modulation, places = projections(
        slot_word,
        timestep,
        frame_order,
        jnp.swapaxes(spatial_qkv, 1, 2).reshape(3 * width, feature_width),
        mod_table,
        mod_mix,
        pieces,
        width,
    )

    carry = None
    local = [[] for _ in range(frames)]
    sent = [[] for _ in range(frames)]
    for number in range(len(PAIR_GROUPS)):
        outs, carry = spatial_group(
            number, query, own_kv, peer_kv, near, far, carry, frames, head_dim, width
        )
        for s, out in enumerate(outs):
            local[s].append(out)
            sent[s].append(out if s == 0 else permute(out, ahead(s)))

    columns = group_columns(width, head_dim)
    after = after_spatial(pieces, local, columns, spatial_out, modulation)
    weights = (spatial_out, jnp.swapaxes(temporal_qkv, 1, 2).reshape(3 * width, feature_width))
    half = piece // HALVES
    back = []
    for h in range(HALVES):
        outs = temporal(there, sent, columns, weights, modulation, places, head_dim, h * half, half)
        back.append([out if s == 0 else permute(out, behind(s)) for s, out in enumerate(outs)])
    result = None
    for h in range(HALVES):
        result = output(h, slot_word, after, temporal_out, modulation, back[h], result)
    return result


def solution(mesh):
    return jax.shard_map(
        per_device,
        mesh=mesh,
        in_specs=(
            P(("groups", "patch"), None),
            P(("groups", "patch"), None),
            P(),
            P(),
            P("groups"),
            P("groups"),
            P(),
            P(),
            P(),
            P(),
        ),
        out_specs=P(("groups", "patch"), None),
        check_vma=False,
    )
```

```python
import functools
import math

import jax
import jax.numpy as jnp
import numpy as np
from jax import lax
from jax.experimental import pallas as pl
from jax.experimental.pallas import tpu as pltpu
from jax.sharding import PartitionSpec as P


HEADS = 16
LANES = 128
QUERY_ROWS = 128
STRIP = 16
PAIR_GROUPS = ((0,), (1,), (2, 3))
EMIT = (False, True, True)
HALVES = 2


epsilon = 1e-06
bf16 = jnp.bfloat16
f32 = jnp.float32
NT = (((1,), (1,)), ((), ()))


def permute(value, target):
    count = lax.axis_size("patch")
    return lax.ppermute(value, "patch", [(source, target(source)) for source in range(count)])


def partner_slot(slot, step, frames):
    if frames & (frames - 1) == 0:
        return slot ^ step
    return (slot + step) % frames


def source_slot(slot, step, frames):
    if frames & (frames - 1) == 0:
        return slot ^ step
    return (slot - step) % frames


def normalize(activations):
    row_mean = jnp.mean(activations, axis=-1, keepdims=True)
    centered = activations - row_mean
    variance = jnp.mean(centered * centered, axis=-1, keepdims=True)
    return centered * lax.rsqrt(variance + epsilon)


def column_mask(first, width, dtype):
    column = lax.broadcasted_iota(jnp.int32, (1, 2 * LANES), 1)
    inside = jnp.logical_and(column >= first, column < first + width)
    return jnp.where(inside, 1.0, 0.0).astype(dtype)


def softmax_scale(head_dim):
    return math.log2(math.e) * head_dim ** (-0.5)


def vmem_specs(count):
    return [pl.BlockSpec(memory_space=pltpu.VMEM) for _ in range(count)]


def on_chip_call(kernel, operands, shapes, flops, limit_mib, transcendentals=0, scratch=()):
    operands = [pltpu.with_memory_space_constraint(array, pltpu.VMEM) for array in operands]
    return pl.pallas_call(
        kernel,
        out_shape=[pltpu.VMEM(shape, dtype) for shape, dtype in shapes],
        in_specs=vmem_specs(len(operands)),
        out_specs=vmem_specs(len(shapes)),
        scratch_shapes=list(scratch),
        compiler_params=pltpu.CompilerParams(vmem_limit_bytes=limit_mib * 2**20),
        cost_estimate=pl.CostEstimate(
            flops=flops,
            bytes_accessed=sum(array.size * array.dtype.itemsize for array in operands),
            transcendentals=transcendentals,
        ),
    )(*operands)


def chunk_kernel(kv_ref, *refs, tiles):
    out_refs, sems = refs[:-1], refs[-1]
    copies = []
    for chunk, ref in zip(tiles, out_refs):
        for at, tile in enumerate(chunk):
            copies.append(
                pltpu.make_async_copy(
                    kv_ref.at[:, tile * LANES : (tile + 1) * LANES],
                    ref.at[:, at * LANES : (at + 1) * LANES],
                    sems.at[len(copies)],
                )
            )
            copies[-1].start()
    for copy in copies:
        copy.wait()


def stage_chunks(stale_kv, tiles):
    rows = stale_kv.shape[0]
    return pl.pallas_call(
        functools.partial(chunk_kernel, tiles=tiles),
        out_shape=[pltpu.VMEM((rows, len(chunk) * LANES), bf16) for chunk in tiles],
        in_specs=[pl.BlockSpec(memory_space=pltpu.HBM)],
        out_specs=vmem_specs(len(tiles)),
        scratch_shapes=[pltpu.SemaphoreType.DMA((sum(len(chunk) for chunk in tiles),))],
        compiler_params=pltpu.CompilerParams(vmem_limit_bytes=2**20),
        name="chunks",
    )(pltpu.with_memory_space_constraint(stale_kv, pltpu.HBM))


def piece_kernel(slot_ref, tokens_ref, *refs, frames):
    out_refs, sems = refs[:-1], refs[-1]
    piece = tokens_ref.shape[0] // frames
    copies = []
    for step in range(frames):
        row = partner_slot(slot_ref[0], step, frames) * piece
        copies.append(
            pltpu.make_async_copy(
                tokens_ref.at[pl.ds(row, piece), :], out_refs[step], sems.at[step]
            )
        )
        copies[-1].start()
    for copy in copies:
        copy.wait()


def stage_pieces(slot, tokens, frames):
    rows, feature_width = tokens.shape
    return pl.pallas_call(
        functools.partial(piece_kernel, frames=frames),
        out_shape=[pltpu.VMEM((rows // frames, feature_width), bf16) for _ in range(frames)],
        in_specs=[
            pl.BlockSpec(memory_space=pltpu.SMEM),
            pl.BlockSpec(memory_space=pltpu.HBM),
        ],
        out_specs=vmem_specs(frames),
        scratch_shapes=[pltpu.SemaphoreType.DMA((frames,))],
        compiler_params=pltpu.CompilerParams(vmem_limit_bytes=2**20),
        name="pieces",
    )(slot, pltpu.with_memory_space_constraint(tokens, pltpu.HBM))


def projection_kernel(slot_ref, time_ref, order_ref, weight_hbm, *refs, frames, width):
    rate_ref, table_ref, mix_ref = refs[:3]
    pieces = refs[3 : 3 + frames]
    query_ref, kv_ref, modulation_ref, place_ref = refs[3 + frames : 7 + frames]
    weight_ref, inputs_ref, sems = refs[7 + frames :]
    padded = query_ref.shape[1]
    middle = width + padded
    parts = (slice(0, padded), slice(padded, middle), slice(middle, weight_ref.shape[0]))
    copies = [
        pltpu.make_async_copy(weight_hbm.at[part, :], weight_ref.at[part, :], sems.at[number])
        for number, part in enumerate(parts)
    ]
    for copy in copies:
        copy.start()

    rows = -(-(frames + 1) // 8) * 8
    row = lax.broadcasted_iota(jnp.int32, (rows, 1), 0)
    position = jnp.where(row == frames, time_ref[0], 0)
    for step in range(frames):
        frame = order_ref[source_slot(slot_ref[0], step, frames)]
        position = jnp.where(row == step, frame, position)
    angles = position.astype(f32) * rate_ref[...]
    waves = jnp.concatenate([jnp.sin(angles), jnp.cos(angles)], axis=1)
    place_ref[...] = waves[:frames]
    modulation = table_ref[...] + mix_ref[...] * waves[frames : frames + 1]
    modulation_ref[...] = modulation

    piece = pieces[0].shape[0]
    gain, shift = 1.0 + modulation[1:2, :], modulation[0:1, :]
    for row in range(0, inputs_ref.shape[0], STRIP):
        at = row % piece
        tokens = pieces[row // piece][at : at + STRIP, :].astype(f32)
        inputs_ref[row : row + STRIP, :] = (normalize(tokens) * gain + shift).astype(bf16)
    inputs = inputs_ref[...]

    def project(first, last):
        return lax.dot_general(
            inputs, weight_ref[first:last, :], NT, preferred_element_type=f32
        ).astype(bf16)

    copies[0].wait()
    query_ref[...] = project(0, padded)
    copies[1].wait()
    kv_ref[:, :padded] = project(width, middle)
    copies[2].wait()
    kv_ref[:, padded:] = project(middle, weight_ref.shape[0])


def projections(slot, timestep, frame_order, weight, mod_table, mod_mix, pieces, width):
    frames = len(pieces)
    piece, feature_width = pieces[0].shape
    padded = -(-width // LANES) * LANES
    rows = frames * piece
    half = feature_width // 2
    rates = np.exp(-math.log(10000.0) * np.arange(half) / half).astype(np.float32)
    rates = jnp.asarray(rates[None])
    operands = [pltpu.with_memory_space_constraint(weight, pltpu.HBM)]
    operands += [
        pltpu.with_memory_space_constraint(x, pltpu.VMEM)
        for x in (rates, mod_table, mod_mix, *pieces)
    ]
    return pl.pallas_call(
        functools.partial(projection_kernel, frames=frames, width=width),
        out_shape=[
            pltpu.VMEM((rows, padded), bf16),
            pltpu.VMEM((rows, 2 * width), bf16),
            pltpu.VMEM(mod_table.shape, f32),
            pltpu.VMEM((frames, feature_width), f32),
        ],
        in_specs=[
            *[pl.BlockSpec(memory_space=pltpu.SMEM) for _ in range(3)],
            pl.BlockSpec(memory_space=pltpu.HBM),
            *vmem_specs(3 + frames),
        ],
        out_specs=vmem_specs(4),
        scratch_shapes=[
            pltpu.VMEM(weight.shape, bf16),
            pltpu.VMEM((rows, feature_width), bf16),
            pltpu.SemaphoreType.DMA((3,)),
        ],
        compiler_params=pltpu.CompilerParams(vmem_limit_bytes=8 * 2**20),
        cost_estimate=pl.CostEstimate(
            flops=2 * rows * feature_width * 3 * width,
            bytes_accessed=2 * weight.size,
            transcendentals=0,
        ),
        name="projections",
    )(slot, timestep, frame_order, *operands)


def stack_rows(rows, width):
    return rows * width // LANES


def stack(tiles, width):
    rows = tiles[0].shape[0]
    whole = width // LANES
    stacked = list(tiles[:whole])
    if width % LANES:
        fold = tiles[whole]
        lane = lax.broadcasted_iota(jnp.int32, (1, LANES), 1)
        low = jnp.where(lane < LANES // 2, fold[: rows // 2], 0.0)
        high = jnp.where(lane < LANES // 2, fold[rows // 2 :], 0.0)
        stacked.append(low + pltpu.roll(high, LANES // 2, 1))
    return jnp.concatenate(stacked, axis=0).astype(bf16)


def unstack(stacked, rows, width, first, count):
    whole = width // LANES
    tiles = [stacked[t * rows + first : t * rows + first + count, :] for t in range(whole)]
    if width % LANES:
        half = rows // 2
        fold = stacked[whole * rows :, :]
        turned = pltpu.roll(fold.astype(f32), LANES // 2, 1).astype(stacked.dtype)
        both = jnp.concatenate([fold, turned], axis=0)
        if first % half == 0 and count == half:
            both = turned if first else fold
        else:
            both = both[first : first + count]
        tiles.append(both[:, : LANES // 2])
    return jnp.concatenate(tiles, axis=1)


def pair_plan(width, head_dim):
    plan = []
    for first in range(0, width, 2 * head_dim):
        key_tile = first // LANES
        value_tile = (width + first) // LANES
        plan.append(
            (key_tile, first - key_tile * LANES, value_tile, width + first - value_tile * LANES)
        )
    return plan


def group_tiles(width, head_dim):
    plan = pair_plan(width, head_dim)
    seen, groups = set(), []
    for group in PAIR_GROUPS:
        need = []
        for pair in group:
            key_tile, _, value_tile, _ = plan[pair]
            need += [key_tile, key_tile + 1, value_tile, value_tile + 1]
        fresh = sorted(set(need) - seen)
        seen |= set(fresh)
        groups.append(tuple(fresh))
    return groups


def spatial_kernel(*refs, group, frames, head_dim, width, tiles, held, emitted, kept, columns, chunks):
    plan = pair_plan(width, head_dim)
    count = len(tiles)
    position = 0
    refs, (scores_ref, weights_ref) = refs[:-2], refs[-2:]
    query_ref, own_ref, peer_ref = refs[:3]
    near_refs = refs[3 : 3 + count]
    far_refs = refs[3 + count : 3 + 2 * count]
    position = 3 + 2 * count
    held_ref = None
    if held:
        held_ref = refs[position]
        position += 1
    rows = query_ref.shape[0]
    piece = rows // frames
    covered = part_pieces(chunks, piece)
    out_count = len(covered) if emitted else 0
    out_refs = dict(zip(covered, refs[position : position + out_count]))
    kept_ref = refs[position + out_count] if kept else None

    where = {tile: (c, j) for c, chunk in enumerate(tiles) for j, tile in enumerate(chunk)}

    def from_chunks(chunk_refs):
        def load(tile):
            chunk, at = where[tile]
            return chunk_refs[chunk][:, at * LANES : (at + 1) * LANES]

        return load

    def from_whole(ref):
        return lambda tile: ref[:, tile * LANES : (tile + 1) * LANES]

    blocks = [from_whole(own_ref), from_whole(peer_ref), from_chunks(near_refs), from_chunks(far_refs)]
    scale = softmax_scale(head_dim)

    def two(block, tile):
        return jnp.concatenate([block(tile), block(tile + 1)], axis=1)

    def score(index):
        chunk, pair = tasks[index]
        key_tile, key_lane, _, _ = plan[pair]
        window = query_ref[
            chunk * QUERY_ROWS : (chunk + 1) * QUERY_ROWS, key_tile * LANES : (key_tile + 2) * LANES
        ]
        stacked = jnp.concatenate(
            [
                window * column_mask(key_lane, head_dim, bf16),
                window * column_mask(key_lane + head_dim, head_dim, bf16),
            ],
            axis=0,
        )
        for number, block in enumerate(blocks):
            scores_ref[index % 2, :, number * rows : (number + 1) * rows] = lax.dot_general(
                stacked, two(block, key_tile), NT, preferred_element_type=f32
            )

    def weigh(index):
        totals = []
        for row in range(0, 2 * QUERY_ROWS, STRIP):
            scores = scores_ref[index % 2, row : row + STRIP, :]
            top = jnp.max(scores, axis=-1, keepdims=True) * scale
            weights = jnp.exp2(scores * scale - top)
            totals.append(jnp.sum(weights, axis=-1, keepdims=True))
            weights_ref[index % 2, row : row + STRIP, :] = weights.astype(bf16)
        return jnp.concatenate(totals, axis=0)

    def mix(index, total):
        _, key_lane, value_tile, value_lane = plan[tasks[index][1]]
        mixed = functools.reduce(
            jnp.add,
            [
                jnp.dot(
                    weights_ref[index % 2, :, number * rows : (number + 1) * rows],
                    two(block, value_tile),
                    preferred_element_type=f32,
                )
                for number, block in enumerate(blocks)
            ],
        )
        mixed = mixed / total
        joined = mixed[:QUERY_ROWS] * column_mask(value_lane, head_dim, f32) + mixed[
            QUERY_ROWS:
        ] * column_mask(value_lane + head_dim, head_dim, f32)
        return pltpu.roll(joined, (key_lane - value_lane) % (2 * LANES), 1)

    tasks = [(chunk, pair) for chunk in chunks for pair in group]
    parts = {}

    def finish(index, total):
        chunk, pair = tasks[index]
        joined = mix(index, total)
        tile = plan[pair][0]
        for side in range(2):
            half = joined[:, side * LANES : (side + 1) * LANES]
            parts[tile + side] = parts[tile + side] + half if tile + side in parts else half
        if pair != group[-1]:
            return
        at = chunk * QUERY_ROWS
        for number, tile in enumerate(held):
            old = held_ref[at : at + QUERY_ROWS, number * LANES : (number + 1) * LANES].astype(f32)
            parts[tile] = parts[tile] + old if tile in parts else old
        if kept:
            values = jnp.concatenate([parts[tile] for tile in kept], axis=1)
            kept_ref[at : at + QUERY_ROWS, :] = values.astype(bf16)
        if emitted:
            for sub in range(QUERY_ROWS // piece):
                cut = slice(sub * piece, (sub + 1) * piece)
                out_refs[(at + sub * piece) // piece][...] = stack(
                    [parts[tile][cut] for tile in emitted], columns
                )
        parts.clear()

    score(0)
    total = None
    for index in range(len(tasks)):
        if index + 1 < len(tasks):
            score(index + 1)
        if index > 0:
            finish(index - 1, total)
        total = weigh(index)
    finish(len(tasks) - 1, total)


def tile_flow(width, head_dim):
    plan = pair_plan(width, head_dim)
    flow, held = [], ()
    for number, group in enumerate(PAIR_GROUPS):
        have = sorted({plan[pair][0] + side for pair in group for side in range(2)} | set(held))
        last = number == len(PAIR_GROUPS) - 1
        complete = [tile for tile in have if last or tile <= plan[group[-1]][0]]
        emitted = tuple(complete) if EMIT[number] else ()
        kept = tuple(tile for tile in have if tile not in emitted)
        flow.append((held, emitted, kept))
        held = kept
    return flow


def emitted_columns(emitted, width):
    return min(width, (emitted[-1] + 1) * LANES) - emitted[0] * LANES if emitted else 0


def group_columns(width, head_dim):
    flow = tile_flow(width, head_dim)
    return tuple(emitted_columns(emitted, width) for _, emitted, _ in flow if emitted)


def part_pieces(chunks, piece):
    per = QUERY_ROWS // piece
    return [chunk * per + sub for chunk in chunks for sub in range(per)]


def row_parts(number, rows):
    chunks = list(range(rows // QUERY_ROWS))
    if number < len(PAIR_GROUPS) - 1 or len(chunks) < 3:
        return [chunks]
    return [[chunk] for chunk in chunks[:1:-1]] + [chunks[1::-1]]


def spatial_group(
    number, part, query, own_kv, peer_kv, near, far, carry, frames, head_dim, width
):
    group = PAIR_GROUPS[number]
    held, emitted, kept = tile_flow(width, head_dim)[number]
    tiles = tuple(group_tiles(width, head_dim)[: number + 1])
    rows = query.shape[0]
    chunks = row_parts(number, rows)[part]
    shapes = []
    columns = emitted_columns(emitted, width)
    if emitted:
        count = len(chunks) * QUERY_ROWS // (rows // frames)
        shapes += [((stack_rows(rows // frames, columns), LANES), bf16) for _ in range(count)]
    if kept:
        shapes.append(((rows, len(kept) * LANES), bf16))
    operands = [query, own_kv, peer_kv, *near[: number + 1], *far[: number + 1]]
    if held:
        operands.append(carry)
    keys = 4 * rows
    results = on_chip_call(
        functools.partial(
            spatial_kernel,
            group=group,
            frames=frames,
            head_dim=head_dim,
            width=width,
            tiles=tiles,
            held=held,
            emitted=emitted,
            kept=kept,
            columns=columns,
            chunks=chunks,
        ),
        operands,
        shapes,
        len(group) * 2 * len(chunks) * QUERY_ROWS * keys * 256 * 4,
        8,
        len(group) * 2 * rows * keys,
        [
            pltpu.VMEM((2, 2 * QUERY_ROWS, keys), f32),
            pltpu.VMEM((2, 2 * QUERY_ROWS, keys), bf16),
        ],
    )
    results = list(results)
    carry = results.pop() if kept else None
    return results, carry


def joined_rows(tokens_refs, mixed_refs, columns, first, count):
    groups = len(columns)
    piece = tokens_refs[0].shape[0]
    cut = slice(first, first + count)
    tokens = jnp.concatenate([ref[cut, :] for ref in tokens_refs], axis=0).astype(f32)
    mixed = jnp.concatenate(
        [
            jnp.concatenate(
                [
                    unstack(mixed_refs[frame * groups + g][...], piece, columns[g], first, count)
                    for g in range(groups)
                ],
                axis=1,
            )
            for frame in range(len(tokens_refs))
        ],
        axis=0,
    )
    return tokens, mixed


def temporal_kernel(*refs, frames, head_dim, columns, first, piece):
    groups = len(columns)
    tokens_refs = refs[:frames]
    mixed_refs = refs[frames : frames + frames * groups]
    position = frames + frames * groups
    out_weight, qkv_weight, modulation_ref, place_ref = refs[position : position + 4]
    out_refs = refs[position + 4 : position + 4 + frames]
    query_ref, kv_ref = refs[position + 4 + frames :]
    width = out_weight.shape[0]
    tokens, mixed = joined_rows(tokens_refs, mixed_refs, columns, first, piece)
    after = tokens + modulation_ref[2:3, :] * jnp.dot(
        mixed, out_weight[...], preferred_element_type=f32
    )
    normal = normalize(after) * (1.0 + modulation_ref[4:5, :]) + modulation_ref[3:4, :]
    inputs = jnp.concatenate(
        [
            (normal[frame * piece : (frame + 1) * piece] + place_ref[frame : frame + 1, :]).astype(bf16)
            for frame in range(frames)
        ],
        axis=0,
    )
    query_ref[...] = lax.dot_general(
        inputs, qkv_weight[: query_ref.shape[1], :], NT, preferred_element_type=f32
    ).astype(bf16)
    kv_ref[...] = lax.dot_general(
        inputs, qkv_weight[width:, :], NT, preferred_element_type=f32
    ).astype(bf16)

    scale = softmax_scale(head_dim)
    step = max(16, min(piece, LANES // frames))
    block = frames * step
    row_at = lax.broadcasted_iota(jnp.int32, (2 * block, block), 0) % step
    column_at = lax.broadcasted_iota(jnp.int32, (2 * block, block), 1) % step
    same = row_at == column_at
    plan = pair_plan(width, head_dim)

    def window(ref, start, tile):
        return jnp.concatenate(
            [
                ref[
                    frame * piece + start : frame * piece + start + step,
                    tile * LANES : (tile + 2) * LANES,
                ]
                for frame in range(frames)
            ],
            axis=0,
        )

    def score(start, tile, lane):
        queries = window(query_ref, start, tile)
        stacked = jnp.concatenate(
            [
                queries * column_mask(lane, head_dim, bf16),
                queries * column_mask(lane + head_dim, head_dim, bf16),
            ],
            axis=0,
        )
        scores = lax.dot_general(
            stacked, window(kv_ref, start, tile), NT, preferred_element_type=f32
        )
        return jnp.where(same, scores * scale, -jnp.inf)

    def weigh(scores):
        weights = jnp.exp2(scores - jnp.max(scores, axis=-1, keepdims=True))
        return (weights / jnp.sum(weights, axis=-1, keepdims=True)).astype(bf16)

    starts = range(0, piece, step)
    tasks = [(start, *entry) for start in starts for entry in plan]
    scores = [score(start, tile, lane) for start, tile, lane, _, _ in tasks]
    weights = [weigh(value) for value in scores]
    mixed_pairs = [
        jnp.dot(value, window(kv_ref, start, value_tile), preferred_element_type=f32)
        for value, (start, _, _, value_tile, _) in zip(weights, tasks)
    ]
    parts = {start: {} for start in starts}
    for pair, (start, tile, lane, _, value_lane) in zip(mixed_pairs, tasks):
        joined = pair[:block] * column_mask(value_lane, head_dim, f32) + pair[
            block:
        ] * column_mask(value_lane + head_dim, head_dim, f32)
        joined = pltpu.roll(joined, (lane - value_lane) % (2 * LANES), 1)
        have = parts[start]
        for side in range(2):
            half = joined[:, side * LANES : (side + 1) * LANES]
            have[tile + side] = have[tile + side] + half if tile + side in have else half
    for frame in range(frames):
        cut = slice(frame * step, (frame + 1) * step)
        out_refs[frame][...] = stack(
            [
                jnp.concatenate([parts[start][tile][cut] for start in starts], axis=0)
                for tile in sorted(parts[0])
            ],
            width,
        )


def temporal(tokens, mixed, columns, weights, modulation, places, head_dim, first, piece):
    frames = len(tokens)
    spatial_out, temporal_qkv = weights
    width, feature_width = spatial_out.shape
    padded = -(-width // LANES) * LANES
    rows = frames * piece
    return on_chip_call(
        functools.partial(
            temporal_kernel,
            frames=frames,
            head_dim=head_dim,
            columns=columns,
            first=first,
            piece=piece,
        ),
        [
            *tokens,
            *[part for frame in mixed for part in frame],
            spatial_out,
            temporal_qkv,
            modulation,
            places,
        ],
        [((stack_rows(piece, width), LANES), bf16) for _ in range(frames)],
        2 * rows * feature_width * width * 5,
        6,
        rows * 128 * 8,
        [pltpu.VMEM((rows, padded), bf16), pltpu.VMEM((rows, 2 * width), bf16)],
    )


def after_kernel(*refs, frames, columns):
    mixed_end = frames * (1 + len(columns))
    weight_ref, modulation_ref, out_ref = refs[mixed_end:]
    piece = refs[0].shape[0]
    tokens, mixed = joined_rows(refs[:frames], refs[frames:mixed_end], columns, 0, piece)
    out_ref[...] = tokens + modulation_ref[2:3, :] * jnp.dot(
        mixed, weight_ref[...], preferred_element_type=f32
    )


def after_spatial(tokens, mixed, columns, weight, modulation):
    frames = len(tokens)
    width, feature_width = weight.shape
    rows = frames * tokens[0].shape[0]
    return on_chip_call(
        functools.partial(after_kernel, frames=frames, columns=columns),
        [*tokens, *[part for frame in mixed for part in frame], weight, modulation],
        [((rows, feature_width), f32)],
        2 * rows * feature_width * width,
        6,
    )[0]


def output_kernel(slot_ref, after_ref, weight_ref, modulation_ref, *refs, frames, number):
    parts = refs[:frames]
    out_ref, stage_ref, sems = refs[-3:]
    piece = after_ref.shape[0] // frames
    half = piece // HALVES
    first = number * half
    width = weight_ref.shape[0]
    mixed = jnp.concatenate(
        [unstack(ref[...].astype(f32), half, width, 0, half).astype(bf16) for ref in parts], axis=0
    )
    after = jnp.concatenate(
        [after_ref[frame * piece + first : frame * piece + first + half, :] for frame in range(frames)],
        axis=0,
    )
    stage_ref[...] = after + modulation_ref[5:6, :] * jnp.dot(
        mixed, weight_ref[...], preferred_element_type=f32
    )
    copies = []
    for frame in range(frames):
        row = partner_slot(slot_ref[0], frame, frames) * piece + first
        copies.append(
            pltpu.make_async_copy(
                stage_ref.at[frame * half : (frame + 1) * half, :],
                out_ref.at[pl.ds(row, half), :],
                sems.at[frame],
            )
        )
        copies[-1].start()
    for copy in copies:
        copy.wait()


def output(number, slot, after, weight, modulation, parts, result):
    frames = len(parts)
    rows, feature_width = after.shape
    operands = [after, weight, modulation, *parts]
    specs = [pl.BlockSpec(memory_space=pltpu.SMEM), *vmem_specs(len(operands))]
    operands = [pltpu.with_memory_space_constraint(array, pltpu.VMEM) for array in operands]
    aliases = {}
    if result is not None:
        aliases = {len(specs): 0}
        specs.append(pl.BlockSpec(memory_space=pltpu.HBM))
        operands.append(result)
    return pl.pallas_call(
        functools.partial(output_kernel, frames=frames, number=number),
        out_shape=jax.ShapeDtypeStruct((rows, feature_width), f32),
        in_specs=specs,
        out_specs=pl.BlockSpec(memory_space=pltpu.HBM),
        scratch_shapes=[
            pltpu.VMEM((rows // HALVES, feature_width), f32),
            pltpu.SemaphoreType.DMA((frames,)),
        ],
        input_output_aliases=aliases,
        compiler_params=pltpu.CompilerParams(vmem_limit_bytes=4 * 2**20),
    )(slot, *operands)


def per_device(
    tokens,
    stale_kv,
    mod_table,
    mod_mix,
    timestep,
    frame_order,
    spatial_qkv,
    spatial_out,
    temporal_qkv,
    temporal_out,
):
    devices = lax.axis_size("patch")
    frames = devices // 4
    slot = lax.axis_index("patch") // 4
    rows, feature_width = tokens.shape
    width = spatial_out.shape[0]
    head_dim = feature_width // HEADS
    piece = rows // frames

    def other_core(device):
        return device ^ 1

    def other_chip(device):
        return device ^ 2

    def ahead(step):
        return lambda device: partner_slot(device // 4, step, frames) * 4 + device % 4

    def behind(step):
        return lambda device: source_slot(device // 4, step, frames) * 4 + device % 4

    near, far = [], []
    for chunk in stage_chunks(stale_kv, group_tiles(width, head_dim)):
        near.append(permute(chunk, other_chip))
        far.append(permute(near[-1], other_core))
    peer_kv = permute(stale_kv, other_core)

    slot_word = slot.astype(jnp.int32)[None]
    pieces = stage_pieces(slot_word, tokens, frames)
    there = [pieces[0]]
    there += [permute(pieces[s], ahead(s)) for s in range(1, frames)]

    query, own_kv, modulation, places = projections(
        slot_word,
        timestep,
        frame_order,
        jnp.swapaxes(spatial_qkv, 1, 2).reshape(3 * width, feature_width),
        mod_table,
        mod_mix,
        pieces,
        width,
    )

    carry = None
    local = [[] for _ in range(frames)]
    sent = [[] for _ in range(frames)]
    for number in range(len(PAIR_GROUPS)):
        handed = carry
        for part, chunks in enumerate(row_parts(number, rows)):
            outs, carry = spatial_group(
                number, part, query, own_kv, peer_kv, near, far, handed, frames, head_dim, width
            )
            covered = part_pieces(chunks, piece)
            for s, out in zip(covered, outs):
                local[s].append(out)
                sent[s].append(out if s == 0 else permute(out, ahead(s)))

    columns = group_columns(width, head_dim)
    after = after_spatial(pieces, local, columns, spatial_out, modulation)
    weights = (spatial_out, jnp.swapaxes(temporal_qkv, 1, 2).reshape(3 * width, feature_width))
    half = piece // HALVES
    back = []
    for h in range(HALVES):
        outs = temporal(there, sent, columns, weights, modulation, places, head_dim, h * half, half)
        back.append([out if s == 0 else permute(out, behind(s)) for s, out in enumerate(outs)])
    result = None
    for h in range(HALVES):
        result = output(h, slot_word, after, temporal_out, modulation, back[h], result)
    return result


def solution(mesh):
    split = P(("groups", "patch"), None)
    return jax.shard_map(
        per_device,
        mesh=mesh,
        in_specs=(split, split, P(), P(), P("groups"), P("groups"), P(), P(), P(), P()),
        out_specs=split,
        check_vma=False,
    )
```

```python
import functools
import math

import jax
import jax.numpy as jnp
import numpy as np
from jax import lax
from jax.experimental import pallas as pl
from jax.experimental.pallas import tpu as pltpu
from jax.sharding import PartitionSpec as P


HEADS = 16
LANES = 128
QUERY_ROWS = 128
STRIP = 16
PAIR_GROUPS = ((0,), (1,), (2, 3))
EMIT = (False, True, True)
HALVES = 2
STAGING_FLOPS = 4 * 10**9


epsilon = 1e-06
bf16 = jnp.bfloat16
f32 = jnp.float32
NT = (((1,), (1,)), ((), ()))


def permute(value, target):
    count = lax.axis_size("patch")
    return lax.ppermute(value, "patch", [(source, target(source)) for source in range(count)])


def partner_slot(slot, step, frames):
    if frames & (frames - 1) == 0:
        return slot ^ step
    return (slot + step) % frames


def source_slot(slot, step, frames):
    if frames & (frames - 1) == 0:
        return slot ^ step
    return (slot - step) % frames


def normalize(activations):
    row_mean = jnp.mean(activations, axis=-1, keepdims=True)
    centered = activations - row_mean
    variance = jnp.mean(centered * centered, axis=-1, keepdims=True)
    return centered * lax.rsqrt(variance + epsilon)


def column_mask(first, width, dtype):
    column = lax.broadcasted_iota(jnp.int32, (1, 2 * LANES), 1)
    inside = jnp.logical_and(column >= first, column < first + width)
    return jnp.where(inside, 1.0, 0.0).astype(dtype)


def softmax_scale(head_dim):
    return math.log2(math.e) * head_dim ** (-0.5)


def vmem_specs(count):
    return [pl.BlockSpec(memory_space=pltpu.VMEM) for _ in range(count)]


def on_chip_call(kernel, operands, shapes, flops, limit_mib, transcendentals=0, scratch=()):
    operands = [pltpu.with_memory_space_constraint(array, pltpu.VMEM) for array in operands]
    return pl.pallas_call(
        kernel,
        out_shape=[pltpu.VMEM(shape, dtype) for shape, dtype in shapes],
        in_specs=vmem_specs(len(operands)),
        out_specs=vmem_specs(len(shapes)),
        scratch_shapes=list(scratch),
        compiler_params=pltpu.CompilerParams(vmem_limit_bytes=limit_mib * 2**20),
        cost_estimate=pl.CostEstimate(
            flops=flops,
            bytes_accessed=sum(array.size * array.dtype.itemsize for array in operands),
            transcendentals=transcendentals,
        ),
    )(*operands)


def chunk_kernel(kv_ref, *refs, tiles):
    out_refs, sems = refs[:-1], refs[-1]
    copies = []
    for chunk, ref in zip(tiles, out_refs):
        for at, tile in enumerate(chunk):
            copies.append(
                pltpu.make_async_copy(
                    kv_ref.at[:, tile * LANES : (tile + 1) * LANES],
                    ref.at[:, at * LANES : (at + 1) * LANES],
                    sems.at[len(copies)],
                )
            )
            copies[-1].start()
    for copy in copies:
        copy.wait()


def stage_chunks(stale_kv, tiles):
    rows = stale_kv.shape[0]
    return pl.pallas_call(
        functools.partial(chunk_kernel, tiles=tiles),
        out_shape=[pltpu.VMEM((rows, len(chunk) * LANES), bf16) for chunk in tiles],
        in_specs=[pl.BlockSpec(memory_space=pltpu.HBM)],
        out_specs=vmem_specs(len(tiles)),
        scratch_shapes=[pltpu.SemaphoreType.DMA((sum(len(chunk) for chunk in tiles),))],
        compiler_params=pltpu.CompilerParams(vmem_limit_bytes=2**20),
        name="chunks",
    )(pltpu.with_memory_space_constraint(stale_kv, pltpu.HBM))


def piece_kernel(slot_ref, tokens_ref, *refs, frames):
    out_refs, sems = refs[:-1], refs[-1]
    piece = tokens_ref.shape[0] // frames
    copies = []
    for step in range(frames):
        row = partner_slot(slot_ref[0], step, frames) * piece
        copies.append(
            pltpu.make_async_copy(
                tokens_ref.at[pl.ds(row, piece), :], out_refs[step], sems.at[step]
            )
        )
        copies[-1].start()
    for copy in copies:
        copy.wait()


def stage_pieces(slot, tokens, frames):
    rows, feature_width = tokens.shape
    return pl.pallas_call(
        functools.partial(piece_kernel, frames=frames),
        out_shape=[pltpu.VMEM((rows // frames, feature_width), bf16) for _ in range(frames)],
        in_specs=[
            pl.BlockSpec(memory_space=pltpu.SMEM),
            pl.BlockSpec(memory_space=pltpu.HBM),
        ],
        out_specs=vmem_specs(frames),
        scratch_shapes=[pltpu.SemaphoreType.DMA((frames,))],
        compiler_params=pltpu.CompilerParams(vmem_limit_bytes=2**20),
        cost_estimate=pl.CostEstimate(
            flops=STAGING_FLOPS, bytes_accessed=4 * tokens.size, transcendentals=0
        ),
        name="pieces",
    )(slot, pltpu.with_memory_space_constraint(tokens, pltpu.HBM))


def projection_kernel(slot_ref, time_ref, order_ref, weight_ref, *refs, frames, width):
    rate_ref, table_ref, mix_ref = refs[:3]
    pieces = refs[3 : 3 + frames]
    query_ref, kv_ref, modulation_ref, place_ref = refs[3 + frames :]
    padded = query_ref.shape[1]

    rows = -(-(frames + 1) // 8) * 8
    row = lax.broadcasted_iota(jnp.int32, (rows, 1), 0)
    position = jnp.where(row == frames, time_ref[0], 0)
    for step in range(frames):
        frame = order_ref[source_slot(slot_ref[0], step, frames)]
        position = jnp.where(row == step, frame, position)
    angles = position.astype(f32) * rate_ref[...]
    waves = jnp.concatenate([jnp.sin(angles), jnp.cos(angles)], axis=1)
    place_ref[...] = waves[:frames]
    modulation = table_ref[...] + mix_ref[...] * waves[frames : frames + 1]
    modulation_ref[...] = modulation

    tokens = jnp.concatenate([ref[...] for ref in pieces], axis=0).astype(f32)
    inputs = normalize(tokens) * (1.0 + modulation[1:2, :]) + modulation[0:1, :]
    inputs = inputs.astype(bf16)
    query_ref[...] = lax.dot_general(
        inputs, weight_ref[:padded, :], NT, preferred_element_type=f32
    ).astype(bf16)
    kv_ref[...] = lax.dot_general(
        inputs, weight_ref[width:, :], NT, preferred_element_type=f32
    ).astype(bf16)


def projections(slot, timestep, frame_order, weight, mod_table, mod_mix, pieces, width):
    frames = len(pieces)
    piece, feature_width = pieces[0].shape
    padded = -(-width // LANES) * LANES
    rows = frames * piece
    half = feature_width // 2
    rates = np.exp(-math.log(10000.0) * np.arange(half) / half).astype(np.float32)
    rates = jnp.asarray(rates[None])
    operands = [
        pltpu.with_memory_space_constraint(x, pltpu.VMEM)
        for x in (weight, rates, mod_table, mod_mix, *pieces)
    ]
    return pl.pallas_call(
        functools.partial(projection_kernel, frames=frames, width=width),
        out_shape=[
            pltpu.VMEM((rows, padded), bf16),
            pltpu.VMEM((rows, 2 * width), bf16),
            pltpu.VMEM(mod_table.shape, f32),
            pltpu.VMEM((frames, feature_width), f32),
        ],
        in_specs=[
            *[pl.BlockSpec(memory_space=pltpu.SMEM) for _ in range(3)],
            *vmem_specs(4 + frames),
        ],
        out_specs=vmem_specs(4),
        compiler_params=pltpu.CompilerParams(vmem_limit_bytes=4 * 2**20),
        cost_estimate=pl.CostEstimate(
            flops=2 * rows * feature_width * 3 * width,
            bytes_accessed=2 * weight.size,
            transcendentals=0,
        ),
        name="projections",
    )(slot, timestep, frame_order, *operands)


def stack_rows(rows, width):
    return rows * width // LANES


def stack(tiles, width):
    rows = tiles[0].shape[0]
    whole = width // LANES
    stacked = list(tiles[:whole])
    if width % LANES:
        fold = tiles[whole]
        lane = lax.broadcasted_iota(jnp.int32, (1, LANES), 1)
        low = jnp.where(lane < LANES // 2, fold[: rows // 2], 0.0)
        high = jnp.where(lane < LANES // 2, fold[rows // 2 :], 0.0)
        stacked.append(low + pltpu.roll(high, LANES // 2, 1))
    return jnp.concatenate(stacked, axis=0).astype(bf16)


def unstack(stacked, rows, width, first, count):
    whole = width // LANES
    tiles = [stacked[t * rows + first : t * rows + first + count, :] for t in range(whole)]
    if width % LANES:
        half = rows // 2
        fold = stacked[whole * rows :, :]
        turned = pltpu.roll(fold.astype(f32), LANES // 2, 1).astype(stacked.dtype)
        both = jnp.concatenate([fold, turned], axis=0)
        if first % half == 0 and count == half:
            both = turned if first else fold
        else:
            both = both[first : first + count]
        tiles.append(both[:, : LANES // 2])
    return jnp.concatenate(tiles, axis=1)


def pair_plan(width, head_dim):
    plan = []
    for first in range(0, width, 2 * head_dim):
        key_tile = first // LANES
        value_tile = (width + first) // LANES
        plan.append(
            (key_tile, first - key_tile * LANES, value_tile, width + first - value_tile * LANES)
        )
    return plan


def group_tiles(width, head_dim):
    plan = pair_plan(width, head_dim)
    seen, groups = set(), []
    for group in PAIR_GROUPS:
        need = []
        for pair in group:
            key_tile, _, value_tile, _ = plan[pair]
            need += [key_tile, key_tile + 1, value_tile, value_tile + 1]
        fresh = sorted(set(need) - seen)
        seen |= set(fresh)
        groups.append(tuple(fresh))
    return groups


def spatial_kernel(*refs, group, frames, head_dim, width, tiles, held, emitted, kept, columns, chunks):
    plan = pair_plan(width, head_dim)
    count = len(tiles)
    position = 0
    refs, (scores_ref, weights_ref) = refs[:-2], refs[-2:]
    query_ref, own_ref, peer_ref = refs[:3]
    near_refs = refs[3 : 3 + count]
    far_refs = refs[3 + count : 3 + 2 * count]
    position = 3 + 2 * count
    held_ref = None
    if held:
        held_ref = refs[position]
        position += 1
    rows = query_ref.shape[0]
    piece = rows // frames
    covered = part_pieces(chunks, piece)
    out_count = len(covered) if emitted else 0
    out_refs = dict(zip(covered, refs[position : position + out_count]))
    kept_ref = refs[position + out_count] if kept else None

    where = {tile: (c, j) for c, chunk in enumerate(tiles) for j, tile in enumerate(chunk)}

    def from_chunks(chunk_refs):
        def load(tile):
            chunk, at = where[tile]
            return chunk_refs[chunk][:, at * LANES : (at + 1) * LANES]

        return load

    def from_whole(ref):
        return lambda tile: ref[:, tile * LANES : (tile + 1) * LANES]

    blocks = [from_whole(own_ref), from_whole(peer_ref), from_chunks(near_refs), from_chunks(far_refs)]
    scale = softmax_scale(head_dim)

    def two(block, tile):
        return jnp.concatenate([block(tile), block(tile + 1)], axis=1)

    def score(index):
        chunk, pair = tasks[index]
        key_tile, key_lane, _, _ = plan[pair]
        window = query_ref[
            chunk * QUERY_ROWS : (chunk + 1) * QUERY_ROWS, key_tile * LANES : (key_tile + 2) * LANES
        ]
        stacked = jnp.concatenate(
            [
                window * column_mask(key_lane, head_dim, bf16),
                window * column_mask(key_lane + head_dim, head_dim, bf16),
            ],
            axis=0,
        )
        for number, block in enumerate(blocks):
            scores_ref[index % 2, :, number * rows : (number + 1) * rows] = lax.dot_general(
                stacked, two(block, key_tile), NT, preferred_element_type=f32
            )

    def weigh(index):
        totals = []
        for row in range(0, 2 * QUERY_ROWS, STRIP):
            scores = scores_ref[index % 2, row : row + STRIP, :]
            top = jnp.max(scores, axis=-1, keepdims=True) * scale
            weights = jnp.exp2(scores * scale - top)
            totals.append(jnp.sum(weights, axis=-1, keepdims=True))
            weights_ref[index % 2, row : row + STRIP, :] = weights.astype(bf16)
        return jnp.concatenate(totals, axis=0)

    def mix(index, total):
        _, key_lane, value_tile, value_lane = plan[tasks[index][1]]
        mixed = functools.reduce(
            jnp.add,
            [
                jnp.dot(
                    weights_ref[index % 2, :, number * rows : (number + 1) * rows],
                    two(block, value_tile),
                    preferred_element_type=f32,
                )
                for number, block in enumerate(blocks)
            ],
        )
        mixed = mixed / total
        joined = mixed[:QUERY_ROWS] * column_mask(value_lane, head_dim, f32) + mixed[
            QUERY_ROWS:
        ] * column_mask(value_lane + head_dim, head_dim, f32)
        return pltpu.roll(joined, (key_lane - value_lane) % (2 * LANES), 1)

    tasks = [(chunk, pair) for chunk in chunks for pair in group]
    parts = {}

    def finish(index, total):
        chunk, pair = tasks[index]
        joined = mix(index, total)
        tile = plan[pair][0]
        for side in range(2):
            half = joined[:, side * LANES : (side + 1) * LANES]
            parts[tile + side] = parts[tile + side] + half if tile + side in parts else half
        if pair != group[-1]:
            return
        at = chunk * QUERY_ROWS
        for number, tile in enumerate(held):
            old = held_ref[at : at + QUERY_ROWS, number * LANES : (number + 1) * LANES].astype(f32)
            parts[tile] = parts[tile] + old if tile in parts else old
        if kept:
            values = jnp.concatenate([parts[tile] for tile in kept], axis=1)
            kept_ref[at : at + QUERY_ROWS, :] = values.astype(bf16)
        if emitted:
            for sub in range(QUERY_ROWS // piece):
                cut = slice(sub * piece, (sub + 1) * piece)
                out_refs[(at + sub * piece) // piece][...] = stack(
                    [parts[tile][cut] for tile in emitted], columns
                )
        parts.clear()

    score(0)
    total = None
    for index in range(len(tasks)):
        if index + 1 < len(tasks):
            score(index + 1)
        if index > 0:
            finish(index - 1, total)
        total = weigh(index)
    finish(len(tasks) - 1, total)


def tile_flow(width, head_dim):
    plan = pair_plan(width, head_dim)
    flow, held = [], ()
    for number, group in enumerate(PAIR_GROUPS):
        have = sorted({plan[pair][0] + side for pair in group for side in range(2)} | set(held))
        last = number == len(PAIR_GROUPS) - 1
        complete = [tile for tile in have if last or tile <= plan[group[-1]][0]]
        emitted = tuple(complete) if EMIT[number] else ()
        kept = tuple(tile for tile in have if tile not in emitted)
        flow.append((held, emitted, kept))
        held = kept
    return flow


def emitted_columns(emitted, width):
    return min(width, (emitted[-1] + 1) * LANES) - emitted[0] * LANES if emitted else 0


def group_columns(width, head_dim):
    flow = tile_flow(width, head_dim)
    return tuple(emitted_columns(emitted, width) for _, emitted, _ in flow if emitted)


def part_pieces(chunks, piece):
    per = QUERY_ROWS // piece
    return [chunk * per + sub for chunk in chunks for sub in range(per)]


def row_parts(number, rows):
    chunks = list(range(rows // QUERY_ROWS))
    if number < len(PAIR_GROUPS) - 1:
        return [chunks]
    return [[chunk] for chunk in reversed(chunks)]


def spatial_group(
    number, part, query, own_kv, peer_kv, near, far, carry, frames, head_dim, width
):
    group = PAIR_GROUPS[number]
    held, emitted, kept = tile_flow(width, head_dim)[number]
    tiles = tuple(group_tiles(width, head_dim)[: number + 1])
    rows = query.shape[0]
    chunks = row_parts(number, rows)[part]
    shapes = []
    columns = emitted_columns(emitted, width)
    if emitted:
        count = len(chunks) * QUERY_ROWS // (rows // frames)
        shapes += [((stack_rows(rows // frames, columns), LANES), bf16) for _ in range(count)]
    if kept:
        shapes.append(((rows, len(kept) * LANES), bf16))
    operands = [query, own_kv, peer_kv, *near[: number + 1], *far[: number + 1]]
    if held:
        operands.append(carry)
    keys = 4 * rows
    results = on_chip_call(
        functools.partial(
            spatial_kernel,
            group=group,
            frames=frames,
            head_dim=head_dim,
            width=width,
            tiles=tiles,
            held=held,
            emitted=emitted,
            kept=kept,
            columns=columns,
            chunks=chunks,
        ),
        operands,
        shapes,
        len(group) * 2 * len(chunks) * QUERY_ROWS * keys * 256 * 4,
        8,
        len(group) * 2 * rows * keys,
        [
            pltpu.VMEM((2, 2 * QUERY_ROWS, keys), f32),
            pltpu.VMEM((2, 2 * QUERY_ROWS, keys), bf16),
        ],
    )
    results = list(results)
    carry = results.pop() if kept else None
    return results, carry


def joined_rows(tokens_refs, mixed_refs, columns, first, count):
    groups = len(columns)
    piece = tokens_refs[0].shape[0]
    cut = slice(first, first + count)
    tokens = jnp.concatenate([ref[cut, :] for ref in tokens_refs], axis=0).astype(f32)
    mixed = jnp.concatenate(
        [
            jnp.concatenate(
                [
                    unstack(mixed_refs[frame * groups + g][...], piece, columns[g], first, count)
                    for g in range(groups)
                ],
                axis=1,
            )
            for frame in range(len(tokens_refs))
        ],
        axis=0,
    )
    return tokens, mixed


def temporal_kernel(*refs, frames, head_dim, columns, first, piece):
    groups = len(columns)
    tokens_refs = refs[:frames]
    mixed_refs = refs[frames : frames + frames * groups]
    position = frames + frames * groups
    out_weight, qkv_weight, modulation_ref, place_ref = refs[position : position + 4]
    out_refs = refs[position + 4 : position + 4 + frames]
    query_ref, kv_ref = refs[position + 4 + frames :]
    width = out_weight.shape[0]
    tokens, mixed = joined_rows(tokens_refs, mixed_refs, columns, first, piece)
    after = tokens + modulation_ref[2:3, :] * jnp.dot(
        mixed, out_weight[...], preferred_element_type=f32
    )
    normal = normalize(after) * (1.0 + modulation_ref[4:5, :]) + modulation_ref[3:4, :]
    inputs = jnp.concatenate(
        [
            (normal[frame * piece : (frame + 1) * piece] + place_ref[frame : frame + 1, :]).astype(bf16)
            for frame in range(frames)
        ],
        axis=0,
    )
    query_ref[...] = lax.dot_general(
        inputs, qkv_weight[: query_ref.shape[1], :], NT, preferred_element_type=f32
    ).astype(bf16)
    kv_ref[...] = lax.dot_general(
        inputs, qkv_weight[width:, :], NT, preferred_element_type=f32
    ).astype(bf16)

    scale = softmax_scale(head_dim)
    step = max(16, min(piece, LANES // frames))
    block = frames * step
    row_at = lax.broadcasted_iota(jnp.int32, (2 * block, block), 0) % step
    column_at = lax.broadcasted_iota(jnp.int32, (2 * block, block), 1) % step
    same = row_at == column_at
    plan = pair_plan(width, head_dim)

    def window(ref, start, tile):
        return jnp.concatenate(
            [
                ref[
                    frame * piece + start : frame * piece + start + step,
                    tile * LANES : (tile + 2) * LANES,
                ]
                for frame in range(frames)
            ],
            axis=0,
        )

    def score(start, tile, lane):
        queries = window(query_ref, start, tile)
        stacked = jnp.concatenate(
            [
                queries * column_mask(lane, head_dim, bf16),
                queries * column_mask(lane + head_dim, head_dim, bf16),
            ],
            axis=0,
        )
        scores = lax.dot_general(
            stacked, window(kv_ref, start, tile), NT, preferred_element_type=f32
        )
        return jnp.where(same, scores * scale, -jnp.inf)

    def weigh(scores):
        weights = jnp.exp2(scores - jnp.max(scores, axis=-1, keepdims=True))
        return (weights / jnp.sum(weights, axis=-1, keepdims=True)).astype(bf16)

    starts = range(0, piece, step)
    tasks = [(start, *entry) for start in starts for entry in plan]
    scores = [score(start, tile, lane) for start, tile, lane, _, _ in tasks]
    weights = [weigh(value) for value in scores]
    mixed_pairs = [
        jnp.dot(value, window(kv_ref, start, value_tile), preferred_element_type=f32)
        for value, (start, _, _, value_tile, _) in zip(weights, tasks)
    ]
    parts = {start: {} for start in starts}
    for pair, (start, tile, lane, _, value_lane) in zip(mixed_pairs, tasks):
        joined = pair[:block] * column_mask(value_lane, head_dim, f32) + pair[
            block:
        ] * column_mask(value_lane + head_dim, head_dim, f32)
        joined = pltpu.roll(joined, (lane - value_lane) % (2 * LANES), 1)
        have = parts[start]
        for side in range(2):
            half = joined[:, side * LANES : (side + 1) * LANES]
            have[tile + side] = have[tile + side] + half if tile + side in have else half
    for frame in range(frames):
        cut = slice(frame * step, (frame + 1) * step)
        out_refs[frame][...] = stack(
            [
                jnp.concatenate([parts[start][tile][cut] for start in starts], axis=0)
                for tile in sorted(parts[0])
            ],
            width,
        )


def temporal(tokens, mixed, columns, weights, modulation, places, head_dim, first, piece):
    frames = len(tokens)
    spatial_out, temporal_qkv = weights
    width, feature_width = spatial_out.shape
    padded = -(-width // LANES) * LANES
    rows = frames * piece
    return on_chip_call(
        functools.partial(
            temporal_kernel,
            frames=frames,
            head_dim=head_dim,
            columns=columns,
            first=first,
            piece=piece,
        ),
        [
            *tokens,
            *[part for frame in mixed for part in frame],
            spatial_out,
            temporal_qkv,
            modulation,
            places,
        ],
        [((stack_rows(piece, width), LANES), bf16) for _ in range(frames)],
        2 * rows * feature_width * width * 5,
        6,
        rows * 128 * 8,
        [pltpu.VMEM((rows, padded), bf16), pltpu.VMEM((rows, 2 * width), bf16)],
    )


def after_kernel(*refs, frames, columns):
    mixed_end = frames * (1 + len(columns))
    weight_ref, modulation_ref, out_ref = refs[mixed_end:]
    piece = refs[0].shape[0]
    tokens, mixed = joined_rows(refs[:frames], refs[frames:mixed_end], columns, 0, piece)
    out_ref[...] = tokens + modulation_ref[2:3, :] * jnp.dot(
        mixed, weight_ref[...], preferred_element_type=f32
    )


def after_spatial(tokens, mixed, columns, weight, modulation):
    frames = len(tokens)
    width, feature_width = weight.shape
    rows = frames * tokens[0].shape[0]
    return on_chip_call(
        functools.partial(after_kernel, frames=frames, columns=columns),
        [*tokens, *[part for frame in mixed for part in frame], weight, modulation],
        [((rows, feature_width), f32)],
        2 * rows * feature_width * width,
        6,
    )[0]


def output_kernel(slot_ref, after_ref, weight_ref, modulation_ref, *refs, frames, number):
    parts = refs[:frames]
    out_ref, stage_ref, sems = refs[-3:]
    piece = after_ref.shape[0] // frames
    half = piece // HALVES
    first = number * half
    width = weight_ref.shape[0]
    mixed = jnp.concatenate(
        [unstack(ref[...].astype(f32), half, width, 0, half).astype(bf16) for ref in parts], axis=0
    )
    after = jnp.concatenate(
        [after_ref[frame * piece + first : frame * piece + first + half, :] for frame in range(frames)],
        axis=0,
    )
    stage_ref[...] = after + modulation_ref[5:6, :] * jnp.dot(
        mixed, weight_ref[...], preferred_element_type=f32
    )
    copies = []
    for frame in range(frames):
        row = partner_slot(slot_ref[0], frame, frames) * piece + first
        copies.append(
            pltpu.make_async_copy(
                stage_ref.at[frame * half : (frame + 1) * half, :],
                out_ref.at[pl.ds(row, half), :],
                sems.at[frame],
            )
        )
        copies[-1].start()
    for copy in copies:
        copy.wait()


def output(number, slot, after, weight, modulation, parts, result):
    frames = len(parts)
    rows, feature_width = after.shape
    operands = [after, weight, modulation, *parts]
    specs = [pl.BlockSpec(memory_space=pltpu.SMEM), *vmem_specs(len(operands))]
    operands = [pltpu.with_memory_space_constraint(array, pltpu.VMEM) for array in operands]
    aliases = {}
    if result is not None:
        aliases = {len(specs): 0}
        specs.append(pl.BlockSpec(memory_space=pltpu.HBM))
        operands.append(result)
    return pl.pallas_call(
        functools.partial(output_kernel, frames=frames, number=number),
        out_shape=jax.ShapeDtypeStruct((rows, feature_width), f32),
        in_specs=specs,
        out_specs=pl.BlockSpec(memory_space=pltpu.HBM),
        scratch_shapes=[
            pltpu.VMEM((rows // HALVES, feature_width), f32),
            pltpu.SemaphoreType.DMA((frames,)),
        ],
        input_output_aliases=aliases,
        compiler_params=pltpu.CompilerParams(vmem_limit_bytes=4 * 2**20),
    )(slot, *operands)


def per_device(
    tokens,
    stale_kv,
    mod_table,
    mod_mix,
    timestep,
    frame_order,
    spatial_qkv,
    spatial_out,
    temporal_qkv,
    temporal_out,
):
    devices = lax.axis_size("patch")
    frames = devices // 4
    slot = lax.axis_index("patch") // 4
    rows, feature_width = tokens.shape
    width = spatial_out.shape[0]
    head_dim = feature_width // HEADS
    piece = rows // frames

    def other_core(device):
        return device ^ 1

    def other_chip(device):
        return device ^ 2

    def ahead(step):
        return lambda device: partner_slot(device // 4, step, frames) * 4 + device % 4

    def behind(step):
        return lambda device: source_slot(device // 4, step, frames) * 4 + device % 4

    near, far = [], []
    for chunk in stage_chunks(stale_kv, group_tiles(width, head_dim)):
        near.append(permute(chunk, other_chip))
        far.append(permute(near[-1], other_core))
    peer_kv = permute(stale_kv, other_core)

    slot_word = slot.astype(jnp.int32)[None]
    spatial_weight = jnp.swapaxes(spatial_qkv, 1, 2).reshape(3 * width, feature_width)
    pieces = stage_pieces(slot_word, tokens, frames)
    there = [pieces[0]]
    there += [permute(pieces[s], ahead(s)) for s in range(1, frames)]

    query, own_kv, modulation, places = projections(
        slot_word,
        timestep,
        frame_order,
        spatial_weight,
        mod_table,
        mod_mix,
        pieces,
        width,
    )

    carry = None
    local = [[] for _ in range(frames)]
    sent = [[] for _ in range(frames)]
    for number in range(len(PAIR_GROUPS)):
        handed = carry
        for part, chunks in enumerate(row_parts(number, rows)):
            outs, carry = spatial_group(
                number, part, query, own_kv, peer_kv, near, far, handed, frames, head_dim, width
            )
            covered = part_pieces(chunks, piece)
            for s, out in zip(covered, outs):
                local[s].append(out)
                sent[s].append(out if s == 0 else permute(out, ahead(s)))

    columns = group_columns(width, head_dim)
    after = after_spatial(pieces, local, columns, spatial_out, modulation)
    weights = (spatial_out, jnp.swapaxes(temporal_qkv, 1, 2).reshape(3 * width, feature_width))
    half = piece // HALVES
    back = []
    for h in range(HALVES):
        outs = temporal(there, sent, columns, weights, modulation, places, head_dim, h * half, half)
        back.append([out if s == 0 else permute(out, behind(s)) for s, out in enumerate(outs)])
    result = None
    for h in range(HALVES):
        result = output(h, slot_word, after, temporal_out, modulation, back[h], result)
    return result


def solution(mesh):
    split = P(("groups", "patch"), None)
    return jax.shard_map(
        per_device,
        mesh=mesh,
        in_specs=(split, split, P(), P(), P("groups"), P("groups"), P(), P(), P(), P()),
        out_specs=split,
        check_vma=False,
    )
```

```python
import functools
import math

import jax
import jax.numpy as jnp
import numpy as np
from jax import lax
from jax.experimental import pallas as pl
from jax.experimental.pallas import tpu as pltpu
from jax.sharding import PartitionSpec as P


HEADS = 16
LANES = 128
QUERY_ROWS = 128
STRIP = 16
PAIR_GROUPS = ((0,), (1,), (2, 3))
EMIT = (False, True, True)
NEAR_GROUPS = ((0,), (1,), (2,), (3,))
STAGING_FLOPS = 4 * 10**9


epsilon = 1e-06
bf16 = jnp.bfloat16
f32 = jnp.float32
NT = (((1,), (1,)), ((), ()))


def permute(value, target):
    count = lax.axis_size("patch")
    return lax.ppermute(value, "patch", [(source, target(source)) for source in range(count)])


def partner_slot(slot, step, frames):
    if frames & (frames - 1) == 0:
        return slot ^ step
    return (slot + step) % frames


def source_slot(slot, step, frames):
    if frames & (frames - 1) == 0:
        return slot ^ step
    return (slot - step) % frames


def normalize(activations):
    row_mean = jnp.mean(activations, axis=-1, keepdims=True)
    centered = activations - row_mean
    variance = jnp.mean(centered * centered, axis=-1, keepdims=True)
    return centered * lax.rsqrt(variance + epsilon)


def column_mask(first, width, dtype):
    column = lax.broadcasted_iota(jnp.int32, (1, 2 * LANES), 1)
    inside = jnp.logical_and(column >= first, column < first + width)
    return jnp.where(inside, 1.0, 0.0).astype(dtype)


def softmax_scale(head_dim):
    return math.log2(math.e) * head_dim ** (-0.5)


def vmem_specs(count):
    return [pl.BlockSpec(memory_space=pltpu.VMEM) for _ in range(count)]


def on_chip_call(kernel, operands, shapes, flops, limit_mib, transcendentals=0, scratch=()):
    operands = [pltpu.with_memory_space_constraint(array, pltpu.VMEM) for array in operands]
    return pl.pallas_call(
        kernel,
        out_shape=[pltpu.VMEM(shape, dtype) for shape, dtype in shapes],
        in_specs=vmem_specs(len(operands)),
        out_specs=vmem_specs(len(shapes)),
        scratch_shapes=list(scratch),
        compiler_params=pltpu.CompilerParams(vmem_limit_bytes=limit_mib * 2**20),
        cost_estimate=pl.CostEstimate(
            flops=flops,
            bytes_accessed=sum(array.size * array.dtype.itemsize for array in operands),
            transcendentals=transcendentals,
        ),
    )(*operands)


def tile_copies(kv_ref, out_refs, tiles, sems):
    copies = []
    for chunk, ref in zip(tiles, out_refs):
        for at, tile in enumerate(chunk):
            copies.append(
                pltpu.make_async_copy(
                    kv_ref.at[:, tile * LANES : (tile + 1) * LANES],
                    ref.at[:, at * LANES : (at + 1) * LANES],
                    sems.at[len(copies)],
                )
            )
    return copies


def first_kernel(kv_ref, out_ref, sems, *, tiles):
    copies = tile_copies(kv_ref, [out_ref], tiles, sems)
    for copy in copies:
        copy.start()
    for copy in copies:
        copy.wait()


def stage_first(stale_kv, tiles):
    return pl.pallas_call(
        functools.partial(first_kernel, tiles=[tiles]),
        out_shape=pltpu.VMEM((stale_kv.shape[0], len(tiles) * LANES), bf16),
        in_specs=[pl.BlockSpec(memory_space=pltpu.HBM)],
        out_specs=pl.BlockSpec(memory_space=pltpu.VMEM),
        scratch_shapes=[pltpu.SemaphoreType.DMA((len(tiles),))],
        compiler_params=pltpu.CompilerParams(vmem_limit_bytes=2**20),
        name="first",
    )(pltpu.with_memory_space_constraint(stale_kv, pltpu.HBM))


def piece_kernel(slot_ref, tokens_ref, kv_ref, *refs, frames, tiles):
    out_refs, piece_sems, tile_sems = refs[:-2], refs[-2], refs[-1]
    piece = tokens_ref.shape[0] // frames
    copies = []
    for step in range(frames):
        row = partner_slot(slot_ref[0], step, frames) * piece
        copies.append(
            pltpu.make_async_copy(
                tokens_ref.at[pl.ds(row, piece), :], out_refs[step], piece_sems.at[step]
            )
        )
    copies += tile_copies(kv_ref, out_refs[frames:], tiles, tile_sems)
    for copy in copies:
        copy.start()
    for copy in copies:
        copy.wait()


def stage_pieces(slot, tokens, stale_kv, tiles, frames):
    rows, feature_width = tokens.shape
    shapes = [(rows // frames, feature_width) for _ in range(frames)]
    shapes += [(rows, len(chunk) * LANES) for chunk in tiles]
    outs = pl.pallas_call(
        functools.partial(piece_kernel, frames=frames, tiles=tiles),
        out_shape=[pltpu.VMEM(shape, bf16) for shape in shapes],
        in_specs=[
            pl.BlockSpec(memory_space=pltpu.SMEM),
            pl.BlockSpec(memory_space=pltpu.HBM),
            pl.BlockSpec(memory_space=pltpu.HBM),
        ],
        out_specs=vmem_specs(len(shapes)),
        scratch_shapes=[
            pltpu.SemaphoreType.DMA((frames,)),
            pltpu.SemaphoreType.DMA((sum(len(chunk) for chunk in tiles),)),
        ],
        compiler_params=pltpu.CompilerParams(vmem_limit_bytes=2**20),
        cost_estimate=pl.CostEstimate(
            flops=STAGING_FLOPS, bytes_accessed=4 * tokens.size, transcendentals=0
        ),
        name="pieces",
    )(
        slot,
        pltpu.with_memory_space_constraint(tokens, pltpu.HBM),
        pltpu.with_memory_space_constraint(stale_kv, pltpu.HBM),
    )
    return outs[:frames], outs[frames:]


def projection_kernel(slot_ref, time_ref, order_ref, weight_ref, *refs, frames, width):
    rate_ref, table_ref, mix_ref = refs[:3]
    pieces = refs[3 : 3 + frames]
    query_ref, kv_ref, modulation_ref, place_ref = refs[3 + frames :]
    padded = query_ref.shape[1]

    rows = -(-(frames + 1) // 8) * 8
    row = lax.broadcasted_iota(jnp.int32, (rows, 1), 0)
    position = jnp.where(row == frames, time_ref[0], 0)
    for step in range(frames):
        frame = order_ref[source_slot(slot_ref[0], step, frames)]
        position = jnp.where(row == step, frame, position)
    angles = position.astype(f32) * rate_ref[...]
    waves = jnp.concatenate([jnp.sin(angles), jnp.cos(angles)], axis=1)
    place_ref[...] = waves[:frames]
    modulation = table_ref[...] + mix_ref[...] * waves[frames : frames + 1]
    modulation_ref[...] = modulation

    tokens = jnp.concatenate([ref[...] for ref in pieces], axis=0).astype(f32)
    inputs = normalize(tokens) * (1.0 + modulation[1:2, :]) + modulation[0:1, :]
    inputs = inputs.astype(bf16)
    query_ref[...] = lax.dot_general(
        inputs, weight_ref[:padded, :], NT, preferred_element_type=f32
    ).astype(bf16)
    kv_ref[...] = lax.dot_general(
        inputs, weight_ref[width:, :], NT, preferred_element_type=f32
    ).astype(bf16)


def projections(slot, timestep, frame_order, weight, mod_table, mod_mix, pieces, width):
    frames = len(pieces)
    piece, feature_width = pieces[0].shape
    padded = -(-width // LANES) * LANES
    rows = frames * piece
    half = feature_width // 2
    rates = np.exp(-math.log(10000.0) * np.arange(half) / half).astype(np.float32)
    rates = jnp.asarray(rates[None])
    operands = [
        pltpu.with_memory_space_constraint(x, pltpu.VMEM)
        for x in (weight, rates, mod_table, mod_mix, *pieces)
    ]
    return pl.pallas_call(
        functools.partial(projection_kernel, frames=frames, width=width),
        out_shape=[
            pltpu.VMEM((rows, padded), bf16),
            pltpu.VMEM((rows, 2 * width), bf16),
            pltpu.VMEM(mod_table.shape, f32),
            pltpu.VMEM((frames, feature_width), f32),
        ],
        in_specs=[
            *[pl.BlockSpec(memory_space=pltpu.SMEM) for _ in range(3)],
            *vmem_specs(4 + frames),
        ],
        out_specs=vmem_specs(4),
        compiler_params=pltpu.CompilerParams(vmem_limit_bytes=4 * 2**20),
        cost_estimate=pl.CostEstimate(
            flops=2 * rows * feature_width * 3 * width,
            bytes_accessed=2 * weight.size,
            transcendentals=0,
        ),
        name="projections",
    )(slot, timestep, frame_order, *operands)


def stack_rows(rows, width):
    return rows * width // LANES


def stack(tiles, width):
    rows = tiles[0].shape[0]
    whole = width // LANES
    stacked = list(tiles[:whole])
    if width % LANES:
        fold = tiles[whole]
        lane = lax.broadcasted_iota(jnp.int32, (1, LANES), 1)
        low = jnp.where(lane < LANES // 2, fold[: rows // 2], 0.0)
        high = jnp.where(lane < LANES // 2, fold[rows // 2 :], 0.0)
        stacked.append(low + pltpu.roll(high, LANES // 2, 1))
    return jnp.concatenate(stacked, axis=0).astype(bf16)


def unstack(stacked, rows, width, first, count):
    whole = width // LANES
    tiles = [stacked[t * rows + first : t * rows + first + count, :] for t in range(whole)]
    if width % LANES:
        half = rows // 2
        fold = stacked[whole * rows :, :]
        turned = pltpu.roll(fold.astype(f32), LANES // 2, 1).astype(stacked.dtype)
        both = jnp.concatenate([fold, turned], axis=0)
        if first % half == 0 and count == half:
            both = turned if first else fold
        else:
            both = both[first : first + count]
        tiles.append(both[:, : LANES // 2])
    return jnp.concatenate(tiles, axis=1)


def pair_plan(width, head_dim):
    plan = []
    for first in range(0, width, 2 * head_dim):
        key_tile = first // LANES
        value_tile = (width + first) // LANES
        plan.append(
            (key_tile, first - key_tile * LANES, value_tile, width + first - value_tile * LANES)
        )
    return plan


def group_tiles(width, head_dim):
    plan = pair_plan(width, head_dim)
    seen, groups = set(), []
    for group in NEAR_GROUPS:
        need = []
        for pair in group:
            key_tile, _, value_tile, _ = plan[pair]
            need += [key_tile, key_tile + 1, value_tile, value_tile + 1]
        fresh = sorted(set(need) - seen)
        seen |= set(fresh)
        groups.append(tuple(fresh))
    return groups


def spatial_kernel(*refs, group, frames, head_dim, width, tiles, held, emitted, kept, columns, chunks):
    plan = pair_plan(width, head_dim)
    count = len(tiles)
    position = 0
    refs, (scores_ref, weights_ref) = refs[:-2], refs[-2:]
    query_ref, own_ref, peer_ref = refs[:3]
    near_refs = refs[3 : 3 + count]
    far_refs = refs[3 + count : 3 + 2 * count]
    position = 3 + 2 * count
    held_ref = None
    if held:
        held_ref = refs[position]
        position += 1
    rows = query_ref.shape[0]
    piece = rows // frames
    covered = part_pieces(chunks, piece)
    out_count = len(covered) if emitted else 0
    out_refs = dict(zip(covered, refs[position : position + out_count]))
    kept_ref = refs[position + out_count] if kept else None

    where = {tile: (c, j) for c, chunk in enumerate(tiles) for j, tile in enumerate(chunk)}

    def from_chunks(chunk_refs):
        def load(tile):
            chunk, at = where[tile]
            return chunk_refs[chunk][:, at * LANES : (at + 1) * LANES]

        return load

    def from_whole(ref):
        return lambda tile: ref[:, tile * LANES : (tile + 1) * LANES]

    blocks = [from_whole(own_ref), from_whole(peer_ref), from_chunks(near_refs), from_chunks(far_refs)]
    scale = softmax_scale(head_dim)

    def two(block, tile):
        return jnp.concatenate([block(tile), block(tile + 1)], axis=1)

    def score(index):
        chunk, pair = tasks[index]
        key_tile, key_lane, _, _ = plan[pair]
        window = query_ref[
            chunk * QUERY_ROWS : (chunk + 1) * QUERY_ROWS, key_tile * LANES : (key_tile + 2) * LANES
        ]
        stacked = jnp.concatenate(
            [
                window * column_mask(key_lane, head_dim, bf16),
                window * column_mask(key_lane + head_dim, head_dim, bf16),
            ],
            axis=0,
        )
        for number, block in enumerate(blocks):
            scores_ref[index % 2, :, number * rows : (number + 1) * rows] = lax.dot_general(
                stacked, two(block, key_tile), NT, preferred_element_type=f32
            )

    def weigh(index):
        totals = []
        for row in range(0, 2 * QUERY_ROWS, STRIP):
            scores = scores_ref[index % 2, row : row + STRIP, :]
            top = jnp.max(scores, axis=-1, keepdims=True) * scale
            weights = jnp.exp2(scores * scale - top)
            totals.append(jnp.sum(weights, axis=-1, keepdims=True))
            weights_ref[index % 2, row : row + STRIP, :] = weights.astype(bf16)
        return jnp.concatenate(totals, axis=0)

    def mix(index, total):
        _, key_lane, value_tile, value_lane = plan[tasks[index][1]]
        mixed = functools.reduce(
            jnp.add,
            [
                jnp.dot(
                    weights_ref[index % 2, :, number * rows : (number + 1) * rows],
                    two(block, value_tile),
                    preferred_element_type=f32,
                )
                for number, block in enumerate(blocks)
            ],
        )
        mixed = mixed / total
        joined = mixed[:QUERY_ROWS] * column_mask(value_lane, head_dim, f32) + mixed[
            QUERY_ROWS:
        ] * column_mask(value_lane + head_dim, head_dim, f32)
        return pltpu.roll(joined, (key_lane - value_lane) % (2 * LANES), 1)

    tasks = [(chunk, pair) for chunk in chunks for pair in group]
    parts = {}

    def finish(index, total):
        chunk, pair = tasks[index]
        joined = mix(index, total)
        tile = plan[pair][0]
        for side in range(2):
            half = joined[:, side * LANES : (side + 1) * LANES]
            parts[tile + side] = parts[tile + side] + half if tile + side in parts else half
        if pair != group[-1]:
            return
        at = chunk * QUERY_ROWS
        for number, tile in enumerate(held):
            old = held_ref[at : at + QUERY_ROWS, number * LANES : (number + 1) * LANES].astype(f32)
            parts[tile] = parts[tile] + old if tile in parts else old
        if kept:
            values = jnp.concatenate([parts[tile] for tile in kept], axis=1)
            kept_ref[at : at + QUERY_ROWS, :] = values.astype(bf16)
        if emitted:
            for sub in range(QUERY_ROWS // piece):
                cut = slice(sub * piece, (sub + 1) * piece)
                out_refs[(at + sub * piece) // piece][...] = stack(
                    [parts[tile][cut] for tile in emitted], columns
                )
        parts.clear()

    score(0)
    total = None
    for index in range(len(tasks)):
        if index + 1 < len(tasks):
            score(index + 1)
        if index > 0:
            finish(index - 1, total)
        total = weigh(index)
    finish(len(tasks) - 1, total)


def near_needed(number):
    last = PAIR_GROUPS[number][-1]
    return next(n for n, group in enumerate(NEAR_GROUPS) if last in group) + 1


def tile_flow(width, head_dim):
    plan = pair_plan(width, head_dim)
    flow, held = [], ()
    for number, group in enumerate(PAIR_GROUPS):
        have = sorted({plan[pair][0] + side for pair in group for side in range(2)} | set(held))
        last = number == len(PAIR_GROUPS) - 1
        complete = [tile for tile in have if last or tile <= plan[group[-1]][0]]
        emitted = tuple(complete) if EMIT[number] else ()
        kept = tuple(tile for tile in have if tile not in emitted)
        flow.append((held, emitted, kept))
        held = kept
    return flow


def emitted_columns(emitted, width):
    return min(width, (emitted[-1] + 1) * LANES) - emitted[0] * LANES if emitted else 0


def group_columns(width, head_dim):
    flow = tile_flow(width, head_dim)
    return tuple(emitted_columns(emitted, width) for _, emitted, _ in flow if emitted)


def target_parts(rows):
    return row_parts(len(PAIR_GROUPS) - 1, rows)


def output_parts(rows, piece):
    parts = [part_pieces(chunks, piece) for chunks in target_parts(rows)]
    if len(parts) < 2:
        return parts
    return [[s for part in parts[:1] + parts[2:] for s in part], parts[1]]


def part_pieces(chunks, piece):
    per = QUERY_ROWS // piece
    return [chunk * per + sub for chunk in chunks for sub in range(per)]


def row_parts(number, rows):
    chunks = list(range(rows // QUERY_ROWS))
    if number < len(PAIR_GROUPS) - 1:
        return [chunks]
    return [[chunk] for chunk in reversed(chunks)]


def spatial_group(
    number, part, query, own_kv, peer_kv, near, far, carry, frames, head_dim, width
):
    group = PAIR_GROUPS[number]
    held, emitted, kept = tile_flow(width, head_dim)[number]
    arrived = near_needed(number)
    tiles = tuple(group_tiles(width, head_dim)[:arrived])
    rows = query.shape[0]
    chunks = row_parts(number, rows)[part]
    shapes = []
    columns = emitted_columns(emitted, width)
    if emitted:
        count = len(chunks) * QUERY_ROWS // (rows // frames)
        shapes += [((stack_rows(rows // frames, columns), LANES), bf16) for _ in range(count)]
    if kept:
        shapes.append(((rows, len(kept) * LANES), bf16))
    operands = [query, own_kv, peer_kv, *near[:arrived], *far[:arrived]]
    if held:
        operands.append(carry)
    keys = 4 * rows
    results = on_chip_call(
        functools.partial(
            spatial_kernel,
            group=group,
            frames=frames,
            head_dim=head_dim,
            width=width,
            tiles=tiles,
            held=held,
            emitted=emitted,
            kept=kept,
            columns=columns,
            chunks=chunks,
        ),
        operands,
        shapes,
        len(group) * 2 * len(chunks) * QUERY_ROWS * keys * 256 * 4,
        8,
        len(group) * 2 * rows * keys,
        [
            pltpu.VMEM((2, 2 * QUERY_ROWS, keys), f32),
            pltpu.VMEM((2, 2 * QUERY_ROWS, keys), bf16),
        ],
    )
    results = list(results)
    carry = results.pop() if kept else None
    return results, carry


def joined_rows(tokens_refs, mixed_refs, columns, first, count):
    groups = len(columns)
    piece = tokens_refs[0].shape[0]
    cut = slice(first, first + count)
    tokens = jnp.concatenate([ref[cut, :] for ref in tokens_refs], axis=0).astype(f32)
    mixed = jnp.concatenate(
        [
            jnp.concatenate(
                [
                    unstack(mixed_refs[frame * groups + g][...], piece, columns[g], first, count)
                    for g in range(groups)
                ],
                axis=1,
            )
            for frame in range(len(tokens_refs))
        ],
        axis=0,
    )
    return tokens, mixed


def temporal_in_kernel(*refs, frames, columns):
    groups = len(columns)
    tokens_refs = refs[:frames]
    mixed_refs = refs[frames : frames + frames * groups]
    out_weight, qkv_weight, modulation_ref, place_ref, query_ref, kv_ref = refs[
        frames + frames * groups :
    ]
    width = out_weight.shape[0]
    piece = tokens_refs[0].shape[0]
    tokens, mixed = joined_rows(tokens_refs, mixed_refs, columns, 0, piece)
    after = tokens + modulation_ref[2:3, :] * jnp.dot(
        mixed, out_weight[...], preferred_element_type=f32
    )
    normal = normalize(after) * (1.0 + modulation_ref[4:5, :])
    inputs = jnp.concatenate(
        [
            (
                normal[frame * piece : (frame + 1) * piece]
                + (modulation_ref[3:4, :] + place_ref[frame : frame + 1, :])
            ).astype(bf16)
            for frame in range(frames)
        ],
        axis=0,
    )
    query_ref[...] = lax.dot_general(
        inputs, qkv_weight[: query_ref.shape[1], :], NT, preferred_element_type=f32
    ).astype(bf16)
    kv_ref[...] = lax.dot_general(
        inputs, qkv_weight[width:, :], NT, preferred_element_type=f32
    ).astype(bf16)


def temporal_in(tokens, mixed, columns, weights, modulation, places):
    frames = len(tokens)
    width, feature_width = weights[0].shape
    padded = -(-width // LANES) * LANES
    rows = frames * tokens[0].shape[0]
    return on_chip_call(
        functools.partial(temporal_in_kernel, frames=frames, columns=columns),
        [*tokens, *[part for frame in mixed for part in frame], *weights, modulation, places],
        [((rows, padded), bf16), ((rows, 2 * width), bf16)],
        2 * rows * feature_width * width * 4,
        8,
    )


def temporal_kernel(query_ref, kv_ref, *out_refs, frames, head_dim, targets):
    piece = query_ref.shape[0] // frames
    width = kv_ref.shape[1] // 2
    scale = softmax_scale(head_dim)
    step = max(16, min(piece, LANES // frames))
    block = len(targets) * step
    row_at = lax.broadcasted_iota(jnp.int32, (2 * block, frames * step), 0) % step
    column_at = lax.broadcasted_iota(jnp.int32, (2 * block, frames * step), 1) % step
    same = row_at == column_at
    plan = pair_plan(width, head_dim)

    def window(ref, members, start, tile):
        return jnp.concatenate(
            [
                ref[
                    frame * piece + start : frame * piece + start + step,
                    tile * LANES : (tile + 2) * LANES,
                ]
                for frame in members
            ],
            axis=0,
        )

    def score(start, tile, lane):
        queries = window(query_ref, targets, start, tile)
        stacked = jnp.concatenate(
            [
                queries * column_mask(lane, head_dim, bf16),
                queries * column_mask(lane + head_dim, head_dim, bf16),
            ],
            axis=0,
        )
        scores = lax.dot_general(
            stacked, window(kv_ref, range(frames), start, tile), NT, preferred_element_type=f32
        )
        return jnp.where(same, scores * scale, -jnp.inf)

    def weigh(scores):
        weights = jnp.exp2(scores - jnp.max(scores, axis=-1, keepdims=True))
        return (weights / jnp.sum(weights, axis=-1, keepdims=True)).astype(bf16)

    starts = range(0, piece, step)
    tasks = [(start, *entry) for start in starts for entry in plan]
    scores = [score(start, tile, lane) for start, tile, lane, _, _ in tasks]
    weights = [weigh(value) for value in scores]
    mixed_pairs = [
        jnp.dot(
            value, window(kv_ref, range(frames), start, value_tile), preferred_element_type=f32
        )
        for value, (start, _, _, value_tile, _) in zip(weights, tasks)
    ]
    parts = {start: {} for start in starts}
    for pair, (start, tile, lane, _, value_lane) in zip(mixed_pairs, tasks):
        joined = pair[:block] * column_mask(value_lane, head_dim, f32) + pair[
            block:
        ] * column_mask(value_lane + head_dim, head_dim, f32)
        joined = pltpu.roll(joined, (lane - value_lane) % (2 * LANES), 1)
        have = parts[start]
        for side in range(2):
            half = joined[:, side * LANES : (side + 1) * LANES]
            have[tile + side] = have[tile + side] + half if tile + side in have else half
    for number in range(len(targets)):
        cut = slice(number * step, (number + 1) * step)
        out_refs[number][...] = stack(
            [
                jnp.concatenate([parts[start][tile][cut] for start in starts], axis=0)
                for tile in sorted(parts[0])
            ],
            width,
        )


def temporal(query, kv, frames, head_dim, targets):
    width = kv.shape[1] // 2
    rows = query.shape[0]
    shape = (stack_rows(rows // frames, width), LANES)
    return on_chip_call(
        functools.partial(temporal_kernel, frames=frames, head_dim=head_dim, targets=targets),
        [query, kv],
        [(shape, bf16) for _ in targets],
        2 * rows * 128 * 256 * 8,
        4,
        rows * 128 * 8,
    )


def after_kernel(*refs, frames, columns):
    mixed_end = frames * (1 + len(columns))
    weight_ref, modulation_ref, out_ref = refs[mixed_end:]
    piece = refs[0].shape[0]
    tokens, mixed = joined_rows(refs[:frames], refs[frames:mixed_end], columns, 0, piece)
    out_ref[...] = tokens + modulation_ref[2:3, :] * jnp.dot(
        mixed, weight_ref[...], preferred_element_type=f32
    )


def after_spatial(tokens, mixed, columns, weight, modulation):
    frames = len(tokens)
    width, feature_width = weight.shape
    rows = frames * tokens[0].shape[0]
    return on_chip_call(
        functools.partial(after_kernel, frames=frames, columns=columns),
        [*tokens, *[part for frame in mixed for part in frame], weight, modulation],
        [((rows, feature_width), f32)],
        2 * rows * feature_width * width,
        6,
    )[0]


def output_kernel(slot_ref, after_ref, weight_ref, modulation_ref, *refs, frames, members):
    parts = refs[: len(members)]
    out_ref, stage_ref, sems = refs[-3:]
    piece = after_ref.shape[0] // frames
    width = weight_ref.shape[0]
    mixed = jnp.concatenate(
        [unstack(ref[...].astype(f32), piece, width, 0, piece).astype(bf16) for ref in parts], axis=0
    )
    after = jnp.concatenate(
        [after_ref[frame * piece : (frame + 1) * piece, :] for frame in members], axis=0
    )
    stage_ref[...] = after + modulation_ref[5:6, :] * jnp.dot(
        mixed, weight_ref[...], preferred_element_type=f32
    )
    copies = []
    for number, frame in enumerate(members):
        row = partner_slot(slot_ref[0], frame, frames) * piece
        copies.append(
            pltpu.make_async_copy(
                stage_ref.at[number * piece : (number + 1) * piece, :],
                out_ref.at[pl.ds(row, piece), :],
                sems.at[number],
            )
        )
        copies[-1].start()
    for copy in copies:
        copy.wait()


def output(slot, after, weight, modulation, parts, members, frames, result):
    rows, feature_width = after.shape
    operands = [after, weight, modulation, *parts]
    specs = [pl.BlockSpec(memory_space=pltpu.SMEM), *vmem_specs(len(operands))]
    operands = [pltpu.with_memory_space_constraint(array, pltpu.VMEM) for array in operands]
    aliases = {}
    if result is not None:
        aliases = {len(specs): 0}
        specs.append(pl.BlockSpec(memory_space=pltpu.HBM))
        operands.append(result)
    return pl.pallas_call(
        functools.partial(output_kernel, frames=frames, members=members),
        out_shape=jax.ShapeDtypeStruct((rows, feature_width), f32),
        in_specs=specs,
        out_specs=pl.BlockSpec(memory_space=pltpu.HBM),
        scratch_shapes=[
            pltpu.VMEM((rows // frames * len(members), feature_width), f32),
            pltpu.SemaphoreType.DMA((len(members),)),
        ],
        input_output_aliases=aliases,
        compiler_params=pltpu.CompilerParams(vmem_limit_bytes=6 * 2**20),
    )(slot, *operands)


def per_device(
    tokens,
    stale_kv,
    mod_table,
    mod_mix,
    timestep,
    frame_order,
    spatial_qkv,
    spatial_out,
    temporal_qkv,
    temporal_out,
):
    devices = lax.axis_size("patch")
    frames = devices // 4
    slot = lax.axis_index("patch") // 4
    rows, feature_width = tokens.shape
    width = spatial_out.shape[0]
    head_dim = feature_width // HEADS
    piece = rows // frames

    def other_core(device):
        return device ^ 1

    def other_chip(device):
        return device ^ 2

    def ahead(step):
        return lambda device: partner_slot(device // 4, step, frames) * 4 + device % 4

    def behind(step):
        return lambda device: source_slot(device // 4, step, frames) * 4 + device % 4

    slot_word = slot.astype(jnp.int32)[None]
    tiles = group_tiles(width, head_dim)
    chunks = [stage_first(stale_kv, tiles[0])]
    pieces, others = stage_pieces(slot_word, tokens, stale_kv, tiles[1:], frames)
    near, far = [], []
    for chunk in [*chunks, *others]:
        near.append(permute(chunk, other_chip))
        far.append(permute(near[-1], other_core))
    peer_kv = permute(stale_kv, other_core)

    spatial_weight = jnp.swapaxes(spatial_qkv, 1, 2).reshape(3 * width, feature_width)
    there = [pieces[0]]
    there += [permute(pieces[s], ahead(s)) for s in range(1, frames)]

    query, own_kv, modulation, places = projections(
        slot_word,
        timestep,
        frame_order,
        spatial_weight,
        mod_table,
        mod_mix,
        pieces,
        width,
    )

    carry = None
    local = [[] for _ in range(frames)]
    sent = [[] for _ in range(frames)]
    for number in range(len(PAIR_GROUPS)):
        handed = carry
        for part, chunks in enumerate(row_parts(number, rows)):
            outs, carry = spatial_group(
                number, part, query, own_kv, peer_kv, near, far, handed, frames, head_dim, width
            )
            covered = part_pieces(chunks, piece)
            for s, out in zip(covered, outs):
                local[s].append(out)
                sent[s].append(out if s == 0 else permute(out, ahead(s)))

    columns = group_columns(width, head_dim)
    after = after_spatial(pieces, local, columns, spatial_out, modulation)
    weights = (spatial_out, jnp.swapaxes(temporal_qkv, 1, 2).reshape(3 * width, feature_width))
    temporal_query, temporal_kv = temporal_in(there, sent, columns, weights, modulation, places)
    back = {}
    for chunks in target_parts(rows):
        targets = part_pieces(chunks, piece)
        outs = temporal(temporal_query, temporal_kv, frames, head_dim, targets)
        for s, out in zip(targets, outs):
            back[s] = out if s == 0 else permute(out, behind(s))
    result = None
    for members in output_parts(rows, piece):
        parts = [back[s] for s in members]
        result = output(slot_word, after, temporal_out, modulation, parts, members, frames, result)
    return result


def solution(mesh):
    split = P(("groups", "patch"), None)
    return jax.shard_map(
        per_device,
        mesh=mesh,
        in_specs=(split, split, P(), P(), P("groups"), P("groups"), P(), P(), P(), P()),
        out_specs=split,
        check_vma=False,
    )
```

```python
import functools
import math

import jax
import jax.numpy as jnp
import numpy as np
from jax import lax
from jax.experimental import pallas as pl
from jax.experimental.pallas import tpu as pltpu
from jax.sharding import PartitionSpec as P


HEADS = 16
LANES = 128
QUERY_ROWS = 128
STRIP = 16
PAIR_GROUPS = ((0,), (1,), (2, 3))
EMIT = (False, True, True)
NEAR_GROUPS = ((0,), (1,), (2,), (3,))
STAGING_FLOPS = 4 * 10**9


epsilon = 1e-06
bf16 = jnp.bfloat16
f32 = jnp.float32
NT = (((1,), (1,)), ((), ()))


def permute(value, target):
    count = lax.axis_size("patch")
    return lax.ppermute(value, "patch", [(source, target(source)) for source in range(count)])


def partner_slot(slot, step, frames):
    if frames & (frames - 1) == 0:
        return slot ^ step
    return (slot + step) % frames


def source_slot(slot, step, frames):
    if frames & (frames - 1) == 0:
        return slot ^ step
    return (slot - step) % frames


def normalize(activations):
    row_mean = jnp.mean(activations, axis=-1, keepdims=True)
    centered = activations - row_mean
    variance = jnp.mean(centered * centered, axis=-1, keepdims=True)
    return centered * lax.rsqrt(variance + epsilon)


def column_mask(first, width, dtype):
    column = lax.broadcasted_iota(jnp.int32, (1, 2 * LANES), 1)
    inside = jnp.logical_and(column >= first, column < first + width)
    return jnp.where(inside, 1.0, 0.0).astype(dtype)


def softmax_scale(head_dim):
    return math.log2(math.e) * head_dim ** (-0.5)


def vmem_specs(count):
    return [pl.BlockSpec(memory_space=pltpu.VMEM) for _ in range(count)]


def on_chip_call(kernel, operands, shapes, flops, limit_mib, transcendentals=0, scratch=()):
    operands = [pltpu.with_memory_space_constraint(array, pltpu.VMEM) for array in operands]
    return pl.pallas_call(
        kernel,
        out_shape=[pltpu.VMEM(shape, dtype) for shape, dtype in shapes],
        in_specs=vmem_specs(len(operands)),
        out_specs=vmem_specs(len(shapes)),
        scratch_shapes=list(scratch),
        compiler_params=pltpu.CompilerParams(vmem_limit_bytes=limit_mib * 2**20),
        cost_estimate=pl.CostEstimate(
            flops=flops,
            bytes_accessed=sum(array.size * array.dtype.itemsize for array in operands),
            transcendentals=transcendentals,
        ),
    )(*operands)


def tile_copies(kv_ref, out_refs, tiles, sems):
    copies = []
    for chunk, ref in zip(tiles, out_refs):
        for at, tile in enumerate(chunk):
            copies.append(
                pltpu.make_async_copy(
                    kv_ref.at[:, tile * LANES : (tile + 1) * LANES],
                    ref.at[:, at * LANES : (at + 1) * LANES],
                    sems.at[len(copies)],
                )
            )
    return copies


def first_kernel(kv_ref, out_ref, sems, *, tiles):
    copies = tile_copies(kv_ref, [out_ref], tiles, sems)
    for copy in copies:
        copy.start()
    for copy in copies:
        copy.wait()


def stage_first(stale_kv, tiles):
    return pl.pallas_call(
        functools.partial(first_kernel, tiles=[tiles]),
        out_shape=pltpu.VMEM((stale_kv.shape[0], len(tiles) * LANES), bf16),
        in_specs=[pl.BlockSpec(memory_space=pltpu.HBM)],
        out_specs=pl.BlockSpec(memory_space=pltpu.VMEM),
        scratch_shapes=[pltpu.SemaphoreType.DMA((len(tiles),))],
        compiler_params=pltpu.CompilerParams(vmem_limit_bytes=2**20),
        name="first",
    )(pltpu.with_memory_space_constraint(stale_kv, pltpu.HBM))


def piece_kernel(slot_ref, tokens_ref, kv_ref, *refs, frames, tiles):
    out_refs, piece_sems, tile_sems = refs[:-2], refs[-2], refs[-1]
    piece = tokens_ref.shape[0] // frames
    copies = []
    for step in range(frames):
        row = partner_slot(slot_ref[0], step, frames) * piece
        copies.append(
            pltpu.make_async_copy(
                tokens_ref.at[pl.ds(row, piece), :], out_refs[step], piece_sems.at[step]
            )
        )
    copies += tile_copies(kv_ref, out_refs[frames:], tiles, tile_sems)
    for copy in copies:
        copy.start()
    for copy in copies:
        copy.wait()


def stage_pieces(slot, tokens, stale_kv, tiles, frames):
    rows, feature_width = tokens.shape
    shapes = [(rows // frames, feature_width) for _ in range(frames)]
    shapes += [(rows, len(chunk) * LANES) for chunk in tiles]
    outs = pl.pallas_call(
        functools.partial(piece_kernel, frames=frames, tiles=tiles),
        out_shape=[pltpu.VMEM(shape, bf16) for shape in shapes],
        in_specs=[
            pl.BlockSpec(memory_space=pltpu.SMEM),
            pl.BlockSpec(memory_space=pltpu.HBM),
            pl.BlockSpec(memory_space=pltpu.HBM),
        ],
        out_specs=vmem_specs(len(shapes)),
        scratch_shapes=[
            pltpu.SemaphoreType.DMA((frames,)),
            pltpu.SemaphoreType.DMA((sum(len(chunk) for chunk in tiles),)),
        ],
        compiler_params=pltpu.CompilerParams(vmem_limit_bytes=2**20),
        cost_estimate=pl.CostEstimate(
            flops=STAGING_FLOPS, bytes_accessed=4 * tokens.size, transcendentals=0
        ),
        name="pieces",
    )(
        slot,
        pltpu.with_memory_space_constraint(tokens, pltpu.HBM),
        pltpu.with_memory_space_constraint(stale_kv, pltpu.HBM),
    )
    return outs[:frames], outs[frames:]


def projection_kernel(slot_ref, time_ref, order_ref, weight_ref, *refs, frames, width):
    rate_ref, table_ref, mix_ref = refs[:3]
    pieces = refs[3 : 3 + frames]
    query_ref, kv_ref, modulation_ref, place_ref = refs[3 + frames :]
    padded = query_ref.shape[1]

    rows = -(-(frames + 1) // 8) * 8
    row = lax.broadcasted_iota(jnp.int32, (rows, 1), 0)
    position = jnp.where(row == frames, time_ref[0], 0)
    for step in range(frames):
        frame = order_ref[source_slot(slot_ref[0], step, frames)]
        position = jnp.where(row == step, frame, position)
    angles = position.astype(f32) * rate_ref[...]
    waves = jnp.concatenate([jnp.sin(angles), jnp.cos(angles)], axis=1)
    place_ref[...] = waves[:frames]
    modulation = table_ref[...] + mix_ref[...] * waves[frames : frames + 1]
    modulation_ref[...] = modulation

    tokens = jnp.concatenate([ref[...] for ref in pieces], axis=0).astype(f32)
    inputs = normalize(tokens) * (1.0 + modulation[1:2, :]) + modulation[0:1, :]
    inputs = inputs.astype(bf16)
    query_ref[...] = lax.dot_general(
        inputs, weight_ref[:padded, :], NT, preferred_element_type=f32
    ).astype(bf16)
    kv_ref[...] = lax.dot_general(
        inputs, weight_ref[width:, :], NT, preferred_element_type=f32
    ).astype(bf16)


def projections(slot, timestep, frame_order, weight, mod_table, mod_mix, pieces, width):
    frames = len(pieces)
    piece, feature_width = pieces[0].shape
    padded = -(-width // LANES) * LANES
    rows = frames * piece
    half = feature_width // 2
    rates = np.exp(-math.log(10000.0) * np.arange(half) / half).astype(np.float32)
    rates = jnp.asarray(rates[None])
    operands = [
        pltpu.with_memory_space_constraint(x, pltpu.VMEM)
        for x in (weight, rates, mod_table, mod_mix, *pieces)
    ]
    return pl.pallas_call(
        functools.partial(projection_kernel, frames=frames, width=width),
        out_shape=[
            pltpu.VMEM((rows, padded), bf16),
            pltpu.VMEM((rows, 2 * width), bf16),
            pltpu.VMEM(mod_table.shape, f32),
            pltpu.VMEM((frames, feature_width), f32),
        ],
        in_specs=[
            *[pl.BlockSpec(memory_space=pltpu.SMEM) for _ in range(3)],
            *vmem_specs(4 + frames),
        ],
        out_specs=vmem_specs(4),
        compiler_params=pltpu.CompilerParams(vmem_limit_bytes=4 * 2**20),
        cost_estimate=pl.CostEstimate(
            flops=2 * rows * feature_width * 3 * width,
            bytes_accessed=2 * weight.size,
            transcendentals=0,
        ),
        name="projections",
    )(slot, timestep, frame_order, *operands)


def stack_rows(rows, width):
    return rows * width // LANES


def stack(tiles, width):
    rows = tiles[0].shape[0]
    whole = width // LANES
    stacked = list(tiles[:whole])
    if width % LANES:
        fold = tiles[whole]
        lane = lax.broadcasted_iota(jnp.int32, (1, LANES), 1)
        low = jnp.where(lane < LANES // 2, fold[: rows // 2], 0.0)
        high = jnp.where(lane < LANES // 2, fold[rows // 2 :], 0.0)
        stacked.append(low + pltpu.roll(high, LANES // 2, 1))
    return jnp.concatenate(stacked, axis=0).astype(bf16)


def unstack(stacked, rows, width, first, count):
    whole = width // LANES
    tiles = [stacked[t * rows + first : t * rows + first + count, :] for t in range(whole)]
    if width % LANES:
        half = rows // 2
        fold = stacked[whole * rows :, :]
        turned = pltpu.roll(fold.astype(f32), LANES // 2, 1).astype(stacked.dtype)
        both = jnp.concatenate([fold, turned], axis=0)
        if first % half == 0 and count == half:
            both = turned if first else fold
        else:
            both = both[first : first + count]
        tiles.append(both[:, : LANES // 2])
    return jnp.concatenate(tiles, axis=1)


def pair_plan(width, head_dim):
    plan = []
    for first in range(0, width, 2 * head_dim):
        key_tile = first // LANES
        value_tile = (width + first) // LANES
        plan.append(
            (key_tile, first - key_tile * LANES, value_tile, width + first - value_tile * LANES)
        )
    return plan


def group_tiles(width, head_dim):
    plan = pair_plan(width, head_dim)
    seen, groups = set(), []
    for group in NEAR_GROUPS:
        need = []
        for pair in group:
            key_tile, _, value_tile, _ = plan[pair]
            need += [key_tile, key_tile + 1, value_tile, value_tile + 1]
        fresh = sorted(set(need) - seen)
        seen |= set(fresh)
        groups.append(tuple(fresh))
    return groups


def spatial_kernel(*refs, group, frames, head_dim, width, tiles, held, emitted, kept, columns, chunks):
    plan = pair_plan(width, head_dim)
    count = len(tiles)
    position = 0
    refs, (scores_ref, weights_ref) = refs[:-2], refs[-2:]
    query_ref, own_ref, peer_ref = refs[:3]
    near_refs = refs[3 : 3 + count]
    far_refs = refs[3 + count : 3 + 2 * count]
    position = 3 + 2 * count
    held_ref = None
    if held:
        held_ref = refs[position]
        position += 1
    rows = query_ref.shape[0]
    piece = rows // frames
    covered = part_pieces(chunks, piece)
    out_count = len(covered) if emitted else 0
    out_refs = dict(zip(covered, refs[position : position + out_count]))
    kept_ref = refs[position + out_count] if kept else None

    where = {tile: (c, j) for c, chunk in enumerate(tiles) for j, tile in enumerate(chunk)}

    def from_chunks(chunk_refs):
        def load(tile):
            chunk, at = where[tile]
            return chunk_refs[chunk][:, at * LANES : (at + 1) * LANES]

        return load

    def from_whole(ref):
        return lambda tile: ref[:, tile * LANES : (tile + 1) * LANES]

    blocks = [from_whole(own_ref), from_whole(peer_ref), from_chunks(near_refs), from_chunks(far_refs)]
    scale = softmax_scale(head_dim)

    def two(block, tile):
        return jnp.concatenate([block(tile), block(tile + 1)], axis=1)

    def score(index):
        chunk, pair = tasks[index]
        key_tile, key_lane, _, _ = plan[pair]
        window = query_ref[
            chunk * QUERY_ROWS : (chunk + 1) * QUERY_ROWS, key_tile * LANES : (key_tile + 2) * LANES
        ]
        stacked = jnp.concatenate(
            [
                window * column_mask(key_lane, head_dim, bf16),
                window * column_mask(key_lane + head_dim, head_dim, bf16),
            ],
            axis=0,
        )
        for number, block in enumerate(blocks):
            scores_ref[index % 2, :, number * rows : (number + 1) * rows] = lax.dot_general(
                stacked, two(block, key_tile), NT, preferred_element_type=f32
            )

    def weigh(index):
        totals = []
        for row in range(0, 2 * QUERY_ROWS, STRIP):
            scores = scores_ref[index % 2, row : row + STRIP, :]
            top = jnp.max(scores, axis=-1, keepdims=True) * scale
            weights = jnp.exp2(scores * scale - top)
            totals.append(jnp.sum(weights, axis=-1, keepdims=True))
            weights_ref[index % 2, row : row + STRIP, :] = weights.astype(bf16)
        return jnp.concatenate(totals, axis=0)

    def mix(index, total):
        _, key_lane, value_tile, value_lane = plan[tasks[index][1]]
        mixed = functools.reduce(
            jnp.add,
            [
                jnp.dot(
                    weights_ref[index % 2, :, number * rows : (number + 1) * rows],
                    two(block, value_tile),
                    preferred_element_type=f32,
                )
                for number, block in enumerate(blocks)
            ],
        )
        mixed = mixed / total
        joined = mixed[:QUERY_ROWS] * column_mask(value_lane, head_dim, f32) + mixed[
            QUERY_ROWS:
        ] * column_mask(value_lane + head_dim, head_dim, f32)
        return pltpu.roll(joined, (key_lane - value_lane) % (2 * LANES), 1)

    tasks = [(chunk, pair) for chunk in chunks for pair in group]
    parts = {}

    def finish(index, total):
        chunk, pair = tasks[index]
        joined = mix(index, total)
        tile = plan[pair][0]
        for side in range(2):
            half = joined[:, side * LANES : (side + 1) * LANES]
            parts[tile + side] = parts[tile + side] + half if tile + side in parts else half
        if pair != group[-1]:
            return
        at = chunk * QUERY_ROWS
        for number, tile in enumerate(held):
            old = held_ref[at : at + QUERY_ROWS, number * LANES : (number + 1) * LANES].astype(f32)
            parts[tile] = parts[tile] + old if tile in parts else old
        if kept:
            values = jnp.concatenate([parts[tile] for tile in kept], axis=1)
            kept_ref[at : at + QUERY_ROWS, :] = values.astype(bf16)
        if emitted:
            for sub in range(QUERY_ROWS // piece):
                cut = slice(sub * piece, (sub + 1) * piece)
                out_refs[(at + sub * piece) // piece][...] = stack(
                    [parts[tile][cut] for tile in emitted], columns
                )
        parts.clear()

    score(0)
    total = None
    for index in range(len(tasks)):
        if index + 1 < len(tasks):
            score(index + 1)
        if index > 0:
            finish(index - 1, total)
        total = weigh(index)
    finish(len(tasks) - 1, total)


def near_needed(number):
    last = PAIR_GROUPS[number][-1]
    return next(n for n, group in enumerate(NEAR_GROUPS) if last in group) + 1


def tile_flow(width, head_dim):
    plan = pair_plan(width, head_dim)
    flow, held = [], ()
    for number, group in enumerate(PAIR_GROUPS):
        have = sorted({plan[pair][0] + side for pair in group for side in range(2)} | set(held))
        last = number == len(PAIR_GROUPS) - 1
        complete = [tile for tile in have if last or tile <= plan[group[-1]][0]]
        emitted = tuple(complete) if EMIT[number] else ()
        kept = tuple(tile for tile in have if tile not in emitted)
        flow.append((held, emitted, kept))
        held = kept
    return flow


def emitted_columns(emitted, width):
    return min(width, (emitted[-1] + 1) * LANES) - emitted[0] * LANES if emitted else 0


def group_columns(width, head_dim):
    flow = tile_flow(width, head_dim)
    return tuple(emitted_columns(emitted, width) for _, emitted, _ in flow if emitted)


def target_parts(rows):
    return row_parts(len(PAIR_GROUPS) - 1, rows)


def input_halves(rows, piece):
    parts = [part_pieces(chunks, piece) for chunks in target_parts(rows)]
    if len(parts) < 3:
        return [[s for part in parts for s in part]]
    return [parts[-1] + parts[0], [s for part in parts[1:-1] for s in part]]


def output_parts(rows, piece):
    parts = [part_pieces(chunks, piece) for chunks in target_parts(rows)]
    if len(parts) < 3:
        return [[s for part in parts for s in part]]
    return [[s for part in parts[2:] for s in part], parts[0] + parts[1]]


def part_pieces(chunks, piece):
    per = QUERY_ROWS // piece
    return [chunk * per + sub for chunk in chunks for sub in range(per)]


def row_parts(number, rows):
    chunks = list(range(rows // QUERY_ROWS))
    if number < len(PAIR_GROUPS) - 1:
        return [chunks]
    return [[chunk] for chunk in reversed(chunks)]


def spatial_group(
    number, part, query, own_kv, peer_kv, near, far, carry, frames, head_dim, width
):
    group = PAIR_GROUPS[number]
    held, emitted, kept = tile_flow(width, head_dim)[number]
    arrived = near_needed(number)
    tiles = tuple(group_tiles(width, head_dim)[:arrived])
    rows = query.shape[0]
    chunks = row_parts(number, rows)[part]
    shapes = []
    columns = emitted_columns(emitted, width)
    if emitted:
        count = len(chunks) * QUERY_ROWS // (rows // frames)
        shapes += [((stack_rows(rows // frames, columns), LANES), bf16) for _ in range(count)]
    if kept:
        shapes.append(((rows, len(kept) * LANES), bf16))
    operands = [query, own_kv, peer_kv, *near[:arrived], *far[:arrived]]
    if held:
        operands.append(carry)
    keys = 4 * rows
    results = on_chip_call(
        functools.partial(
            spatial_kernel,
            group=group,
            frames=frames,
            head_dim=head_dim,
            width=width,
            tiles=tiles,
            held=held,
            emitted=emitted,
            kept=kept,
            columns=columns,
            chunks=chunks,
        ),
        operands,
        shapes,
        len(group) * 2 * len(chunks) * QUERY_ROWS * keys * 256 * 4,
        8,
        len(group) * 2 * rows * keys,
        [
            pltpu.VMEM((2, 2 * QUERY_ROWS, keys), f32),
            pltpu.VMEM((2, 2 * QUERY_ROWS, keys), bf16),
        ],
    )
    results = list(results)
    carry = results.pop() if kept else None
    return results, carry


def joined_rows(tokens_refs, mixed_refs, columns, first, count):
    groups = len(columns)
    piece = tokens_refs[0].shape[0]
    cut = slice(first, first + count)
    tokens = jnp.concatenate([ref[cut, :] for ref in tokens_refs], axis=0).astype(f32)
    mixed = jnp.concatenate(
        [
            jnp.concatenate(
                [
                    unstack(mixed_refs[frame * groups + g][...], piece, columns[g], first, count)
                    for g in range(groups)
                ],
                axis=1,
            )
            for frame in range(len(tokens_refs))
        ],
        axis=0,
    )
    return tokens, mixed


def temporal_in_kernel(*refs, members, columns):
    groups, frames = len(columns), len(members)
    tokens_refs = refs[:frames]
    mixed_refs = refs[frames : frames + frames * groups]
    out_weight, qkv_weight, modulation_ref, place_ref, query_ref, kv_ref = refs[
        frames + frames * groups :
    ]
    width = out_weight.shape[0]
    piece = tokens_refs[0].shape[0]
    tokens, mixed = joined_rows(tokens_refs, mixed_refs, columns, 0, piece)
    after = tokens + modulation_ref[2:3, :] * jnp.dot(
        mixed, out_weight[...], preferred_element_type=f32
    )
    normal = normalize(after) * (1.0 + modulation_ref[4:5, :])
    inputs = jnp.concatenate(
        [
            (
                normal[frame * piece : (frame + 1) * piece]
                + (modulation_ref[3:4, :] + place_ref[member : member + 1, :])
            ).astype(bf16)
            for frame, member in enumerate(members)
        ],
        axis=0,
    )
    query_ref[...] = lax.dot_general(
        inputs, qkv_weight[: query_ref.shape[1], :], NT, preferred_element_type=f32
    ).astype(bf16)
    kv_ref[...] = lax.dot_general(
        inputs, qkv_weight[width:, :], NT, preferred_element_type=f32
    ).astype(bf16)


def temporal_in(members, tokens, mixed, columns, weights, modulation, places):
    width, feature_width = weights[0].shape
    padded = -(-width // LANES) * LANES
    rows = len(members) * tokens[0].shape[0]
    return on_chip_call(
        functools.partial(temporal_in_kernel, members=members, columns=columns),
        [
            *[tokens[s] for s in members],
            *[part for s in members for part in mixed[s]],
            *weights,
            modulation,
            places,
        ],
        [((rows, padded), bf16), ((rows, 2 * width), bf16)],
        2 * rows * feature_width * width * 4,
        8,
    )


def temporal_kernel(*refs, frames, head_dim, targets, halves):
    query_refs, kv_refs = refs[: len(halves)], refs[len(halves) : 2 * len(halves)]
    out_refs = refs[2 * len(halves) :]
    piece = sum(ref.shape[0] for ref in query_refs) // frames
    width = kv_refs[0].shape[1] // 2
    where = {s: (h, at) for h, members in enumerate(halves) for at, s in enumerate(members)}
    scale = softmax_scale(head_dim)
    step = max(16, min(piece, LANES // frames))
    block = len(targets) * step
    row_at = lax.broadcasted_iota(jnp.int32, (2 * block, frames * step), 0) % step
    column_at = lax.broadcasted_iota(jnp.int32, (2 * block, frames * step), 1) % step
    same = row_at == column_at
    plan = pair_plan(width, head_dim)

    def window(half_refs, members, start, tile):
        rows = []
        for s in members:
            half, at = where[s]
            first = at * piece + start
            rows.append(half_refs[half][first : first + step, tile * LANES : (tile + 2) * LANES])
        return jnp.concatenate(rows, axis=0)

    def score(start, tile, lane):
        queries = window(query_refs, targets, start, tile)
        stacked = jnp.concatenate(
            [
                queries * column_mask(lane, head_dim, bf16),
                queries * column_mask(lane + head_dim, head_dim, bf16),
            ],
            axis=0,
        )
        scores = lax.dot_general(
            stacked, window(kv_refs, range(frames), start, tile), NT, preferred_element_type=f32
        )
        return jnp.where(same, scores * scale, -jnp.inf)

    def weigh(scores):
        weights = jnp.exp2(scores - jnp.max(scores, axis=-1, keepdims=True))
        return (weights / jnp.sum(weights, axis=-1, keepdims=True)).astype(bf16)

    starts = range(0, piece, step)
    tasks = [(start, *entry) for start in starts for entry in plan]
    scores = [score(start, tile, lane) for start, tile, lane, _, _ in tasks]
    weights = [weigh(value) for value in scores]
    mixed_pairs = [
        jnp.dot(
            value, window(kv_refs, range(frames), start, value_tile), preferred_element_type=f32
        )
        for value, (start, _, _, value_tile, _) in zip(weights, tasks)
    ]
    parts = {start: {} for start in starts}
    for pair, (start, tile, lane, _, value_lane) in zip(mixed_pairs, tasks):
        joined = pair[:block] * column_mask(value_lane, head_dim, f32) + pair[
            block:
        ] * column_mask(value_lane + head_dim, head_dim, f32)
        joined = pltpu.roll(joined, (lane - value_lane) % (2 * LANES), 1)
        have = parts[start]
        for side in range(2):
            half = joined[:, side * LANES : (side + 1) * LANES]
            have[tile + side] = have[tile + side] + half if tile + side in have else half
    for number in range(len(targets)):
        cut = slice(number * step, (number + 1) * step)
        out_refs[number][...] = stack(
            [
                jnp.concatenate([parts[start][tile][cut] for start in starts], axis=0)
                for tile in sorted(parts[0])
            ],
            width,
        )


def temporal(queries, kvs, halves, frames, head_dim, targets):
    width = kvs[0].shape[1] // 2
    rows = sum(query.shape[0] for query in queries)
    shape = (stack_rows(rows // frames, width), LANES)
    return on_chip_call(
        functools.partial(
            temporal_kernel, frames=frames, head_dim=head_dim, targets=targets, halves=halves
        ),
        [*queries, *kvs],
        [(shape, bf16) for _ in targets],
        2 * rows * 128 * 256 * 8,
        4,
        rows * 128 * 8,
    )


def after_kernel(*refs, frames, columns):
    mixed_end = frames * (1 + len(columns))
    weight_ref, modulation_ref, out_ref = refs[mixed_end:]
    piece = refs[0].shape[0]
    tokens, mixed = joined_rows(refs[:frames], refs[frames:mixed_end], columns, 0, piece)
    out_ref[...] = tokens + modulation_ref[2:3, :] * jnp.dot(
        mixed, weight_ref[...], preferred_element_type=f32
    )


def after_spatial(tokens, mixed, columns, weight, modulation):
    frames = len(tokens)
    width, feature_width = weight.shape
    rows = frames * tokens[0].shape[0]
    return on_chip_call(
        functools.partial(after_kernel, frames=frames, columns=columns),
        [*tokens, *[part for frame in mixed for part in frame], weight, modulation],
        [((rows, feature_width), f32)],
        2 * rows * feature_width * width,
        6,
    )[0]


def output_kernel(slot_ref, after_ref, weight_ref, modulation_ref, *refs, frames, members):
    parts = refs[: len(members)]
    out_ref, stage_ref, sems = refs[-3:]
    piece = after_ref.shape[0] // frames
    width = weight_ref.shape[0]
    mixed = jnp.concatenate(
        [unstack(ref[...].astype(f32), piece, width, 0, piece).astype(bf16) for ref in parts], axis=0
    )
    after = jnp.concatenate(
        [after_ref[frame * piece : (frame + 1) * piece, :] for frame in members], axis=0
    )
    stage_ref[...] = after + modulation_ref[5:6, :] * jnp.dot(
        mixed, weight_ref[...], preferred_element_type=f32
    )
    copies = []
    for number, frame in enumerate(members):
        row = partner_slot(slot_ref[0], frame, frames) * piece
        copies.append(
            pltpu.make_async_copy(
                stage_ref.at[number * piece : (number + 1) * piece, :],
                out_ref.at[pl.ds(row, piece), :],
                sems.at[number],
            )
        )
        copies[-1].start()
    for copy in copies:
        copy.wait()


def output(slot, after, weight, modulation, parts, members, frames, result):
    rows, feature_width = after.shape
    operands = [after, weight, modulation, *parts]
    specs = [pl.BlockSpec(memory_space=pltpu.SMEM), *vmem_specs(len(operands))]
    operands = [pltpu.with_memory_space_constraint(array, pltpu.VMEM) for array in operands]
    aliases = {}
    if result is not None:
        aliases = {len(specs): 0}
        specs.append(pl.BlockSpec(memory_space=pltpu.HBM))
        operands.append(result)
    return pl.pallas_call(
        functools.partial(output_kernel, frames=frames, members=members),
        out_shape=jax.ShapeDtypeStruct((rows, feature_width), f32),
        in_specs=specs,
        out_specs=pl.BlockSpec(memory_space=pltpu.HBM),
        scratch_shapes=[
            pltpu.VMEM((rows // frames * len(members), feature_width), f32),
            pltpu.SemaphoreType.DMA((len(members),)),
        ],
        input_output_aliases=aliases,
        compiler_params=pltpu.CompilerParams(vmem_limit_bytes=6 * 2**20),
    )(slot, *operands)


def per_device(
    tokens,
    stale_kv,
    mod_table,
    mod_mix,
    timestep,
    frame_order,
    spatial_qkv,
    spatial_out,
    temporal_qkv,
    temporal_out,
):
    devices = lax.axis_size("patch")
    frames = devices // 4
    slot = lax.axis_index("patch") // 4
    rows, feature_width = tokens.shape
    width = spatial_out.shape[0]
    head_dim = feature_width // HEADS
    piece = rows // frames

    def other_core(device):
        return device ^ 1

    def other_chip(device):
        return device ^ 2

    def ahead(step):
        return lambda device: partner_slot(device // 4, step, frames) * 4 + device % 4

    def behind(step):
        return lambda device: source_slot(device // 4, step, frames) * 4 + device % 4

    slot_word = slot.astype(jnp.int32)[None]
    tiles = group_tiles(width, head_dim)
    chunks = [stage_first(stale_kv, tiles[0])]
    pieces, others = stage_pieces(slot_word, tokens, stale_kv, tiles[1:], frames)
    near, far = [], []
    for chunk in [*chunks, *others]:
        near.append(permute(chunk, other_chip))
        far.append(permute(near[-1], other_core))
    peer_kv = permute(stale_kv, other_core)

    spatial_weight = jnp.swapaxes(spatial_qkv, 1, 2).reshape(3 * width, feature_width)
    there = [pieces[0]]
    there += [permute(pieces[s], ahead(s)) for s in range(1, frames)]

    query, own_kv, modulation, places = projections(
        slot_word,
        timestep,
        frame_order,
        spatial_weight,
        mod_table,
        mod_mix,
        pieces,
        width,
    )

    carry = None
    local = [[] for _ in range(frames)]
    sent = [[] for _ in range(frames)]
    for number in range(len(PAIR_GROUPS)):
        handed = carry
        for part, chunks in enumerate(row_parts(number, rows)):
            outs, carry = spatial_group(
                number, part, query, own_kv, peer_kv, near, far, handed, frames, head_dim, width
            )
            covered = part_pieces(chunks, piece)
            for s, out in zip(covered, outs):
                local[s].append(out)
                sent[s].append(out if s == 0 else permute(out, ahead(s)))

    columns = group_columns(width, head_dim)
    after = after_spatial(pieces, local, columns, spatial_out, modulation)
    weights = (spatial_out, jnp.swapaxes(temporal_qkv, 1, 2).reshape(3 * width, feature_width))
    halves = input_halves(rows, piece)
    inputs = [
        temporal_in(members, there, sent, columns, weights, modulation, places)
        for members in halves
    ]
    queries, kvs = [query for query, _ in inputs], [kv for _, kv in inputs]
    back = {}
    for chunks in target_parts(rows):
        targets = part_pieces(chunks, piece)
        outs = temporal(queries, kvs, halves, frames, head_dim, targets)
        for s, out in zip(targets, outs):
            back[s] = out if s == 0 else permute(out, behind(s))
    result = None
    for members in output_parts(rows, piece):
        parts = [back[s] for s in members]
        result = output(slot_word, after, temporal_out, modulation, parts, members, frames, result)
    return result


def solution(mesh):
    split = P(("groups", "patch"), None)
    return jax.shard_map(
        per_device,
        mesh=mesh,
        in_specs=(split, split, P(), P(), P("groups"), P("groups"), P(), P(), P(), P()),
        out_specs=split,
        check_vma=False,
    )
```

```python
import functools
import math

import jax
import jax.numpy as jnp
import numpy as np
from jax import lax
from jax.experimental import pallas as pl
from jax.experimental.pallas import tpu as pltpu
from jax.sharding import PartitionSpec as P


HEADS = 16
LANES = 128
QUERY_ROWS = 128
STRIP = 16
PAIR_GROUPS = ((0,), (1,), (2, 3))
EMIT = (False, True, True)
NEAR_GROUPS = ((0,), (1,), (2,), (3,))
STAGING_FLOPS = 4 * 10**9


epsilon = 1e-06
bf16 = jnp.bfloat16
f32 = jnp.float32
NT = (((1,), (1,)), ((), ()))


def permute(value, target):
    count = lax.axis_size("patch")
    return lax.ppermute(value, "patch", [(source, target(source)) for source in range(count)])


def partner_slot(slot, step, frames):
    if frames & (frames - 1) == 0:
        return slot ^ step
    return (slot + step) % frames


def source_slot(slot, step, frames):
    if frames & (frames - 1) == 0:
        return slot ^ step
    return (slot - step) % frames


def normalize(activations):
    row_mean = jnp.mean(activations, axis=-1, keepdims=True)
    centered = activations - row_mean
    variance = jnp.mean(centered * centered, axis=-1, keepdims=True)
    return centered * lax.rsqrt(variance + epsilon)


def column_mask(first, width, dtype):
    column = lax.broadcasted_iota(jnp.int32, (1, 2 * LANES), 1)
    inside = jnp.logical_and(column >= first, column < first + width)
    return jnp.where(inside, 1.0, 0.0).astype(dtype)


def softmax_scale(head_dim):
    return math.log2(math.e) * head_dim ** (-0.5)


def vmem_specs(count):
    return [pl.BlockSpec(memory_space=pltpu.VMEM) for _ in range(count)]


def on_chip_call(kernel, operands, shapes, flops, limit_mib, transcendentals=0, scratch=()):
    operands = [pltpu.with_memory_space_constraint(array, pltpu.VMEM) for array in operands]
    return pl.pallas_call(
        kernel,
        out_shape=[pltpu.VMEM(shape, dtype) for shape, dtype in shapes],
        in_specs=vmem_specs(len(operands)),
        out_specs=vmem_specs(len(shapes)),
        scratch_shapes=list(scratch),
        compiler_params=pltpu.CompilerParams(vmem_limit_bytes=limit_mib * 2**20),
        cost_estimate=pl.CostEstimate(
            flops=flops,
            bytes_accessed=sum(array.size * array.dtype.itemsize for array in operands),
            transcendentals=transcendentals,
        ),
    )(*operands)


def tile_copies(kv_ref, out_refs, tiles, sems):
    copies = []
    for chunk, ref in zip(tiles, out_refs):
        for at, tile in enumerate(chunk):
            copies.append(
                pltpu.make_async_copy(
                    kv_ref.at[:, tile * LANES : (tile + 1) * LANES],
                    ref.at[:, at * LANES : (at + 1) * LANES],
                    sems.at[len(copies)],
                )
            )
    return copies


def first_kernel(kv_ref, out_ref, sems, *, tiles):
    copies = tile_copies(kv_ref, [out_ref], tiles, sems)
    for copy in copies:
        copy.start()
    for copy in copies:
        copy.wait()


def stage_first(stale_kv, tiles):
    return pl.pallas_call(
        functools.partial(first_kernel, tiles=[tiles]),
        out_shape=pltpu.VMEM((stale_kv.shape[0], len(tiles) * LANES), bf16),
        in_specs=[pl.BlockSpec(memory_space=pltpu.HBM)],
        out_specs=pl.BlockSpec(memory_space=pltpu.VMEM),
        scratch_shapes=[pltpu.SemaphoreType.DMA((len(tiles),))],
        compiler_params=pltpu.CompilerParams(vmem_limit_bytes=2**20),
        name="first",
    )(pltpu.with_memory_space_constraint(stale_kv, pltpu.HBM))


def piece_kernel(slot_ref, tokens_ref, kv_ref, *refs, frames, tiles):
    out_refs, piece_sems, tile_sems = refs[:-2], refs[-2], refs[-1]
    piece = tokens_ref.shape[0] // frames
    copies = []
    for step in range(frames):
        row = partner_slot(slot_ref[0], step, frames) * piece
        copies.append(
            pltpu.make_async_copy(
                tokens_ref.at[pl.ds(row, piece), :], out_refs[step], piece_sems.at[step]
            )
        )
    copies += tile_copies(kv_ref, out_refs[frames:], tiles, tile_sems)
    for copy in copies:
        copy.start()
    for copy in copies:
        copy.wait()


def stage_pieces(slot, tokens, stale_kv, tiles, frames):
    rows, feature_width = tokens.shape
    shapes = [(rows // frames, feature_width) for _ in range(frames)]
    shapes += [(rows, len(chunk) * LANES) for chunk in tiles]
    outs = pl.pallas_call(
        functools.partial(piece_kernel, frames=frames, tiles=tiles),
        out_shape=[pltpu.VMEM(shape, bf16) for shape in shapes],
        in_specs=[
            pl.BlockSpec(memory_space=pltpu.SMEM),
            pl.BlockSpec(memory_space=pltpu.HBM),
            pl.BlockSpec(memory_space=pltpu.HBM),
        ],
        out_specs=vmem_specs(len(shapes)),
        scratch_shapes=[
            pltpu.SemaphoreType.DMA((frames,)),
            pltpu.SemaphoreType.DMA((sum(len(chunk) for chunk in tiles),)),
        ],
        compiler_params=pltpu.CompilerParams(vmem_limit_bytes=2**20),
        cost_estimate=pl.CostEstimate(
            flops=STAGING_FLOPS, bytes_accessed=4 * tokens.size, transcendentals=0
        ),
        name="pieces",
    )(
        slot,
        pltpu.with_memory_space_constraint(tokens, pltpu.HBM),
        pltpu.with_memory_space_constraint(stale_kv, pltpu.HBM),
    )
    return outs[:frames], outs[frames:]


def projection_kernel(slot_ref, time_ref, order_ref, weight_ref, *refs, frames, width):
    rate_ref, table_ref, mix_ref = refs[:3]
    pieces = refs[3 : 3 + frames]
    query_ref, kv_ref, modulation_ref, place_ref = refs[3 + frames :]
    padded = query_ref.shape[1]

    rows = -(-(frames + 1) // 8) * 8
    row = lax.broadcasted_iota(jnp.int32, (rows, 1), 0)
    position = jnp.where(row == frames, time_ref[0], 0)
    for step in range(frames):
        frame = order_ref[source_slot(slot_ref[0], step, frames)]
        position = jnp.where(row == step, frame, position)
    angles = position.astype(f32) * rate_ref[...]
    waves = jnp.concatenate([jnp.sin(angles), jnp.cos(angles)], axis=1)
    place_ref[...] = waves[:frames]
    modulation = table_ref[...] + mix_ref[...] * waves[frames : frames + 1]
    modulation_ref[...] = modulation

    tokens = jnp.concatenate([ref[...] for ref in pieces], axis=0).astype(f32)
    inputs = normalize(tokens) * (1.0 + modulation[1:2, :]) + modulation[0:1, :]
    inputs = inputs.astype(bf16)
    query_ref[...] = lax.dot_general(
        inputs, weight_ref[:padded, :], NT, preferred_element_type=f32
    ).astype(bf16)
    kv_ref[...] = lax.dot_general(
        inputs, weight_ref[width:, :], NT, preferred_element_type=f32
    ).astype(bf16)


def projections(slot, timestep, frame_order, weight, mod_table, mod_mix, pieces, width):
    frames = len(pieces)
    piece, feature_width = pieces[0].shape
    padded = -(-width // LANES) * LANES
    rows = frames * piece
    half = feature_width // 2
    rates = np.exp(-math.log(10000.0) * np.arange(half) / half).astype(np.float32)
    rates = jnp.asarray(rates[None])
    operands = [
        pltpu.with_memory_space_constraint(x, pltpu.VMEM)
        for x in (weight, rates, mod_table, mod_mix, *pieces)
    ]
    return pl.pallas_call(
        functools.partial(projection_kernel, frames=frames, width=width),
        out_shape=[
            pltpu.VMEM((rows, padded), bf16),
            pltpu.VMEM((rows, 2 * width), bf16),
            pltpu.VMEM(mod_table.shape, f32),
            pltpu.VMEM((frames, feature_width), f32),
        ],
        in_specs=[
            *[pl.BlockSpec(memory_space=pltpu.SMEM) for _ in range(3)],
            *vmem_specs(4 + frames),
        ],
        out_specs=vmem_specs(4),
        compiler_params=pltpu.CompilerParams(vmem_limit_bytes=4 * 2**20),
        cost_estimate=pl.CostEstimate(
            flops=2 * rows * feature_width * 3 * width,
            bytes_accessed=2 * weight.size,
            transcendentals=0,
        ),
        name="projections",
    )(slot, timestep, frame_order, *operands)


def stack_rows(rows, width):
    return rows * width // LANES


def stack(tiles, width):
    rows = tiles[0].shape[0]
    whole = width // LANES
    stacked = list(tiles[:whole])
    if width % LANES:
        fold = tiles[whole]
        lane = lax.broadcasted_iota(jnp.int32, (1, LANES), 1)
        low = jnp.where(lane < LANES // 2, fold[: rows // 2], 0.0)
        high = jnp.where(lane < LANES // 2, fold[rows // 2 :], 0.0)
        stacked.append(low + pltpu.roll(high, LANES // 2, 1))
    return jnp.concatenate(stacked, axis=0).astype(bf16)


def unstack(stacked, rows, width, first, count):
    whole = width // LANES
    tiles = [stacked[t * rows + first : t * rows + first + count, :] for t in range(whole)]
    if width % LANES:
        half = rows // 2
        fold = stacked[whole * rows :, :]
        turned = pltpu.roll(fold.astype(f32), LANES // 2, 1).astype(stacked.dtype)
        both = jnp.concatenate([fold, turned], axis=0)
        if first % half == 0 and count == half:
            both = turned if first else fold
        else:
            both = both[first : first + count]
        tiles.append(both[:, : LANES // 2])
    return jnp.concatenate(tiles, axis=1)


def pair_plan(width, head_dim):
    plan = []
    for first in range(0, width, 2 * head_dim):
        key_tile = first // LANES
        value_tile = (width + first) // LANES
        plan.append(
            (key_tile, first - key_tile * LANES, value_tile, width + first - value_tile * LANES)
        )
    return plan


def group_tiles(width, head_dim):
    plan = pair_plan(width, head_dim)
    seen, groups = set(), []
    for group in NEAR_GROUPS:
        need = []
        for pair in group:
            key_tile, _, value_tile, _ = plan[pair]
            need += [key_tile, key_tile + 1, value_tile, value_tile + 1]
        fresh = sorted(set(need) - seen)
        seen |= set(fresh)
        groups.append(tuple(fresh))
    return groups


def spatial_kernel(*refs, group, frames, head_dim, width, tiles, held, emitted, kept, columns, chunks, merged):
    plan = pair_plan(width, head_dim)
    count = len(tiles)
    position = 0
    refs, (scores_ref, weights_ref) = refs[:-2], refs[-2:]
    query_ref, own_ref, peer_ref = refs[:3]
    near_refs = refs[3 : 3 + count]
    far_refs = refs[3 + count : 3 + 2 * count]
    position = 3 + 2 * count
    held_ref = None
    if held:
        held_ref = refs[position]
        position += 1
    rows = query_ref.shape[0]
    piece = rows // frames
    covered = part_pieces(chunks, piece)
    earlier = dict(zip(covered, refs[position : position + len(covered)])) if merged else {}
    position += len(earlier)
    out_count = len(covered) if emitted else 0
    out_refs = dict(zip(covered, refs[position : position + out_count]))
    kept_ref = refs[position + out_count] if kept else None

    where = {tile: (c, j) for c, chunk in enumerate(tiles) for j, tile in enumerate(chunk)}

    def from_chunks(chunk_refs):
        def load(tile):
            chunk, at = where[tile]
            return chunk_refs[chunk][:, at * LANES : (at + 1) * LANES]

        return load

    def from_whole(ref):
        return lambda tile: ref[:, tile * LANES : (tile + 1) * LANES]

    blocks = [from_whole(own_ref), from_whole(peer_ref), from_chunks(near_refs), from_chunks(far_refs)]
    scale = softmax_scale(head_dim)

    def two(block, tile):
        return jnp.concatenate([block(tile), block(tile + 1)], axis=1)

    def score(index):
        chunk, pair = tasks[index]
        key_tile, key_lane, _, _ = plan[pair]
        window = query_ref[
            chunk * QUERY_ROWS : (chunk + 1) * QUERY_ROWS, key_tile * LANES : (key_tile + 2) * LANES
        ]
        stacked = jnp.concatenate(
            [
                window * column_mask(key_lane, head_dim, bf16),
                window * column_mask(key_lane + head_dim, head_dim, bf16),
            ],
            axis=0,
        )
        for number, block in enumerate(blocks):
            scores_ref[index % 2, :, number * rows : (number + 1) * rows] = lax.dot_general(
                stacked, two(block, key_tile), NT, preferred_element_type=f32
            )

    def weigh(index):
        totals = []
        for row in range(0, 2 * QUERY_ROWS, STRIP):
            scores = scores_ref[index % 2, row : row + STRIP, :]
            top = jnp.max(scores, axis=-1, keepdims=True) * scale
            weights = jnp.exp2(scores * scale - top)
            totals.append(jnp.sum(weights, axis=-1, keepdims=True))
            weights_ref[index % 2, row : row + STRIP, :] = weights.astype(bf16)
        return jnp.concatenate(totals, axis=0)

    def mix(index, total):
        _, key_lane, value_tile, value_lane = plan[tasks[index][1]]
        mixed = functools.reduce(
            jnp.add,
            [
                jnp.dot(
                    weights_ref[index % 2, :, number * rows : (number + 1) * rows],
                    two(block, value_tile),
                    preferred_element_type=f32,
                )
                for number, block in enumerate(blocks)
            ],
        )
        mixed = mixed / total
        joined = mixed[:QUERY_ROWS] * column_mask(value_lane, head_dim, f32) + mixed[
            QUERY_ROWS:
        ] * column_mask(value_lane + head_dim, head_dim, f32)
        return pltpu.roll(joined, (key_lane - value_lane) % (2 * LANES), 1)

    tasks = [(chunk, pair) for chunk in chunks for pair in group]
    parts = {}

    def finish(index, total):
        chunk, pair = tasks[index]
        joined = mix(index, total)
        tile = plan[pair][0]
        for side in range(2):
            half = joined[:, side * LANES : (side + 1) * LANES]
            parts[tile + side] = parts[tile + side] + half if tile + side in parts else half
        if pair != group[-1]:
            return
        at = chunk * QUERY_ROWS
        for number, tile in enumerate(held):
            old = held_ref[at : at + QUERY_ROWS, number * LANES : (number + 1) * LANES].astype(f32)
            parts[tile] = parts[tile] + old if tile in parts else old
        if kept:
            values = jnp.concatenate([parts[tile] for tile in kept], axis=1)
            kept_ref[at : at + QUERY_ROWS, :] = values.astype(bf16)
        if emitted:
            for sub in range(QUERY_ROWS // piece):
                cut = slice(sub * piece, (sub + 1) * piece)
                target = (at + sub * piece) // piece
                value = stack([parts[tile][cut] for tile in emitted], columns)
                if merged:
                    value = jnp.concatenate([earlier[target][...], value], axis=0)
                out_refs[target][...] = value
        parts.clear()

    score(0)
    total = None
    for index in range(len(tasks)):
        if index + 1 < len(tasks):
            score(index + 1)
        if index > 0:
            finish(index - 1, total)
        total = weigh(index)
    finish(len(tasks) - 1, total)


def near_needed(number):
    last = PAIR_GROUPS[number][-1]
    return next(n for n, group in enumerate(NEAR_GROUPS) if last in group) + 1


def tile_flow(width, head_dim):
    plan = pair_plan(width, head_dim)
    flow, held = [], ()
    for number, group in enumerate(PAIR_GROUPS):
        have = sorted({plan[pair][0] + side for pair in group for side in range(2)} | set(held))
        last = number == len(PAIR_GROUPS) - 1
        complete = [tile for tile in have if last or tile <= plan[group[-1]][0]]
        emitted = tuple(complete) if EMIT[number] else ()
        kept = tuple(tile for tile in have if tile not in emitted)
        flow.append((held, emitted, kept))
        held = kept
    return flow


def emitted_columns(emitted, width):
    return min(width, (emitted[-1] + 1) * LANES) - emitted[0] * LANES if emitted else 0


def group_columns(width, head_dim):
    flow = tile_flow(width, head_dim)
    return tuple(emitted_columns(emitted, width) for _, emitted, _ in flow if emitted)


def target_parts(rows):
    return row_parts(len(PAIR_GROUPS) - 1, rows)


def merged_pieces(rows, piece):
    parts = target_parts(rows)
    return part_pieces(parts[-2], piece) if len(parts) > 2 else []


def input_halves(rows, piece):
    parts = [part_pieces(chunks, piece) for chunks in target_parts(rows)]
    if len(parts) < 3:
        return [[s for part in parts for s in part]]
    return [parts[-1] + parts[0], [s for part in parts[1:-1] for s in part]]


def output_parts(rows, piece):
    parts = [part_pieces(chunks, piece) for chunks in target_parts(rows)]
    if len(parts) < 3:
        return [[s for part in parts for s in part]]
    return [[s for part in parts[:1] + parts[2:] for s in part], parts[1]]


def back_parts(rows):
    parts = target_parts(rows)
    return parts[:1] + parts[2:-1] + parts[1:2] + parts[-1:] if len(parts) > 2 else parts


def part_pieces(chunks, piece):
    per = QUERY_ROWS // piece
    return [chunk * per + sub for chunk in chunks for sub in range(per)]


def row_parts(number, rows):
    chunks = list(range(rows // QUERY_ROWS))
    if number < len(PAIR_GROUPS) - 1:
        return [chunks]
    return [[chunk] for chunk in reversed(chunks)]


def spatial_group(
    number, part, query, own_kv, peer_kv, near, far, carry, earlier, frames, head_dim, width
):
    group = PAIR_GROUPS[number]
    held, emitted, kept = tile_flow(width, head_dim)[number]
    arrived = near_needed(number)
    tiles = tuple(group_tiles(width, head_dim)[:arrived])
    rows = query.shape[0]
    chunks = row_parts(number, rows)[part]
    shapes = []
    columns = emitted_columns(emitted, width)
    if emitted:
        count = len(chunks) * QUERY_ROWS // (rows // frames)
        length = stack_rows(rows // frames, columns) + (earlier[0].shape[0] if earlier else 0)
        shapes += [((length, LANES), bf16) for _ in range(count)]
    if kept:
        shapes.append(((rows, len(kept) * LANES), bf16))
    operands = [query, own_kv, peer_kv, *near[:arrived], *far[:arrived]]
    if held:
        operands.append(carry)
    operands += earlier
    keys = 4 * rows
    results = on_chip_call(
        functools.partial(
            spatial_kernel,
            group=group,
            frames=frames,
            head_dim=head_dim,
            width=width,
            tiles=tiles,
            held=held,
            emitted=emitted,
            kept=kept,
            columns=columns,
            chunks=chunks,
            merged=bool(earlier),
        ),
        operands,
        shapes,
        len(group) * 2 * len(chunks) * QUERY_ROWS * keys * 256 * 4,
        8,
        len(group) * 2 * rows * keys,
        [
            pltpu.VMEM((2, 2 * QUERY_ROWS, keys), f32),
            pltpu.VMEM((2, 2 * QUERY_ROWS, keys), bf16),
        ],
    )
    results = list(results)
    carry = results.pop() if kept else None
    return results, carry


def joined_rows(tokens_refs, mixed_refs, columns, counts):
    piece = tokens_refs[0].shape[0]
    tokens = jnp.concatenate([ref[...] for ref in tokens_refs], axis=0).astype(f32)
    sizes = [stack_rows(piece, width) for width in columns]
    rows, position = [], 0
    for count in counts:
        refs = mixed_refs[position : position + count]
        position += count
        if count == 1:
            starts = [sum(sizes[:g]) for g in range(len(sizes))]
            stacks = [refs[0][at : at + size, :] for at, size in zip(starts, sizes)]
        else:
            stacks = [ref[...] for ref in refs]
        rows.append(
            jnp.concatenate(
                [unstack(x, piece, width, 0, piece) for x, width in zip(stacks, columns)], axis=1
            )
        )
    return tokens, jnp.concatenate(rows, axis=0)


def temporal_in_kernel(*refs, members, columns, counts):
    frames = len(members)
    mixed_end = frames + sum(counts)
    tokens_refs = refs[:frames]
    mixed_refs = refs[frames:mixed_end]
    out_weight, qkv_weight, modulation_ref, place_ref, query_ref, kv_ref = refs[mixed_end:]
    width = out_weight.shape[0]
    piece = tokens_refs[0].shape[0]
    tokens, mixed = joined_rows(tokens_refs, mixed_refs, columns, counts)
    after = tokens + modulation_ref[2:3, :] * jnp.dot(
        mixed, out_weight[...], preferred_element_type=f32
    )
    normal = normalize(after) * (1.0 + modulation_ref[4:5, :])
    inputs = jnp.concatenate(
        [
            (
                normal[frame * piece : (frame + 1) * piece]
                + (modulation_ref[3:4, :] + place_ref[member : member + 1, :])
            ).astype(bf16)
            for frame, member in enumerate(members)
        ],
        axis=0,
    )
    query_ref[...] = lax.dot_general(
        inputs, qkv_weight[: query_ref.shape[1], :], NT, preferred_element_type=f32
    ).astype(bf16)
    kv_ref[...] = lax.dot_general(
        inputs, qkv_weight[width:, :], NT, preferred_element_type=f32
    ).astype(bf16)


def temporal_in(members, tokens, mixed, columns, weights, modulation, places):
    width, feature_width = weights[0].shape
    padded = -(-width // LANES) * LANES
    rows = len(members) * tokens[0].shape[0]
    return on_chip_call(
        functools.partial(
            temporal_in_kernel,
            members=members,
            columns=columns,
            counts=[len(mixed[s]) for s in members],
        ),
        [
            *[tokens[s] for s in members],
            *[part for s in members for part in mixed[s]],
            *weights,
            modulation,
            places,
        ],
        [((rows, padded), bf16), ((rows, 2 * width), bf16)],
        2 * rows * feature_width * width * 4,
        8,
    )


def temporal_kernel(*refs, frames, head_dim, targets, halves):
    query_refs, kv_refs = refs[: len(halves)], refs[len(halves) : 2 * len(halves)]
    out_refs = refs[2 * len(halves) :]
    piece = sum(ref.shape[0] for ref in query_refs) // frames
    width = kv_refs[0].shape[1] // 2
    where = {s: (h, at) for h, members in enumerate(halves) for at, s in enumerate(members)}
    scale = softmax_scale(head_dim)
    step = max(16, min(piece, LANES // frames))
    block = len(targets) * step
    row_at = lax.broadcasted_iota(jnp.int32, (2 * block, frames * step), 0) % step
    column_at = lax.broadcasted_iota(jnp.int32, (2 * block, frames * step), 1) % step
    same = row_at == column_at
    plan = pair_plan(width, head_dim)

    def window(half_refs, members, start, tile):
        rows = []
        for s in members:
            half, at = where[s]
            first = at * piece + start
            rows.append(half_refs[half][first : first + step, tile * LANES : (tile + 2) * LANES])
        return jnp.concatenate(rows, axis=0)

    def score(start, tile, lane):
        queries = window(query_refs, targets, start, tile)
        stacked = jnp.concatenate(
            [
                queries * column_mask(lane, head_dim, bf16),
                queries * column_mask(lane + head_dim, head_dim, bf16),
            ],
            axis=0,
        )
        scores = lax.dot_general(
            stacked, window(kv_refs, range(frames), start, tile), NT, preferred_element_type=f32
        )
        return jnp.where(same, scores * scale, -jnp.inf)

    def weigh(scores):
        weights = jnp.exp2(scores - jnp.max(scores, axis=-1, keepdims=True))
        return (weights / jnp.sum(weights, axis=-1, keepdims=True)).astype(bf16)

    starts = range(0, piece, step)
    tasks = [(start, *entry) for start in starts for entry in plan]
    scores = [score(start, tile, lane) for start, tile, lane, _, _ in tasks]
    weights = [weigh(value) for value in scores]
    mixed_pairs = [
        jnp.dot(
            value, window(kv_refs, range(frames), start, value_tile), preferred_element_type=f32
        )
        for value, (start, _, _, value_tile, _) in zip(weights, tasks)
    ]
    parts = {start: {} for start in starts}
    for pair, (start, tile, lane, _, value_lane) in zip(mixed_pairs, tasks):
        joined = pair[:block] * column_mask(value_lane, head_dim, f32) + pair[
            block:
        ] * column_mask(value_lane + head_dim, head_dim, f32)
        joined = pltpu.roll(joined, (lane - value_lane) % (2 * LANES), 1)
        have = parts[start]
        for side in range(2):
            half = joined[:, side * LANES : (side + 1) * LANES]
            have[tile + side] = have[tile + side] + half if tile + side in have else half
    for number in range(len(targets)):
        cut = slice(number * step, (number + 1) * step)
        out_refs[number][...] = stack(
            [
                jnp.concatenate([parts[start][tile][cut] for start in starts], axis=0)
                for tile in sorted(parts[0])
            ],
            width,
        )


def temporal(queries, kvs, halves, frames, head_dim, targets):
    width = kvs[0].shape[1] // 2
    rows = sum(query.shape[0] for query in queries)
    shape = (stack_rows(rows // frames, width), LANES)
    return on_chip_call(
        functools.partial(
            temporal_kernel, frames=frames, head_dim=head_dim, targets=targets, halves=halves
        ),
        [*queries, *kvs],
        [(shape, bf16) for _ in targets],
        2 * rows * 128 * 256 * 8,
        4,
        rows * 128 * 8,
    )


def after_kernel(*refs, frames, columns, counts):
    mixed_end = frames + sum(counts)
    weight_ref, modulation_ref, out_ref = refs[mixed_end:]
    tokens, mixed = joined_rows(refs[:frames], refs[frames:mixed_end], columns, counts)
    out_ref[...] = tokens + modulation_ref[2:3, :] * jnp.dot(
        mixed, weight_ref[...], preferred_element_type=f32
    )


def after_spatial(tokens, mixed, columns, weight, modulation):
    frames = len(tokens)
    width, feature_width = weight.shape
    rows = frames * tokens[0].shape[0]
    return on_chip_call(
        functools.partial(
            after_kernel, frames=frames, columns=columns, counts=[len(part) for part in mixed]
        ),
        [*tokens, *[part for frame in mixed for part in frame], weight, modulation],
        [((rows, feature_width), f32)],
        2 * rows * feature_width * width,
        6,
    )[0]


def output_kernel(slot_ref, after_ref, weight_ref, modulation_ref, *refs, frames, members):
    parts = refs[: len(members)]
    out_ref, stage_ref, sems = refs[-3:]
    piece = after_ref.shape[0] // frames
    width = weight_ref.shape[0]
    mixed = jnp.concatenate(
        [unstack(ref[...].astype(f32), piece, width, 0, piece).astype(bf16) for ref in parts], axis=0
    )
    after = jnp.concatenate(
        [after_ref[frame * piece : (frame + 1) * piece, :] for frame in members], axis=0
    )
    stage_ref[...] = after + modulation_ref[5:6, :] * jnp.dot(
        mixed, weight_ref[...], preferred_element_type=f32
    )
    copies = []
    for number, frame in enumerate(members):
        row = partner_slot(slot_ref[0], frame, frames) * piece
        copies.append(
            pltpu.make_async_copy(
                stage_ref.at[number * piece : (number + 1) * piece, :],
                out_ref.at[pl.ds(row, piece), :],
                sems.at[number],
            )
        )
        copies[-1].start()
    for copy in copies:
        copy.wait()


def output(slot, after, weight, modulation, parts, members, frames, result):
    rows, feature_width = after.shape
    operands = [after, weight, modulation, *parts]
    specs = [pl.BlockSpec(memory_space=pltpu.SMEM), *vmem_specs(len(operands))]
    operands = [pltpu.with_memory_space_constraint(array, pltpu.VMEM) for array in operands]
    aliases = {}
    if result is not None:
        aliases = {len(specs): 0}
        specs.append(pl.BlockSpec(memory_space=pltpu.HBM))
        operands.append(result)
    return pl.pallas_call(
        functools.partial(output_kernel, frames=frames, members=members),
        out_shape=jax.ShapeDtypeStruct((rows, feature_width), f32),
        in_specs=specs,
        out_specs=pl.BlockSpec(memory_space=pltpu.HBM),
        scratch_shapes=[
            pltpu.VMEM((rows // frames * len(members), feature_width), f32),
            pltpu.SemaphoreType.DMA((len(members),)),
        ],
        input_output_aliases=aliases,
        compiler_params=pltpu.CompilerParams(vmem_limit_bytes=6 * 2**20),
    )(slot, *operands)


def per_device(
    tokens,
    stale_kv,
    mod_table,
    mod_mix,
    timestep,
    frame_order,
    spatial_qkv,
    spatial_out,
    temporal_qkv,
    temporal_out,
):
    devices = lax.axis_size("patch")
    frames = devices // 4
    slot = lax.axis_index("patch") // 4
    rows, feature_width = tokens.shape
    width = spatial_out.shape[0]
    head_dim = feature_width // HEADS
    piece = rows // frames

    def other_core(device):
        return device ^ 1

    def other_chip(device):
        return device ^ 2

    def ahead(step):
        return lambda device: partner_slot(device // 4, step, frames) * 4 + device % 4

    def behind(step):
        return lambda device: source_slot(device // 4, step, frames) * 4 + device % 4

    slot_word = slot.astype(jnp.int32)[None]
    tiles = group_tiles(width, head_dim)
    chunks = [stage_first(stale_kv, tiles[0])]
    pieces, others = stage_pieces(slot_word, tokens, stale_kv, tiles[1:], frames)
    near, far = [], []
    for chunk in [*chunks, *others]:
        near.append(permute(chunk, other_chip))
        far.append(permute(near[-1], other_core))
    peer_kv = permute(stale_kv, other_core)

    spatial_weight = jnp.swapaxes(spatial_qkv, 1, 2).reshape(3 * width, feature_width)
    there = [pieces[0]]
    there += [permute(pieces[s], ahead(s)) for s in range(1, frames)]

    query, own_kv, modulation, places = projections(
        slot_word,
        timestep,
        frame_order,
        spatial_weight,
        mod_table,
        mod_mix,
        pieces,
        width,
    )

    merged = merged_pieces(rows, piece)
    carry = None
    local = [[] for _ in range(frames)]
    sent = [[] for _ in range(frames)]
    for number in range(len(PAIR_GROUPS)):
        handed = carry
        for part, chunks in enumerate(row_parts(number, rows)):
            covered = part_pieces(chunks, piece)
            held_back = number == len(PAIR_GROUPS) - 1 and covered == merged
            outs, carry = spatial_group(
                number,
                part,
                query,
                own_kv,
                peer_kv,
                near,
                far,
                handed,
                [local[s].pop() for s in covered] if held_back else [],
                frames,
                head_dim,
                width,
            )
            for s, out in zip(covered, outs):
                local[s].append(out)
                if s == 0:
                    sent[s].append(out)
                elif s not in merged or held_back:
                    sent[s].append(permute(out, ahead(s)))

    columns = group_columns(width, head_dim)
    after = after_spatial(pieces, local, columns, spatial_out, modulation)
    weights = (spatial_out, jnp.swapaxes(temporal_qkv, 1, 2).reshape(3 * width, feature_width))
    halves = input_halves(rows, piece)
    inputs = [
        temporal_in(members, there, sent, columns, weights, modulation, places)
        for members in halves
    ]
    queries, kvs = [query for query, _ in inputs], [kv for _, kv in inputs]
    back = {}
    for chunks in back_parts(rows):
        targets = part_pieces(chunks, piece)
        outs = temporal(queries, kvs, halves, frames, head_dim, targets)
        for s, out in zip(targets, outs):
            back[s] = out if s == 0 else permute(out, behind(s))
    result = None
    for members in output_parts(rows, piece):
        parts = [back[s] for s in members]
        result = output(slot_word, after, temporal_out, modulation, parts, members, frames, result)
    return result


def solution(mesh):
    split = P(("groups", "patch"), None)
    return jax.shard_map(
        per_device,
        mesh=mesh,
        in_specs=(split, split, P(), P(), P("groups"), P("groups"), P(), P(), P(), P()),
        out_specs=split,
        check_vma=False,
    )
```

```python
import functools
import math

import jax
import jax.numpy as jnp
import numpy as np
from jax import lax
from jax.experimental import pallas as pl
from jax.experimental.pallas import tpu as pltpu
from jax.sharding import PartitionSpec as P


HEADS = 16
LANES = 128
QUERY_ROWS = 128
STRIP = 16
PAIR_GROUPS = ((0,), (1,), (2, 3))
EMIT = (False, True, True)
NEAR_GROUPS = ((0,), (1,), (2,), (3,))
STAGING_FLOPS = 4 * 10**9


epsilon = 1e-06
bf16 = jnp.bfloat16
f32 = jnp.float32
NT = (((1,), (1,)), ((), ()))


def permute(value, target):
    count = lax.axis_size("patch")
    return lax.ppermute(value, "patch", [(source, target(source)) for source in range(count)])


def partner_slot(slot, step, frames):
    if frames & (frames - 1) == 0:
        return slot ^ step
    return (slot + step) % frames


def source_slot(slot, step, frames):
    if frames & (frames - 1) == 0:
        return slot ^ step
    return (slot - step) % frames


def normalize(activations):
    row_mean = jnp.mean(activations, axis=-1, keepdims=True)
    centered = activations - row_mean
    variance = jnp.mean(centered * centered, axis=-1, keepdims=True)
    return centered * lax.rsqrt(variance + epsilon)


def column_mask(first, width, dtype):
    column = lax.broadcasted_iota(jnp.int32, (1, 2 * LANES), 1)
    inside = jnp.logical_and(column >= first, column < first + width)
    return jnp.where(inside, 1.0, 0.0).astype(dtype)


def softmax_scale(head_dim):
    return math.log2(math.e) * head_dim ** (-0.5)


def vmem_specs(count):
    return [pl.BlockSpec(memory_space=pltpu.VMEM) for _ in range(count)]


def on_chip_call(kernel, operands, shapes, flops, limit_mib, transcendentals=0, scratch=()):
    operands = [pltpu.with_memory_space_constraint(array, pltpu.VMEM) for array in operands]
    return pl.pallas_call(
        kernel,
        out_shape=[pltpu.VMEM(shape, dtype) for shape, dtype in shapes],
        in_specs=vmem_specs(len(operands)),
        out_specs=vmem_specs(len(shapes)),
        scratch_shapes=list(scratch),
        compiler_params=pltpu.CompilerParams(vmem_limit_bytes=limit_mib * 2**20),
        cost_estimate=pl.CostEstimate(
            flops=flops,
            bytes_accessed=sum(array.size * array.dtype.itemsize for array in operands),
            transcendentals=transcendentals,
        ),
    )(*operands)


def tile_copies(kv_ref, out_refs, tiles, sems):
    copies = []
    for chunk, ref in zip(tiles, out_refs):
        for at, tile in enumerate(chunk):
            copies.append(
                pltpu.make_async_copy(
                    kv_ref.at[:, tile * LANES : (tile + 1) * LANES],
                    ref.at[:, at * LANES : (at + 1) * LANES],
                    sems.at[len(copies)],
                )
            )
    return copies


def first_kernel(kv_ref, out_ref, sems, *, tiles):
    copies = tile_copies(kv_ref, [out_ref], tiles, sems)
    for copy in copies:
        copy.start()
    for copy in copies:
        copy.wait()


def stage_first(stale_kv, tiles):
    return pl.pallas_call(
        functools.partial(first_kernel, tiles=[tiles]),
        out_shape=pltpu.VMEM((stale_kv.shape[0], len(tiles) * LANES), bf16),
        in_specs=[pl.BlockSpec(memory_space=pltpu.HBM)],
        out_specs=pl.BlockSpec(memory_space=pltpu.VMEM),
        scratch_shapes=[pltpu.SemaphoreType.DMA((len(tiles),))],
        compiler_params=pltpu.CompilerParams(vmem_limit_bytes=2**20),
        name="first",
    )(pltpu.with_memory_space_constraint(stale_kv, pltpu.HBM))


def piece_kernel(slot_ref, tokens_ref, kv_ref, *refs, frames, tiles):
    out_refs, piece_sems, tile_sems = refs[:-2], refs[-2], refs[-1]
    piece = tokens_ref.shape[0] // frames
    copies = []
    for step in range(frames):
        row = partner_slot(slot_ref[0], step, frames) * piece
        copies.append(
            pltpu.make_async_copy(
                tokens_ref.at[pl.ds(row, piece), :], out_refs[step], piece_sems.at[step]
            )
        )
    copies += tile_copies(kv_ref, out_refs[frames:], tiles, tile_sems)
    for copy in copies:
        copy.start()
    for copy in copies:
        copy.wait()


def stage_pieces(slot, tokens, stale_kv, tiles, frames):
    rows, feature_width = tokens.shape
    shapes = [(rows // frames, feature_width) for _ in range(frames)]
    shapes += [(rows, len(chunk) * LANES) for chunk in tiles]
    outs = pl.pallas_call(
        functools.partial(piece_kernel, frames=frames, tiles=tiles),
        out_shape=[pltpu.VMEM(shape, bf16) for shape in shapes],
        in_specs=[
            pl.BlockSpec(memory_space=pltpu.SMEM),
            pl.BlockSpec(memory_space=pltpu.HBM),
            pl.BlockSpec(memory_space=pltpu.HBM),
        ],
        out_specs=vmem_specs(len(shapes)),
        scratch_shapes=[
            pltpu.SemaphoreType.DMA((frames,)),
            pltpu.SemaphoreType.DMA((sum(len(chunk) for chunk in tiles),)),
        ],
        compiler_params=pltpu.CompilerParams(vmem_limit_bytes=2**20),
        cost_estimate=pl.CostEstimate(
            flops=STAGING_FLOPS, bytes_accessed=4 * tokens.size, transcendentals=0
        ),
        name="pieces",
    )(
        slot,
        pltpu.with_memory_space_constraint(tokens, pltpu.HBM),
        pltpu.with_memory_space_constraint(stale_kv, pltpu.HBM),
    )
    return outs[:frames], outs[frames:]


def projection_kernel(slot_ref, time_ref, order_ref, weight_ref, *refs, frames, width):
    rate_ref, table_ref, mix_ref = refs[:3]
    pieces = refs[3 : 3 + frames]
    query_ref, kv_ref, modulation_ref, place_ref = refs[3 + frames :]
    padded = query_ref.shape[1]

    rows = -(-(frames + 1) // 8) * 8
    row = lax.broadcasted_iota(jnp.int32, (rows, 1), 0)
    position = jnp.where(row == frames, time_ref[0], 0)
    for step in range(frames):
        frame = order_ref[source_slot(slot_ref[0], step, frames)]
        position = jnp.where(row == step, frame, position)
    angles = position.astype(f32) * rate_ref[...]
    waves = jnp.concatenate([jnp.sin(angles), jnp.cos(angles)], axis=1)
    place_ref[...] = waves[:frames]
    modulation = table_ref[...] + mix_ref[...] * waves[frames : frames + 1]
    modulation_ref[...] = modulation

    tokens = jnp.concatenate([ref[...] for ref in pieces], axis=0).astype(f32)
    inputs = normalize(tokens) * (1.0 + modulation[1:2, :]) + modulation[0:1, :]
    inputs = inputs.astype(bf16)
    query_ref[...] = lax.dot_general(
        inputs, weight_ref[:padded, :], NT, preferred_element_type=f32
    ).astype(bf16)
    kv_ref[...] = lax.dot_general(
        inputs, weight_ref[width:, :], NT, preferred_element_type=f32
    ).astype(bf16)


def projections(slot, timestep, frame_order, weight, mod_table, mod_mix, pieces, width):
    frames = len(pieces)
    piece, feature_width = pieces[0].shape
    padded = -(-width // LANES) * LANES
    rows = frames * piece
    half = feature_width // 2
    rates = np.exp(-math.log(10000.0) * np.arange(half) / half).astype(np.float32)
    rates = jnp.asarray(rates[None])
    operands = [
        pltpu.with_memory_space_constraint(x, pltpu.VMEM)
        for x in (weight, rates, mod_table, mod_mix, *pieces)
    ]
    return pl.pallas_call(
        functools.partial(projection_kernel, frames=frames, width=width),
        out_shape=[
            pltpu.VMEM((rows, padded), bf16),
            pltpu.VMEM((rows, 2 * width), bf16),
            pltpu.VMEM(mod_table.shape, f32),
            pltpu.VMEM((frames, feature_width), f32),
        ],
        in_specs=[
            *[pl.BlockSpec(memory_space=pltpu.SMEM) for _ in range(3)],
            *vmem_specs(4 + frames),
        ],
        out_specs=vmem_specs(4),
        compiler_params=pltpu.CompilerParams(vmem_limit_bytes=4 * 2**20),
        cost_estimate=pl.CostEstimate(
            flops=2 * rows * feature_width * 3 * width,
            bytes_accessed=2 * weight.size,
            transcendentals=0,
        ),
        name="projections",
    )(slot, timestep, frame_order, *operands)


def stack_rows(rows, width):
    return rows * width // LANES


def stack(tiles, width):
    rows = tiles[0].shape[0]
    whole = width // LANES
    stacked = list(tiles[:whole])
    if width % LANES:
        fold = tiles[whole]
        lane = lax.broadcasted_iota(jnp.int32, (1, LANES), 1)
        low = jnp.where(lane < LANES // 2, fold[: rows // 2], 0.0)
        high = jnp.where(lane < LANES // 2, fold[rows // 2 :], 0.0)
        stacked.append(low + pltpu.roll(high, LANES // 2, 1))
    return jnp.concatenate(stacked, axis=0).astype(bf16)


def unstack(stacked, rows, width, first, count):
    whole = width // LANES
    tiles = [stacked[t * rows + first : t * rows + first + count, :] for t in range(whole)]
    if width % LANES:
        half = rows // 2
        fold = stacked[whole * rows :, :]
        turned = pltpu.roll(fold.astype(f32), LANES // 2, 1).astype(stacked.dtype)
        both = jnp.concatenate([fold, turned], axis=0)
        if first % half == 0 and count == half:
            both = turned if first else fold
        else:
            both = both[first : first + count]
        tiles.append(both[:, : LANES // 2])
    return jnp.concatenate(tiles, axis=1)


def pair_plan(width, head_dim):
    plan = []
    for first in range(0, width, 2 * head_dim):
        key_tile = first // LANES
        value_tile = (width + first) // LANES
        plan.append(
            (key_tile, first - key_tile * LANES, value_tile, width + first - value_tile * LANES)
        )
    return plan


def group_tiles(width, head_dim):
    plan = pair_plan(width, head_dim)
    seen, groups = set(), []
    for group in NEAR_GROUPS:
        need = []
        for pair in group:
            key_tile, _, value_tile, _ = plan[pair]
            need += [key_tile, key_tile + 1, value_tile, value_tile + 1]
        fresh = sorted(set(need) - seen)
        seen |= set(fresh)
        groups.append(tuple(fresh))
    return groups


def spatial_kernel(*refs, group, frames, head_dim, width, tiles, held, emitted, kept, columns, chunks, merged):
    plan = pair_plan(width, head_dim)
    count = len(tiles)
    position = 0
    refs, (scores_ref, weights_ref) = refs[:-2], refs[-2:]
    query_ref, own_ref, peer_ref = refs[:3]
    near_refs = refs[3 : 3 + count]
    far_refs = refs[3 + count : 3 + 2 * count]
    position = 3 + 2 * count
    held_ref = None
    if held:
        held_ref = refs[position]
        position += 1
    rows = query_ref.shape[0]
    piece = rows // frames
    covered = part_pieces(chunks, piece)
    earlier = dict(zip(covered, refs[position : position + len(covered)])) if merged else {}
    position += len(earlier)
    out_count = len(covered) if emitted else 0
    out_refs = dict(zip(covered, refs[position : position + out_count]))
    kept_ref = refs[position + out_count] if kept else None

    where = {tile: (c, j) for c, chunk in enumerate(tiles) for j, tile in enumerate(chunk)}

    def from_chunks(chunk_refs):
        def load(tile):
            chunk, at = where[tile]
            return chunk_refs[chunk][:, at * LANES : (at + 1) * LANES]

        return load

    def from_whole(ref):
        return lambda tile: ref[:, tile * LANES : (tile + 1) * LANES]

    blocks = [from_whole(own_ref), from_whole(peer_ref), from_chunks(near_refs), from_chunks(far_refs)]
    scale = softmax_scale(head_dim)

    def two(block, tile):
        return jnp.concatenate([block(tile), block(tile + 1)], axis=1)

    def score(index):
        chunk, pair = tasks[index]
        key_tile, key_lane, _, _ = plan[pair]
        window = query_ref[
            chunk * QUERY_ROWS : (chunk + 1) * QUERY_ROWS, key_tile * LANES : (key_tile + 2) * LANES
        ]
        stacked = jnp.concatenate(
            [
                window * column_mask(key_lane, head_dim, bf16),
                window * column_mask(key_lane + head_dim, head_dim, bf16),
            ],
            axis=0,
        )
        for number, block in enumerate(blocks):
            scores_ref[index % 2, :, number * rows : (number + 1) * rows] = lax.dot_general(
                stacked, two(block, key_tile), NT, preferred_element_type=f32
            )

    def weigh(index):
        totals = []
        for row in range(0, 2 * QUERY_ROWS, STRIP):
            scores = scores_ref[index % 2, row : row + STRIP, :]
            top = jnp.max(scores, axis=-1, keepdims=True) * scale
            weights = jnp.exp2(scores * scale - top)
            totals.append(jnp.sum(weights, axis=-1, keepdims=True))
            weights_ref[index % 2, row : row + STRIP, :] = weights.astype(bf16)
        return jnp.concatenate(totals, axis=0)

    def mix(index, total):
        _, key_lane, value_tile, value_lane = plan[tasks[index][1]]
        mixed = functools.reduce(
            jnp.add,
            [
                jnp.dot(
                    weights_ref[index % 2, :, number * rows : (number + 1) * rows],
                    two(block, value_tile),
                    preferred_element_type=f32,
                )
                for number, block in enumerate(blocks)
            ],
        )
        mixed = mixed / total
        joined = mixed[:QUERY_ROWS] * column_mask(value_lane, head_dim, f32) + mixed[
            QUERY_ROWS:
        ] * column_mask(value_lane + head_dim, head_dim, f32)
        return pltpu.roll(joined, (key_lane - value_lane) % (2 * LANES), 1)

    tasks = [(chunk, pair) for chunk in chunks for pair in group]
    parts = {}

    def finish(index, total):
        chunk, pair = tasks[index]
        joined = mix(index, total)
        tile = plan[pair][0]
        for side in range(2):
            half = joined[:, side * LANES : (side + 1) * LANES]
            parts[tile + side] = parts[tile + side] + half if tile + side in parts else half
        if pair != group[-1]:
            return
        at = chunk * QUERY_ROWS
        for number, tile in enumerate(held):
            old = held_ref[at : at + QUERY_ROWS, number * LANES : (number + 1) * LANES].astype(f32)
            parts[tile] = parts[tile] + old if tile in parts else old
        if kept:
            values = jnp.concatenate([parts[tile] for tile in kept], axis=1)
            kept_ref[at : at + QUERY_ROWS, :] = values.astype(bf16)
        if emitted:
            for sub in range(QUERY_ROWS // piece):
                cut = slice(sub * piece, (sub + 1) * piece)
                target = (at + sub * piece) // piece
                value = stack([parts[tile][cut] for tile in emitted], columns)
                if merged:
                    value = jnp.concatenate([earlier[target][...], value], axis=0)
                out_refs[target][...] = value
        parts.clear()

    score(0)
    total = None
    for index in range(len(tasks)):
        if index + 1 < len(tasks):
            score(index + 1)
        if index > 0:
            finish(index - 1, total)
        total = weigh(index)
    finish(len(tasks) - 1, total)


def near_needed(number):
    last = PAIR_GROUPS[number][-1]
    return next(n for n, group in enumerate(NEAR_GROUPS) if last in group) + 1


def tile_flow(width, head_dim):
    plan = pair_plan(width, head_dim)
    flow, held = [], ()
    for number, group in enumerate(PAIR_GROUPS):
        have = sorted({plan[pair][0] + side for pair in group for side in range(2)} | set(held))
        last = number == len(PAIR_GROUPS) - 1
        complete = [tile for tile in have if last or tile <= plan[group[-1]][0]]
        emitted = tuple(complete) if EMIT[number] else ()
        kept = tuple(tile for tile in have if tile not in emitted)
        flow.append((held, emitted, kept))
        held = kept
    return flow


def emitted_columns(emitted, width):
    return min(width, (emitted[-1] + 1) * LANES) - emitted[0] * LANES if emitted else 0


def group_columns(width, head_dim):
    flow = tile_flow(width, head_dim)
    return tuple(emitted_columns(emitted, width) for _, emitted, _ in flow if emitted)


def target_parts(rows):
    return row_parts(len(PAIR_GROUPS) - 1, rows)


def merged_pieces(rows, piece):
    parts = target_parts(rows)
    return part_pieces(parts[-2], piece) if len(parts) > 2 else []


def input_halves(rows, piece):
    parts = [part_pieces(chunks, piece) for chunks in target_parts(rows)]
    if len(parts) < 3:
        return [[s for part in parts for s in part]]
    return [parts[-1] + parts[0], [s for part in parts[1:-1] for s in part]]


def output_parts(rows, piece):
    parts = [part_pieces(chunks, piece) for chunks in target_parts(rows)]
    if len(parts) < 3:
        return [[s for part in parts for s in part]]
    return [[s for part in parts[:1] + parts[2:] for s in part], parts[1]]


def back_parts(rows):
    parts = target_parts(rows)
    if len(parts) < 3:
        return parts
    between = [chunk for part in parts[1:-1] for chunk in part]
    return [parts[0], between, parts[-1]]


def part_pieces(chunks, piece):
    per = QUERY_ROWS // piece
    return [chunk * per + sub for chunk in chunks for sub in range(per)]


def row_parts(number, rows):
    chunks = list(range(rows // QUERY_ROWS))
    if number < len(PAIR_GROUPS) - 1:
        return [chunks]
    return [[chunk] for chunk in reversed(chunks)]


def spatial_group(
    number, part, query, own_kv, peer_kv, near, far, carry, earlier, frames, head_dim, width
):
    group = PAIR_GROUPS[number]
    held, emitted, kept = tile_flow(width, head_dim)[number]
    arrived = near_needed(number)
    tiles = tuple(group_tiles(width, head_dim)[:arrived])
    rows = query.shape[0]
    chunks = row_parts(number, rows)[part]
    shapes = []
    columns = emitted_columns(emitted, width)
    if emitted:
        count = len(chunks) * QUERY_ROWS // (rows // frames)
        length = stack_rows(rows // frames, columns) + (earlier[0].shape[0] if earlier else 0)
        shapes += [((length, LANES), bf16) for _ in range(count)]
    if kept:
        shapes.append(((rows, len(kept) * LANES), bf16))
    operands = [query, own_kv, peer_kv, *near[:arrived], *far[:arrived]]
    if held:
        operands.append(carry)
    operands += earlier
    keys = 4 * rows
    results = on_chip_call(
        functools.partial(
            spatial_kernel,
            group=group,
            frames=frames,
            head_dim=head_dim,
            width=width,
            tiles=tiles,
            held=held,
            emitted=emitted,
            kept=kept,
            columns=columns,
            chunks=chunks,
            merged=bool(earlier),
        ),
        operands,
        shapes,
        len(group) * 2 * len(chunks) * QUERY_ROWS * keys * 256 * 4,
        8,
        len(group) * 2 * rows * keys,
        [
            pltpu.VMEM((2, 2 * QUERY_ROWS, keys), f32),
            pltpu.VMEM((2, 2 * QUERY_ROWS, keys), bf16),
        ],
    )
    results = list(results)
    carry = results.pop() if kept else None
    return results, carry


def joined_rows(tokens_refs, mixed_refs, columns, counts):
    piece = tokens_refs[0].shape[0]
    tokens = jnp.concatenate([ref[...] for ref in tokens_refs], axis=0).astype(f32)
    sizes = [stack_rows(piece, width) for width in columns]
    rows, position = [], 0
    for count in counts:
        refs = mixed_refs[position : position + count]
        position += count
        if count == 1:
            starts = [sum(sizes[:g]) for g in range(len(sizes))]
            stacks = [refs[0][at : at + size, :] for at, size in zip(starts, sizes)]
        else:
            stacks = [ref[...] for ref in refs]
        rows.append(
            jnp.concatenate(
                [unstack(x, piece, width, 0, piece) for x, width in zip(stacks, columns)], axis=1
            )
        )
    return tokens, jnp.concatenate(rows, axis=0)


def temporal_in_kernel(*refs, members, columns, counts):
    frames = len(members)
    mixed_end = frames + sum(counts)
    tokens_refs = refs[:frames]
    mixed_refs = refs[frames:mixed_end]
    out_weight, qkv_weight, modulation_ref, place_ref, query_ref, kv_ref = refs[mixed_end:]
    width = out_weight.shape[0]
    piece = tokens_refs[0].shape[0]
    tokens, mixed = joined_rows(tokens_refs, mixed_refs, columns, counts)
    after = tokens + modulation_ref[2:3, :] * jnp.dot(
        mixed, out_weight[...], preferred_element_type=f32
    )
    normal = normalize(after) * (1.0 + modulation_ref[4:5, :])
    inputs = jnp.concatenate(
        [
            (
                normal[frame * piece : (frame + 1) * piece]
                + (modulation_ref[3:4, :] + place_ref[member : member + 1, :])
            ).astype(bf16)
            for frame, member in enumerate(members)
        ],
        axis=0,
    )
    query_ref[...] = lax.dot_general(
        inputs, qkv_weight[: query_ref.shape[1], :], NT, preferred_element_type=f32
    ).astype(bf16)
    kv_ref[...] = lax.dot_general(
        inputs, qkv_weight[width:, :], NT, preferred_element_type=f32
    ).astype(bf16)


def temporal_in(members, tokens, mixed, columns, weights, modulation, places):
    width, feature_width = weights[0].shape
    padded = -(-width // LANES) * LANES
    rows = len(members) * tokens[0].shape[0]
    return on_chip_call(
        functools.partial(
            temporal_in_kernel,
            members=members,
            columns=columns,
            counts=[len(mixed[s]) for s in members],
        ),
        [
            *[tokens[s] for s in members],
            *[part for s in members for part in mixed[s]],
            *weights,
            modulation,
            places,
        ],
        [((rows, padded), bf16), ((rows, 2 * width), bf16)],
        2 * rows * feature_width * width * 4,
        8,
    )


def temporal_kernel(*refs, frames, head_dim, targets, halves):
    query_refs, kv_refs = refs[: len(halves)], refs[len(halves) : 2 * len(halves)]
    out_refs = refs[2 * len(halves) :]
    piece = sum(ref.shape[0] for ref in query_refs) // frames
    width = kv_refs[0].shape[1] // 2
    where = {s: (h, at) for h, members in enumerate(halves) for at, s in enumerate(members)}
    scale = softmax_scale(head_dim)
    step = max(16, min(piece, LANES // frames))
    block = len(targets) * step
    row_at = lax.broadcasted_iota(jnp.int32, (2 * block, frames * step), 0) % step
    column_at = lax.broadcasted_iota(jnp.int32, (2 * block, frames * step), 1) % step
    same = row_at == column_at
    plan = pair_plan(width, head_dim)

    def window(half_refs, members, start, tile):
        rows = []
        for s in members:
            half, at = where[s]
            first = at * piece + start
            rows.append(half_refs[half][first : first + step, tile * LANES : (tile + 2) * LANES])
        return jnp.concatenate(rows, axis=0)

    def score(start, tile, lane):
        queries = window(query_refs, targets, start, tile)
        stacked = jnp.concatenate(
            [
                queries * column_mask(lane, head_dim, bf16),
                queries * column_mask(lane + head_dim, head_dim, bf16),
            ],
            axis=0,
        )
        scores = lax.dot_general(
            stacked, window(kv_refs, range(frames), start, tile), NT, preferred_element_type=f32
        )
        return jnp.where(same, scores * scale, -jnp.inf)

    def weigh(scores):
        weights = jnp.exp2(scores - jnp.max(scores, axis=-1, keepdims=True))
        return (weights / jnp.sum(weights, axis=-1, keepdims=True)).astype(bf16)

    starts = range(0, piece, step)
    tasks = [(start, *entry) for start in starts for entry in plan]
    scores = [score(start, tile, lane) for start, tile, lane, _, _ in tasks]
    weights = [weigh(value) for value in scores]
    mixed_pairs = [
        jnp.dot(
            value, window(kv_refs, range(frames), start, value_tile), preferred_element_type=f32
        )
        for value, (start, _, _, value_tile, _) in zip(weights, tasks)
    ]
    parts = {start: {} for start in starts}
    for pair, (start, tile, lane, _, value_lane) in zip(mixed_pairs, tasks):
        joined = pair[:block] * column_mask(value_lane, head_dim, f32) + pair[
            block:
        ] * column_mask(value_lane + head_dim, head_dim, f32)
        joined = pltpu.roll(joined, (lane - value_lane) % (2 * LANES), 1)
        have = parts[start]
        for side in range(2):
            half = joined[:, side * LANES : (side + 1) * LANES]
            have[tile + side] = have[tile + side] + half if tile + side in have else half
    for number in range(len(targets)):
        cut = slice(number * step, (number + 1) * step)
        out_refs[number][...] = stack(
            [
                jnp.concatenate([parts[start][tile][cut] for start in starts], axis=0)
                for tile in sorted(parts[0])
            ],
            width,
        )


def temporal(queries, kvs, halves, frames, head_dim, targets):
    width = kvs[0].shape[1] // 2
    rows = sum(query.shape[0] for query in queries)
    shape = (stack_rows(rows // frames, width), LANES)
    return on_chip_call(
        functools.partial(
            temporal_kernel, frames=frames, head_dim=head_dim, targets=targets, halves=halves
        ),
        [*queries, *kvs],
        [(shape, bf16) for _ in targets],
        2 * rows * 128 * 256 * 8,
        4,
        rows * 128 * 8,
    )


def after_kernel(*refs, frames, columns, counts):
    mixed_end = frames + sum(counts)
    weight_ref, modulation_ref, out_ref = refs[mixed_end:]
    tokens, mixed = joined_rows(refs[:frames], refs[frames:mixed_end], columns, counts)
    out_ref[...] = tokens + modulation_ref[2:3, :] * jnp.dot(
        mixed, weight_ref[...], preferred_element_type=f32
    )


def after_spatial(tokens, mixed, columns, weight, modulation):
    frames = len(tokens)
    width, feature_width = weight.shape
    rows = frames * tokens[0].shape[0]
    return on_chip_call(
        functools.partial(
            after_kernel, frames=frames, columns=columns, counts=[len(part) for part in mixed]
        ),
        [*tokens, *[part for frame in mixed for part in frame], weight, modulation],
        [((rows, feature_width), f32)],
        2 * rows * feature_width * width,
        6,
    )[0]


def output_kernel(slot_ref, after_ref, weight_ref, modulation_ref, *refs, frames, members):
    parts = refs[: len(members)]
    out_ref, stage_ref, sems = refs[-3:]
    piece = after_ref.shape[0] // frames
    width = weight_ref.shape[0]
    mixed = jnp.concatenate(
        [unstack(ref[...].astype(f32), piece, width, 0, piece).astype(bf16) for ref in parts], axis=0
    )
    after = jnp.concatenate(
        [after_ref[frame * piece : (frame + 1) * piece, :] for frame in members], axis=0
    )
    stage_ref[...] = after + modulation_ref[5:6, :] * jnp.dot(
        mixed, weight_ref[...], preferred_element_type=f32
    )
    copies = []
    for number, frame in enumerate(members):
        row = partner_slot(slot_ref[0], frame, frames) * piece
        copies.append(
            pltpu.make_async_copy(
                stage_ref.at[number * piece : (number + 1) * piece, :],
                out_ref.at[pl.ds(row, piece), :],
                sems.at[number],
            )
        )
        copies[-1].start()
    for copy in copies:
        copy.wait()


def output(slot, after, weight, modulation, parts, members, frames, result):
    rows, feature_width = after.shape
    operands = [after, weight, modulation, *parts]
    specs = [pl.BlockSpec(memory_space=pltpu.SMEM), *vmem_specs(len(operands))]
    operands = [pltpu.with_memory_space_constraint(array, pltpu.VMEM) for array in operands]
    aliases = {}
    if result is not None:
        aliases = {len(specs): 0}
        specs.append(pl.BlockSpec(memory_space=pltpu.HBM))
        operands.append(result)
    return pl.pallas_call(
        functools.partial(output_kernel, frames=frames, members=members),
        out_shape=jax.ShapeDtypeStruct((rows, feature_width), f32),
        in_specs=specs,
        out_specs=pl.BlockSpec(memory_space=pltpu.HBM),
        scratch_shapes=[
            pltpu.VMEM((rows // frames * len(members), feature_width), f32),
            pltpu.SemaphoreType.DMA((len(members),)),
        ],
        input_output_aliases=aliases,
        compiler_params=pltpu.CompilerParams(vmem_limit_bytes=6 * 2**20),
    )(slot, *operands)


def per_device(
    tokens,
    stale_kv,
    mod_table,
    mod_mix,
    timestep,
    frame_order,
    spatial_qkv,
    spatial_out,
    temporal_qkv,
    temporal_out,
):
    devices = lax.axis_size("patch")
    frames = devices // 4
    slot = lax.axis_index("patch") // 4
    rows, feature_width = tokens.shape
    width = spatial_out.shape[0]
    head_dim = feature_width // HEADS
    piece = rows // frames

    def other_core(device):
        return device ^ 1

    def other_chip(device):
        return device ^ 2

    def ahead(step):
        return lambda device: partner_slot(device // 4, step, frames) * 4 + device % 4

    def behind(step):
        return lambda device: source_slot(device // 4, step, frames) * 4 + device % 4

    slot_word = slot.astype(jnp.int32)[None]
    tiles = group_tiles(width, head_dim)
    chunks = [stage_first(stale_kv, tiles[0])]
    pieces, others = stage_pieces(slot_word, tokens, stale_kv, tiles[1:], frames)
    near, far = [], []
    for chunk in [*chunks, *others]:
        near.append(permute(chunk, other_chip))
        far.append(permute(near[-1], other_core))
    peer_kv = permute(stale_kv, other_core)

    spatial_weight = jnp.swapaxes(spatial_qkv, 1, 2).reshape(3 * width, feature_width)
    there = [pieces[0]]
    there += [permute(pieces[s], ahead(s)) for s in range(1, frames)]

    query, own_kv, modulation, places = projections(
        slot_word,
        timestep,
        frame_order,
        spatial_weight,
        mod_table,
        mod_mix,
        pieces,
        width,
    )

    merged = merged_pieces(rows, piece)
    carry = None
    local = [[] for _ in range(frames)]
    sent = [[] for _ in range(frames)]
    for number in range(len(PAIR_GROUPS)):
        handed = carry
        for part, chunks in enumerate(row_parts(number, rows)):
            covered = part_pieces(chunks, piece)
            held_back = number == len(PAIR_GROUPS) - 1 and covered == merged
            outs, carry = spatial_group(
                number,
                part,
                query,
                own_kv,
                peer_kv,
                near,
                far,
                handed,
                [local[s].pop() for s in covered] if held_back else [],
                frames,
                head_dim,
                width,
            )
            for s, out in zip(covered, outs):
                local[s].append(out)
                if s == 0:
                    sent[s].append(out)
                elif s not in merged or held_back:
                    sent[s].append(permute(out, ahead(s)))

    columns = group_columns(width, head_dim)
    after = after_spatial(pieces, local, columns, spatial_out, modulation)
    weights = (spatial_out, jnp.swapaxes(temporal_qkv, 1, 2).reshape(3 * width, feature_width))
    halves = input_halves(rows, piece)
    inputs = [
        temporal_in(members, there, sent, columns, weights, modulation, places)
        for members in halves
    ]
    queries, kvs = [query for query, _ in inputs], [kv for _, kv in inputs]
    back = {}
    for chunks in back_parts(rows):
        targets = part_pieces(chunks, piece)
        outs = temporal(queries, kvs, halves, frames, head_dim, targets)
        for s, out in zip(targets, outs):
            back[s] = out if s == 0 else permute(out, behind(s))
    result = None
    for members in output_parts(rows, piece):
        parts = [back[s] for s in members]
        result = output(slot_word, after, temporal_out, modulation, parts, members, frames, result)
    return result


def solution(mesh):
    split = P(("groups", "patch"), None)
    return jax.shard_map(
        per_device,
        mesh=mesh,
        in_specs=(split, split, P(), P(), P("groups"), P("groups"), P(), P(), P(), P()),
        out_specs=split,
        check_vma=False,
    )
```
